128 devices in a mesh: dp: 64 (over y, x, z_lo, core), mp: 2 (over z_hi).
Axes of the slice: x: 4, y: 4, z: 4 (z_hi: 2, z_lo: 2; z = z_hi * 2 + z_lo), core: 2. Of those that a mesh axis runs over, the one named last changes fastest.
Arguments:
- clean_latent: float32 [64, 4096], P('dp'), may hold values from -6 to 6
- noise_draw: float32 [64, 4096], P('dp'), may hold values from -6 to 6
- timestep: int32 [64], P('dp'), may hold values from 1 to 8
- bucket: int32 [64], P('dp'), may hold values from 0 to 7
- bucket_weights: float32 [8], replicated, may hold values from 0.25 to 4
- teacher_embed: float32 [16, 2048], replicated, may hold values from -1.5 to 1.5
- teacher_final: float32 [16, 2048], replicated, may hold values from -0.125 to 0.125
- teacher_mod: float32 [16, 3, 2048], replicated, may hold values from -3 to 3
- teacher_qkv: bfloat16 [2048, 3, 1024], P(None, None, 'mp'), may hold values from -1 to 1
- teacher_out: bfloat16 [2048, 1024], P(None, 'mp'), may hold values from -0.1875 to 0.1875
- student_embed: float32 [16, 2048], replicated, may hold values from -1.5 to 1.5
- student_final: float32 [16, 2048], replicated, may hold values from -0.125 to 0.125
- student_mod: float32 [8, 3, 2048], replicated, may hold values from -3 to 3
- student_qkv: bfloat16 [2048, 3, 1024], P('dp', None, 'mp'), may hold values from -1 to 1
- student_out: bfloat16 [2048, 1024], P('dp', 'mp'), may hold values from -0.1875 to 0.1875
- moment_qkv: float32 [2048, 3, 1024], P('dp', None, 'mp'), may hold values from -2 to 2
- second_qkv: float32 [2048, 3, 1024], P('dp', None, 'mp'), may hold values from 0.05 to 0.5
- moment_out: float32 [2048, 1024], P('dp', 'mp'), may hold values from -2 to 2
- second_out: float32 [2048, 1024], P('dp', 'mp'), may hold values from 0.05 to 0.5
Outputs:
- new_moment_qkv: float32 [2048, 3, 1024], P('dp', None, 'mp')
- new_second_qkv: float32 [2048, 3, 1024], P('dp', None, 'mp')
- update_qkv: float32 [2048, 3, 1024], P('dp', None, 'mp')
- new_moment_out: float32 [2048, 1024], P('dp', 'mp')
- new_second_out: float32 [2048, 1024], P('dp', 'mp')
- update_out: float32 [2048, 1024], P('dp', 'mp')
- loss: float32 [], replicated
The draws below stay inside these ranges and needn't reach their ends.
All inputs are finite; a program needn't handle non-finite values.
Results may differ from the reference program's by a relative error of at most 0.00035.
Values may be sent and summed in bfloat16 or wider, within the bound.
A program may use at most 128 MiB of HBM per device.

```python
import math
import jax
import jax.numpy as jnp
from jax import lax

D = 2048
HEADS = 16
HS = 64
INNER = 1024
PATCH_CH = 16
SEQ = 256
LATENT = 4096
SAMPLES = 64
K = 8
TGRID = 16
NBUCKET = 8


def aligned_projection(seed_key, salt):
    folded = jax.random.fold_in(seed_key, salt)
    initial = jax.random.normal(folded, (D, 3, INNER), jnp.float32) / math.sqrt(D)
    return jnp.clip(initial, -1.0, 1.0).astype(jnp.bfloat16)


def draw_teacher_qkv(key, part):
    return aligned_projection(key, 11)


def draw_student_qkv(key, part):
    return aligned_projection(key, 23)


def set_ends(entries, key, smallest, largest):
    place = [jax.random.randint(jax.random.fold_in(key, axis), (), 0, length) for axis, length in enumerate(entries.shape)]
    longest = entries.shape.index(max(entries.shape))
    next_to = place[:longest] + [(place[longest] + 1) % entries.shape[longest]] + place[longest + 1:]
    return entries.at[tuple(place)].set(smallest).at[tuple(next_to)].set(largest)


def block_scale(key, extent, shards, least, high):
    gain = 1.0
    for position, blocks in shards:
        draws = jax.random.uniform(jax.random.fold_in(jax.random.fold_in(key, 6), position), (blocks,), jnp.float32, least / len(shards), high / len(shards))
        gain = gain * jnp.repeat(jnp.exp(draws), extent[position] // blocks).reshape((-1,) + (1,) * (len(extent) - 1 - position))
    return gain


def noise(rng, extent, scale, bound, shards=(), kind=jnp.bfloat16):
    values = jax.random.normal(rng, extent, jnp.float32) * scale
    if len(shards) > 0:
        values = block_scale(rng, extent, shards, -0.22, 0.18) * values
    return jnp.clip(values, min=-bound, max=bound).astype(kind)


def setup_inputs(seed: int = 0) -> dict:
    splits = jax.random.split(jax.random.key(seed), 20)
    return {
        "clean_latent": noise(splits[0], (SAMPLES, LATENT), 1.0, 6.0, ((0, 64),), jnp.float32),
        "noise_draw": noise(splits[1], (SAMPLES, LATENT), 1.0, 6.0, ((0, 64),), jnp.float32),
        "timestep": set_ends(jax.random.randint(splits[2], (SAMPLES,), 1, K + 1), jax.random.fold_in(splits[2], 1), 1, K).astype(jnp.int32),
        "bucket": set_ends(jax.random.randint(splits[3], (SAMPLES,), 0, NBUCKET), jax.random.fold_in(splits[3], 1), 0, NBUCKET - 1).astype(jnp.int32),
        "bucket_weights": jnp.clip(jnp.exp(jax.random.uniform(splits[4], (NBUCKET,), jnp.float32, math.log(0.25), math.log(4.0))), 0.25, 4.0),
        "teacher_embed": noise(splits[5], (PATCH_CH, D), PATCH_CH ** -0.5, 1.5, (), jnp.float32),
        "teacher_final": noise(splits[6], (PATCH_CH, D), D ** -0.5, 0.125, (), jnp.float32),
        "teacher_mod": noise(splits[7], (TGRID, 3, D), 0.5, 3.0, (), jnp.float32),
        "teacher_qkv": draw_teacher_qkv(jax.random.fold_in(splits[19], 71), 0),
        "teacher_out": noise(splits[9], (D, INNER), INNER ** -0.5, 0.1875, ((1, 2),)),
        "student_embed": noise(splits[10], (PATCH_CH, D), PATCH_CH ** -0.5, 1.5, (), jnp.float32),
        "student_final": noise(splits[11], (PATCH_CH, D), D ** -0.5, 0.125, (), jnp.float32),
        "student_mod": noise(splits[12], (K, 3, D), 0.5, 3.0, (), jnp.float32),
        "student_qkv": draw_student_qkv(jax.random.fold_in(splits[19], 71), 0),
        "student_out": noise(splits[14], (D, INNER), INNER ** -0.5, 0.1875, ((0, 64), (1, 2))),
        "moment_qkv": noise(splits[15], (D, 3, INNER), 0.3, 2.0, ((0, 64), (2, 2)), jnp.float32),
        "second_qkv": jnp.clip(jnp.exp(math.log(0.5) - 2.3025851 * jax.random.uniform(splits[16], (D, 3, INNER), jnp.float32) ** block_scale(splits[16], (D, 3, INNER), ((0, 64), (2, 2)), -0.2, 0.2)), 0.05, 0.5),
        "moment_out": noise(splits[17], (D, INNER), 0.3, 2.0, ((0, 64), (1, 2)), jnp.float32),
        "second_out": jnp.clip(jnp.exp(math.log(0.5) - 2.3025851 * jax.random.uniform(splits[18], (D, INNER), jnp.float32) ** block_scale(splits[18], (D, INNER), ((0, 64), (1, 2)), -0.2, 0.2)), 0.05, 0.5),
    }


LN_EPS = 0.01
BETA_ONE = 0.9
BETA_TWO = 0.99
ADAM_EPS = 1e-08

def plan():
    grid = jnp.arange(TGRID + 1, dtype=jnp.float32)
    lamb = 6.0 - 12.0 * grid / TGRID
    return (jnp.sqrt(jax.nn.sigmoid(lamb)), jnp.sqrt(jax.nn.sigmoid(-lamb)))

def positions():
    index = jnp.arange(SEQ, dtype=jnp.float32)[:, None]
    half = D // 2
    freqs = jnp.exp(-math.log(10000.0) * jnp.arange(half, dtype=jnp.float32) / half)
    angles = index * freqs[None, :]
    return jnp.concatenate([jnp.sin(angles), jnp.cos(angles)], axis=1)

def normalize(values):
    center = values - lax.optimization_barrier(jnp.mean(values, axis=-1, keepdims=True))
    inverse = lax.rsqrt(lax.optimization_barrier(jnp.mean(center * center, axis=-1, keepdims=True)) + LN_EPS)
    return (center * inverse, inverse)

def norm_back(upstream, normed, inverse):
    first_mean = lax.optimization_barrier(jnp.mean(upstream, axis=-1, keepdims=True))
    second_mean = lax.optimization_barrier(jnp.mean(upstream * normed, axis=-1, keepdims=True))
    return (upstream - first_mean - normed * second_mean) * inverse

def front(latent, modrow, embed, w_qkv, w_out, placed):
    hidden = jnp.dot(latent, embed, precision=lax.Precision.HIGHEST) + placed
    normed, unused = normalize(hidden)
    shaped = (normed * (1.0 + modrow[1]) + modrow[0]).astype(jnp.bfloat16)
    packed = jnp.dot(shaped, w_qkv.reshape(D, 3 * INNER), preferred_element_type=jnp.float32)
    packed = packed.astype(jnp.bfloat16).reshape(SEQ, 3, HEADS, HS)
    queries = packed[:, 0]
    keys_all = packed[:, 1]
    values = packed[:, 2]
    scores = jnp.einsum('qhd,khd->hqk', queries.astype(jnp.float32), keys_all.astype(jnp.float32)) / math.sqrt(HS)
    weights = jax.nn.softmax(scores, axis=-1)
    rounded = weights.astype(jnp.bfloat16)
    attended = jnp.einsum('hqk,khd->qhd', rounded.astype(jnp.float32), values.astype(jnp.float32))
    attended = attended.astype(jnp.bfloat16).reshape(SEQ, INNER)
    projected = lax.dot_general(attended, w_out, (((1,), (1,)), ((), ())), preferred_element_type=jnp.float32)
    return (hidden, shaped, queries, keys_all, values, weights, rounded, attended, projected)

def tail(hidden, modrow, projected, final):
    mixed = hidden + modrow[2] * projected
    normed, inverse = normalize(mixed)
    predicted = jnp.dot(normed, final.T, precision=lax.Precision.HIGHEST)
    return (predicted, normed, inverse)

def reference(clean_latent, noise_draw, timestep, bucket, bucket_weights, teacher_embed, teacher_final, teacher_mod, teacher_qkv, teacher_out, student_embed, student_final, student_mod, student_qkv, student_out, moment_qkv, second_qkv, moment_out, second_out):
    alphas, sigmas = plan()
    placed = positions()

    def teacher_eps(latent, modrow):
        parts = front(latent, modrow, teacher_embed, teacher_qkv, teacher_out, placed)
        return tail(parts[0], modrow, parts[8], teacher_final)[0]

    def sample_step(carry, inputs):
        clean_row, noise_row, step_index, bucket_id = inputs
        first = 2 * step_index
        middle = first - 1
        last = first - 2
        a_first, s_first = (alphas[first], sigmas[first])
        a_middle, s_middle = (alphas[middle], sigmas[middle])
        a_last, s_last = (alphas[last], sigmas[last])
        latent0 = (a_first * clean_row + s_first * noise_row).reshape(SEQ, PATCH_CH)
        eps_zero = teacher_eps(latent0, teacher_mod[first - 1])
        latent1 = a_middle * (latent0 - s_first * eps_zero) / a_first + s_middle * eps_zero
        eps_one = teacher_eps(latent1, teacher_mod[middle - 1])
        latent2 = a_last * (latent1 - s_middle * eps_one) / a_middle + s_last * eps_one
        target = (latent0 - a_first / a_last * latent2) / (s_first - a_first * s_last / a_last)
        modrow = student_mod[step_index - 1]
        hidden, shaped, queries, keys_all, values, weights, rounded, attended, projected = front(latent0, modrow, student_embed, student_qkv, student_out, placed)
        predicted, normed, inverse = tail(hidden, modrow, projected, student_final)
        weight = bucket_weights[bucket_id]
        error = predicted - target
        sample_loss = weight * jnp.sum(error * error)
        d_pred = 2.0 * weight * error
        d_normed = jnp.dot(d_pred, student_final, precision=lax.Precision.HIGHEST)
        d_mixed = norm_back(d_normed, normed, inverse)
        d_proj = (modrow[2] * d_mixed).astype(jnp.bfloat16)
        grad_out = lax.dot_general(d_proj, attended, (((0,), (0,)), ((), ())), preferred_element_type=jnp.float32)
        d_attn = jnp.dot(d_proj, student_out, preferred_element_type=jnp.float32).astype(jnp.bfloat16)
        d_attn = d_attn.reshape(SEQ, HEADS, HS).astype(jnp.float32)
        d_prob = jnp.einsum('qhd,khd->hqk', d_attn, values.astype(jnp.float32))
        d_score = (weights * (d_prob - lax.optimization_barrier(jnp.sum(weights * d_prob, axis=-1, keepdims=True))) / math.sqrt(HS)).astype(jnp.bfloat16)
        d_score = d_score.astype(jnp.float32)
        d_query = jnp.einsum('hqk,khd->qhd', d_score, keys_all.astype(jnp.float32)).astype(jnp.bfloat16)
        d_key = jnp.einsum('hqk,qhd->khd', d_score, queries.astype(jnp.float32)).astype(jnp.bfloat16)
        d_value = jnp.einsum('hqk,qhd->khd', rounded.astype(jnp.float32), d_attn).astype(jnp.bfloat16)
        d_pack = jnp.stack([d_query, d_key, d_value], axis=1).reshape(SEQ, 3 * INNER)
        grad_qkv = lax.dot_general(shaped, d_pack, (((0,), (0,)), ((), ())), preferred_element_type=jnp.float32)
        return ((carry[0] + grad_qkv, carry[1] + grad_out, carry[2] + sample_loss), None)
    start_carry = (jnp.zeros((D, 3 * INNER), jnp.float32), jnp.zeros((D, INNER), jnp.float32), jnp.zeros((), jnp.float32))
    sums, unused = lax.scan(sample_step, start_carry, (clean_latent, noise_draw, timestep, bucket))
    grad_qkv = sums[0].reshape(D, 3, INNER)
    grad_out = sums[1]
    squares = jnp.sum(grad_qkv * grad_qkv) + jnp.sum(grad_out * grad_out)
    rms_value = jnp.sqrt(squares / (4 * D * INNER))
    factor = 1.0 / jnp.maximum(rms_value, 1.0)

    def adam(moment, second, grad):
        normed_grad = grad * factor
        new_moment = BETA_ONE * moment + (1.0 - BETA_ONE) * normed_grad
        new_second = BETA_TWO * second + (1.0 - BETA_TWO) * normed_grad * normed_grad
        return (new_moment, new_second, new_moment / (jnp.sqrt(new_second) + ADAM_EPS))
    mq, vq, uq = adam(moment_qkv, second_qkv, grad_qkv)
    mo, vo, uo = adam(moment_out, second_out, grad_out)
    loss = sums[2] / (SAMPLES * LATENT)
    return (mq, vq, uq, mo, vo, uo, loss)
```

```python
import math

import jax
import jax.numpy as jnp
from jax import lax
from jax.experimental import pallas as pl
from jax.experimental.pallas import tpu as pltpu
from jax.sharding import Mesh
from jax.sharding import PartitionSpec as P

D = 2048
HS = 64
INNER = 1024
PATCH_CH = 16
SEQ = 256
LATENT = 4096
K = 8
TGRID = 16
NBUCKET = 8
DP = ("dp_0", "dp_1", "dp_2", "dp_3")
DP_MP = ("dp_0", "dp_1", "dp_2", "dp_3", "mp")


LN_EPS = 0.01
BETA_ONE = 0.9
BETA_TWO = 0.99
ADAM_EPS = 1e-08


ROWS = 1024
HALF = 1024
AXES = ("dp_0", "dp_1", "dp_2", "dp_3", "mp")


def remote(src, dst, send, recv, axis, target):
    return pltpu.make_async_remote_copy(
        src_ref=src,
        dst_ref=dst,
        send_sem=send,
        recv_sem=recv,
        device_id={axis: target},
        device_id_type=pl.DeviceIdType.MESH,
    )


def ring_start(axis, part, relay, direct, send, recv):
    me = lax.axis_index(axis)
    right, left, far = (lax.rem(me + k, 4) for k in (1, 3, 2))
    half = part.shape[1] // 2
    top, low = pl.ds(0, half), pl.ds(half, half)
    copies = [
        remote(part.at[far, top], relay.at[0], send.at[0], recv.at[0], axis, right),
        remote(part.at[far, low], relay.at[1], send.at[1], recv.at[1], axis, left),
        remote(part.at[right, low], direct.at[0], send.at[2], recv.at[2], axis, right),
        remote(part.at[left, top], direct.at[1], send.at[3], recv.at[3], axis, left),
    ]
    for c in copies:
        c.start()
    return copies


def ring_relay(axis, copies, part, relay, passed, summed, send, recv):
    me = lax.axis_index(axis)
    right, left = (lax.rem(me + k, 4) for k in (1, 3))
    half = part.shape[1] // 2
    top, low = pl.ds(0, half), pl.ds(half, half)
    copies[0].wait_recv()
    passed[0] = relay[0] + part[right, top]
    first = remote(passed.at[0], summed.at[0], send.at[4], recv.at[4], axis, right)
    first.start()
    copies[1].wait_recv()
    passed[1] = relay[1] + part[left, low]
    second = remote(passed.at[1], summed.at[1], send.at[5], recv.at[5], axis, left)
    second.start()
    return [first, second]


def ring_finish(axis, copies, more, part, direct, summed):
    me = lax.axis_index(axis)
    half = part.shape[1] // 2
    copies[3].wait_recv()
    more[0].wait_recv()
    upper = part[me, pl.ds(0, half)] + direct[1] + summed[0]
    copies[2].wait_recv()
    more[1].wait_recv()
    lower = part[me, pl.ds(half, half)] + direct[0] + summed[1]
    for c in [*copies, *more]:
        c.wait_send()
    return upper, lower


def reduce_kernel(
    shaped_own,
    shaped_other,
    proj_own,
    proj_other,
    packed,
    out,
    shaped_in,
    proj_in,
    packed_in,
    part_a,
    part_b,
    part_c,
    part_d,
    *rest,
):
    boxes_a, boxes_b, boxes_c, boxes_d = rest[0:4], rest[4:8], rest[8:12], rest[12:16]
    last, last_in, pair_send, pair_recv, send, recv, z_send, z_recv = rest[16:]
    y, x, z, core = (lax.axis_index(a) for a in AXES[:4])
    barrier = pltpu.get_barrier_semaphore()
    friends = [("dp_3", 1 - core), ("dp_2", 1 - z)]
    friends += [("dp_1", lax.rem(x + k, 4)) for k in (1, 3)]
    friends += [("dp_0", lax.rem(y + k, 4)) for k in (1, 3)]
    for axis, target in friends:
        pl.semaphore_signal(
            barrier, inc=1, device_id={axis: target}, device_id_type=pl.DeviceIdType.MESH
        )
    pl.semaphore_wait(barrier, len(friends))

    pair = [
        remote(a, b, pair_send.at[k], pair_recv.at[k], "dp_3", 1 - core)
        for k, (a, b) in enumerate(
            [(packed, packed_in), (shaped_other, shaped_in), (proj_other, proj_in)]
        )
    ]
    for c in pair:
        c.start()

    def products(s_ref, p_ref, b_ref, add):
        def step(k, carry):
            rows = pl.ds(pl.multiple_of(k * 256, 256), 256)
            s, p = s_ref[rows], p_ref[rows]
            g = jnp.dot(s, b_ref[:, :HALF], preferred_element_type=jnp.float32)
            for j in range(4):
                block = g[64 * j : 64 * j + 64]
                spot = pl.ds(pl.multiple_of(k * 64, 64), 64)
                part_a[j, spot] = part_a[j, spot] + block if add else block
            h = jnp.dot(s, b_ref[:, HALF : HALF + 512], preferred_element_type=jnp.float32)
            part_b[k, :, 0:512] = part_b[k, :, 0:512] + h if add else h
            o = jnp.dot(p, b_ref[:, HALF + 512 :], preferred_element_type=jnp.float32)
            part_b[k, :, 512:1024] = part_b[k, :, 512:1024] + o if add else o
            return carry

        lax.fori_loop(0, 4, step, 0)

    products(shaped_own, proj_own, packed, False)
    for c in pair:
        c.wait_recv()
    products(shaped_in, proj_in, packed_in, True)

    first_a = ring_start("dp_1", part_a, boxes_a[0], boxes_a[1], send.at[0], recv.at[0])
    first_b = ring_start("dp_0", part_b, boxes_b[0], boxes_b[1], send.at[1], recv.at[1])
    more_a = ring_relay(
        "dp_1", first_a, part_a, boxes_a[0], boxes_a[2], boxes_a[3], send.at[0], recv.at[0]
    )
    more_b = ring_relay(
        "dp_0", first_b, part_b, boxes_b[0], boxes_b[2], boxes_b[3], send.at[1], recv.at[1]
    )
    upper, lower = ring_finish("dp_1", first_a, more_a, part_a, boxes_a[1], boxes_a[3])
    for k in range(2):
        part_c[k] = upper[64 * k : 64 * k + 64]
        part_c[2 + k] = lower[64 * k : 64 * k + 64]
    first_c = ring_start("dp_0", part_c, boxes_c[0], boxes_c[1], send.at[2], recv.at[2])
    upper, lower = ring_finish("dp_0", first_b, more_b, part_b, boxes_b[1], boxes_b[3])
    for k in range(2):
        part_d[k] = upper[64 * k : 64 * k + 64]
        part_d[2 + k] = lower[64 * k : 64 * k + 64]
    first_d = ring_start("dp_1", part_d, boxes_d[0], boxes_d[1], send.at[3], recv.at[3])
    more_c = ring_relay(
        "dp_0", first_c, part_c, boxes_c[0], boxes_c[2], boxes_c[3], send.at[2], recv.at[2]
    )
    more_d = ring_relay(
        "dp_1", first_d, part_d, boxes_d[0], boxes_d[2], boxes_d[3], send.at[3], recv.at[3]
    )
    z_copies = []
    for k, (axis, first, more, part, boxes) in enumerate(
        [
            ("dp_0", first_c, more_c, part_c, boxes_c),
            ("dp_1", first_d, more_d, part_d, boxes_d),
        ]
    ):
        upper, lower = ring_finish(axis, first, more, part, boxes[1], boxes[3])
        last[k, 0] = upper
        last[k, 1] = lower
        c = remote(
            last.at[k, 1 - z], last_in.at[k], z_send.at[k], z_recv.at[k], "dp_2", 1 - z
        )
        c.start()
        z_copies.append(c)
    for k, c in enumerate(z_copies):
        c.wait_recv()
        out[:, k * HALF : (k + 1) * HALF] = last[k, z] + last_in[k]
    for c in [*pair, *z_copies]:
        c.wait_send()


def reduce_gradients(shaped, d_proj, packed):
    core = lax.axis_index("dp_3")

    def split(values):
        rows = values.T.reshape(ROWS // 32, 2, 32, SEQ)
        own = lax.dynamic_index_in_dim(rows, core, 1, keepdims=False)
        other = lax.dynamic_index_in_dim(rows, 1 - core, 1, keepdims=False)
        return own.reshape(ROWS, SEQ), other.reshape(ROWS, SEQ)

    shaped_own, shaped_other = split(shaped)
    proj_own, proj_other = split(d_proj)
    vmem = pl.BlockSpec(memory_space=pltpu.VMEM)
    wire = jnp.float32

    def boxes(half):
        return [pltpu.VMEM((2, half, HALF), wire)] * 4

    return pl.pallas_call(
        reduce_kernel,
        out_shape=jax.ShapeDtypeStruct((32, 2 * HALF), jnp.float32),
        in_specs=[vmem] * 5,
        out_specs=vmem,
        scratch_shapes=[
            pltpu.VMEM((ROWS, SEQ), jnp.bfloat16),
            pltpu.VMEM((ROWS, SEQ), jnp.bfloat16),
            pltpu.VMEM((SEQ, 2 * HALF), jnp.bfloat16),
            pltpu.VMEM((4, 256, HALF), jnp.float32),
            pltpu.VMEM((4, 256, HALF), jnp.float32),
            pltpu.VMEM((4, 64, HALF), jnp.float32),
            pltpu.VMEM((4, 64, HALF), jnp.float32),
            *boxes(128),
            *boxes(128),
            *boxes(32),
            *boxes(32),
            pltpu.VMEM((2, 2, 32, HALF), jnp.float32),
            pltpu.VMEM((2, 32, HALF), jnp.float32),
            pltpu.SemaphoreType.DMA((3,)),
            pltpu.SemaphoreType.DMA((3,)),
            pltpu.SemaphoreType.DMA((4, 6)),
            pltpu.SemaphoreType.DMA((4, 6)),
            pltpu.SemaphoreType.DMA((2,)),
            pltpu.SemaphoreType.DMA((2,)),
        ],
        compiler_params=pltpu.CompilerParams(
            collective_id=1, has_side_effects=True, vmem_limit_bytes=60 * 2**20
        ),
    )(shaped_own, shaped_other, proj_own, proj_other, packed)


def swapped(values):
    return lax.ppermute(values, "mp", [(0, 1), (1, 0)])


def plan():
    grid = jnp.arange(TGRID + 1, dtype=jnp.float32)
    lamb = 6.0 - 12.0 * grid / TGRID
    return (jnp.sqrt(jax.nn.sigmoid(lamb)), jnp.sqrt(jax.nn.sigmoid(-lamb)))


def positions():
    index = jnp.arange(SEQ, dtype=jnp.float32)[:, None]
    half = D // 2
    freqs = jnp.exp(-math.log(10000.0) * jnp.arange(half, dtype=jnp.float32) / half)
    angles = index * freqs[None, :]
    return jnp.concatenate([jnp.sin(angles), jnp.cos(angles)], axis=1)


def normalize(values):
    center = values - jnp.mean(values, axis=-1, keepdims=True)
    inverse = lax.rsqrt(jnp.mean(center * center, axis=-1, keepdims=True) + LN_EPS)
    return (center * inverse, inverse)


def norm_back(upstream, normed, inverse):
    first_mean = jnp.mean(upstream, axis=-1, keepdims=True)
    second_mean = jnp.mean(upstream * normed, axis=-1, keepdims=True)
    return (upstream - first_mean - normed * second_mean) * inverse


def one_hot_rows(index, width):
    return (index[:, None] == jnp.arange(width, dtype=jnp.int32)[None, :]).astype(jnp.float32)


def per_device(
    clean_latent,
    noise_draw,
    timestep,
    bucket,
    bucket_weights,
    teacher_embed,
    teacher_final,
    teacher_mod,
    teacher_qkv,
    teacher_out,
    student_embed,
    student_final,
    student_mod,
    student_qkv,
    student_out,
    moment_qkv,
    second_qkv,
    moment_out,
    second_out,
):
    samples = clean_latent.shape[0]
    rows_all = samples * SEQ
    local_inner = teacher_out.shape[1]
    local_heads = local_inner // HS
    alphas, sigmas = plan()
    table = jnp.stack([alphas, sigmas], axis=1)

    def coefficients(tau):
        picked = jnp.dot(one_hot_rows(tau, TGRID + 1), table, precision=lax.Precision.HIGHEST)
        picked = jnp.repeat(picked, SEQ, axis=0)
        return (picked[:, 0:1], picked[:, 1:2])

    def modulation(mod_table, index, length):
        picked = jnp.dot(
            one_hot_rows(index, length),
            mod_table.reshape(length, 3 * D),
            precision=lax.Precision.HIGHEST,
        )
        return picked.reshape(samples, 3, D)

    def gate_rows(modrows):
        return jnp.repeat(modrows[:, 2], SEQ, axis=0)

    placed = positions()

    def front(latent, modrows, embed, w_qkv, w_out, other_out):
        hidden = (
            jnp.dot(latent, embed, precision=lax.Precision.HIGHEST).reshape(samples, SEQ, D)
            + placed[None]
        )
        normed, unused = normalize(hidden)
        shaped = (
            (normed * (1.0 + modrows[:, None, 1]) + modrows[:, None, 0])
            .astype(jnp.bfloat16)
            .reshape(rows_all, D)
        )
        hidden = hidden.reshape(rows_all, D)
        packed = jnp.dot(
            shaped, w_qkv.reshape(D, 3 * local_inner), preferred_element_type=jnp.float32
        )
        packed = packed.astype(jnp.bfloat16).reshape(samples, SEQ, 3, local_heads, HS)
        queries = packed[:, :, 0]
        keys_all = packed[:, :, 1]
        values = packed[:, :, 2]
        scores = jnp.einsum(
            "sqhd,skhd->shqk", queries, keys_all, preferred_element_type=jnp.float32
        ) / math.sqrt(HS)
        highest = jnp.max(scores, axis=-1, keepdims=True)
        expos = jnp.exp(scores - highest)
        weights = expos / jnp.sum(expos, axis=-1, keepdims=True)
        rounded = weights.astype(jnp.bfloat16)
        attended = jnp.einsum(
            "shqk,skhd->sqhd", rounded, values, preferred_element_type=jnp.float32
        )
        attended = attended.astype(jnp.bfloat16).reshape(rows_all, local_inner)
        contract = (((1,), (1,)), ((), ()))
        projected = lax.dot_general(
            attended, w_out, contract, preferred_element_type=jnp.float32
        ) + lax.dot_general(
            swapped(attended), other_out, contract, preferred_element_type=jnp.float32
        )
        return (hidden, shaped, queries, keys_all, values, weights, rounded, attended, projected)

    def tail(hidden, modrows, projected, final):
        mixed = hidden + gate_rows(modrows) * projected
        normed, inverse = normalize(mixed)
        predicted = lax.dot_general(
            normed, final, (((1,), (1,)), ((), ())), precision=lax.Precision.HIGHEST
        )
        return (predicted, normed, inverse)

    def teacher_eps(latent, modrows):
        parts = front(latent, modrows, teacher_embed, teacher_qkv, teacher_out, teacher_other)
        return tail(parts[0], modrows, parts[8], teacher_final)[0]

    teacher_other = swapped(teacher_out)
    flat = jnp.concatenate(
        [student_qkv.reshape(-1, 3 * local_inner), student_out, swapped(student_out)], axis=1
    )
    whole = lax.all_gather(flat, DP, axis=0, tiled=True)
    whole_qkv = whole[:, : 3 * local_inner]
    whole_out = whole[:, 3 * local_inner : 4 * local_inner]
    whole_other = whole[:, 4 * local_inner :]
    first = 2 * timestep
    middle = first - 1
    last = first - 2
    a_first, s_first = coefficients(first)
    a_middle, s_middle = coefficients(middle)
    a_last, s_last = coefficients(last)
    clean_rows = clean_latent.reshape(rows_all, PATCH_CH)
    noise_rows = noise_draw.reshape(rows_all, PATCH_CH)
    latent0 = a_first * clean_rows + s_first * noise_rows
    eps_zero = teacher_eps(latent0, modulation(teacher_mod, first - 1, TGRID))
    latent1 = a_middle * (latent0 - s_first * eps_zero) / a_first + s_middle * eps_zero
    eps_one = teacher_eps(latent1, modulation(teacher_mod, middle - 1, TGRID))
    latent2 = a_last * (latent1 - s_middle * eps_one) / a_middle + s_last * eps_one
    target = (latent0 - a_first / a_last * latent2) / (s_first - a_first * s_last / a_last)
    student_rows_mod = modulation(student_mod, timestep - 1, K)
    hidden, shaped, queries, keys_all, values, weights, rounded, attended, projected = front(
        latent0, student_rows_mod, student_embed, whole_qkv, whole_out, whole_other
    )
    predicted, normed, inverse = tail(hidden, student_rows_mod, projected, student_final)
    sample_weight = jnp.dot(
        one_hot_rows(bucket, NBUCKET), bucket_weights, precision=lax.Precision.HIGHEST
    )
    row_weight = jnp.repeat(sample_weight, SEQ, axis=0)[:, None]
    error = predicted - target
    loss_part = jnp.sum(row_weight * error * error)
    d_pred = 2.0 * row_weight * error
    d_normed = jnp.dot(d_pred, student_final, precision=lax.Precision.HIGHEST)
    d_mixed = norm_back(d_normed, normed, inverse)
    d_proj = (gate_rows(student_rows_mod) * d_mixed).astype(jnp.bfloat16)
    d_attn = jnp.dot(d_proj, whole_out, preferred_element_type=jnp.float32).astype(jnp.bfloat16)
    d_attn = d_attn.reshape(samples, SEQ, local_heads, HS)
    d_prob = jnp.einsum("sqhd,skhd->shqk", d_attn, values, preferred_element_type=jnp.float32)
    d_score = (
        weights * (d_prob - jnp.sum(weights * d_prob, axis=-1, keepdims=True)) / math.sqrt(HS)
    ).astype(jnp.bfloat16)
    d_query = jnp.einsum(
        "shqk,skhd->sqhd", d_score, keys_all, preferred_element_type=jnp.float32
    ).astype(jnp.bfloat16)
    d_key = jnp.einsum(
        "shqk,sqhd->skhd", d_score, queries, preferred_element_type=jnp.float32
    ).astype(jnp.bfloat16)
    d_value = jnp.einsum(
        "shqk,sqhd->skhd", rounded, d_attn, preferred_element_type=jnp.float32
    ).astype(jnp.bfloat16)
    packed = jnp.concatenate(
        [v.reshape(rows_all, local_inner) for v in (d_query, d_key, d_value, attended)], axis=1
    )
    grads = reduce_gradients(shaped, d_proj, packed)
    grad_qkv = grads[:, : 3 * local_inner].reshape(-1, 3, local_inner)
    grad_out = grads[:, 3 * local_inner :]
    squares, loss_sum = lax.psum(
        jnp.stack([jnp.sum(grads * grads), loss_part / lax.axis_size("mp")]), DP_MP
    )
    rms_value = jnp.sqrt(squares / (4 * D * INNER))
    factor = 1.0 / jnp.maximum(rms_value, 1.0)

    def adam(moment, second, grad):
        normed_grad = grad * factor
        new_moment = BETA_ONE * moment + (1.0 - BETA_ONE) * normed_grad
        new_second = BETA_TWO * second + (1.0 - BETA_TWO) * normed_grad * normed_grad
        return (new_moment, new_second, new_moment / (jnp.sqrt(new_second) + ADAM_EPS))

    mq, vq, uq = adam(moment_qkv, second_qkv, grad_qkv)
    mo, vo, uo = adam(moment_out, second_out, grad_out)
    loss = loss_sum / (samples * lax.axis_size(DP) * LATENT)
    return (mq, vq, uq, mo, vo, uo, loss)


def solution(mesh):
    torus = Mesh(
        mesh.devices.reshape(4, 4, 2, 2, mesh.shape["mp"]), ("dp_0", "dp_1", "dp_2", "dp_3", "mp")
    )
    in_specs = (
        P(DP, None),
        P(DP, None),
        P(DP),
        P(DP),
        P(),
        P(),
        P(),
        P(),
        P(None, None, "mp"),
        P(None, "mp"),
        P(),
        P(),
        P(),
        P(DP, None, "mp"),
        P(DP, "mp"),
        P(DP, None, "mp"),
        P(DP, None, "mp"),
        P(DP, "mp"),
        P(DP, "mp"),
    )
    out_specs = (
        P(DP, None, "mp"),
        P(DP, None, "mp"),
        P(DP, None, "mp"),
        P(DP, "mp"),
        P(DP, "mp"),
        P(DP, "mp"),
        P(),
    )
    return jax.shard_map(
        per_device, mesh=torus, in_specs=in_specs, out_specs=out_specs, check_vma=False
    )
```

```python
import math

import jax
import jax.numpy as jnp
from jax import lax
from jax.experimental import pallas as pl
from jax.experimental.pallas import tpu as pltpu
from jax.sharding import Mesh
from jax.sharding import PartitionSpec as P

D = 2048
HS = 64
INNER = 1024
PATCH_CH = 16
SEQ = 256
LATENT = 4096
K = 8
TGRID = 16
NBUCKET = 8
DP = ("dp_0", "dp_1", "dp_2", "dp_3")
DP_MP = ("dp_0", "dp_1", "dp_2", "dp_3", "mp")


LN_EPS = 0.01
BETA_ONE = 0.9
BETA_TWO = 0.99
ADAM_EPS = 1e-08


ROWS = 1024
HALF = 1024
AXES = ("dp_0", "dp_1", "dp_2", "dp_3", "mp")


def remote(src, dst, send, recv, axis, target):
    return pltpu.make_async_remote_copy(
        src_ref=src,
        dst_ref=dst,
        send_sem=send,
        recv_sem=recv,
        device_id={axis: target} if isinstance(axis, str) else dict(zip(axis, target)),
        device_id_type=pl.DeviceIdType.MESH,
    )


def greet(friends):
    barrier = pltpu.get_barrier_semaphore()
    for axis, target in friends:
        pl.semaphore_signal(
            barrier,
            inc=1,
            device_id={axis: target} if isinstance(axis, str) else dict(zip(axis, target)),
            device_id_type=pl.DeviceIdType.MESH,
        )
    pl.semaphore_wait(barrier, len(friends))


def all_places():
    y, x, z, core, mp = (lax.axis_index(a) for a in AXES)
    return [
        (core, [("dp_3", 1 - core)]),
        (2 * mp + z, [("dp_2", 1 - z), ("mp", 1 - mp), (("dp_2", "mp"), (1 - z, 1 - mp))]),
        (x, [("dp_1", lax.rem(x + k, 4)) for k in (1, 2, 3)]),
        (y, [("dp_0", lax.rem(y + k, 4)) for k in (1, 2, 3)]),
    ]


def sum_over_all(value, inbox, send, recv):
    for stage, (slot, partners) in enumerate(all_places()):
        inbox[stage, slot] = value
        copies = [
            remote(
                inbox.at[stage, slot],
                inbox.at[stage, slot],
                send.at[stage, k],
                recv.at[stage, k],
                axis,
                target,
            )
            for k, (axis, target) in enumerate(partners)
        ]
        for c in copies:
            c.start()
        for c in copies:
            c.wait_recv()
        value = inbox[stage, 0]
        for k in range(1, len(partners) + 1):
            value = value + inbox[stage, k]
        for c in copies:
            c.wait_send()
    return value


def ring_start(axis, part, relay, direct, send, recv):
    me = lax.axis_index(axis)
    right, left, far = (lax.rem(me + k, 4) for k in (1, 3, 2))
    half = part.shape[1] // 2
    top, low = pl.ds(0, half), pl.ds(half, half)
    copies = [
        remote(part.at[far, top], relay.at[0], send.at[0], recv.at[0], axis, right),
        remote(part.at[far, low], relay.at[1], send.at[1], recv.at[1], axis, left),
        remote(part.at[right, low], direct.at[0], send.at[2], recv.at[2], axis, right),
        remote(part.at[left, top], direct.at[1], send.at[3], recv.at[3], axis, left),
    ]
    for c in copies:
        c.start()
    return copies


def ring_relay(axis, copies, part, relay, passed, summed, send, recv):
    me = lax.axis_index(axis)
    right, left = (lax.rem(me + k, 4) for k in (1, 3))
    half = part.shape[1] // 2
    top, low = pl.ds(0, half), pl.ds(half, half)
    copies[0].wait_recv()
    passed[0] = relay[0] + part[right, top]
    first = remote(passed.at[0], summed.at[0], send.at[4], recv.at[4], axis, right)
    first.start()
    copies[1].wait_recv()
    passed[1] = relay[1] + part[left, low]
    second = remote(passed.at[1], summed.at[1], send.at[5], recv.at[5], axis, left)
    second.start()
    return [first, second]


def ring_finish(axis, copies, more, part, direct, summed):
    me = lax.axis_index(axis)
    half = part.shape[1] // 2
    copies[3].wait_recv()
    more[0].wait_recv()
    upper = part[me, pl.ds(0, half)] + direct[1] + summed[0]
    copies[2].wait_recv()
    more[1].wait_recv()
    lower = part[me, pl.ds(half, half)] + direct[0] + summed[1]
    for c in [*copies, *more]:
        c.wait_send()
    return upper, lower


def reduce_kernel(
    shaped_own,
    shaped_other,
    proj_own,
    proj_other,
    packed,
    loss_part,
    out,
    totals,
    shaped_in,
    proj_in,
    packed_in,
    part_a,
    part_b,
    part_c,
    part_d,
    *rest,
):
    boxes_a, boxes_b, boxes_c, boxes_d = rest[0:4], rest[4:8], rest[8:12], rest[12:16]
    last, last_in, pair_send, pair_recv, send, recv, z_send, z_recv = rest[16:24]
    inbox, sum_send, sum_recv = rest[24:]
    y, x, z, core = (lax.axis_index(a) for a in AXES[:4])
    greet([friend for _, partners in all_places() for friend in partners])
    pair = [
        remote(a, b, pair_send.at[k], pair_recv.at[k], "dp_3", 1 - core)
        for k, (a, b) in enumerate(
            [(packed, packed_in), (shaped_other, shaped_in), (proj_other, proj_in)]
        )
    ]
    for c in pair:
        c.start()

    def products(s_ref, p_ref, b_ref, add):
        def step(k, carry):
            rows = pl.ds(pl.multiple_of(k * 256, 256), 256)
            s, p = s_ref[rows], p_ref[rows]
            g = jnp.dot(s, b_ref[:, :HALF], preferred_element_type=jnp.float32)
            for j in range(4):
                block = g[64 * j : 64 * j + 64]
                spot = pl.ds(pl.multiple_of(k * 64, 64), 64)
                part_a[j, spot] = part_a[j, spot] + block if add else block
            h = jnp.dot(s, b_ref[:, HALF : HALF + 512], preferred_element_type=jnp.float32)
            part_b[k, :, 0:512] = part_b[k, :, 0:512] + h if add else h
            o = jnp.dot(p, b_ref[:, HALF + 512 :], preferred_element_type=jnp.float32)
            part_b[k, :, 512:1024] = part_b[k, :, 512:1024] + o if add else o
            return carry

        lax.fori_loop(0, 4, step, 0)

    products(shaped_own, proj_own, packed, False)
    for c in pair:
        c.wait_recv()
    products(shaped_in, proj_in, packed_in, True)

    first_a = ring_start("dp_1", part_a, boxes_a[0], boxes_a[1], send.at[0], recv.at[0])
    first_b = ring_start("dp_0", part_b, boxes_b[0], boxes_b[1], send.at[1], recv.at[1])
    more_a = ring_relay(
        "dp_1", first_a, part_a, boxes_a[0], boxes_a[2], boxes_a[3], send.at[0], recv.at[0]
    )
    more_b = ring_relay(
        "dp_0", first_b, part_b, boxes_b[0], boxes_b[2], boxes_b[3], send.at[1], recv.at[1]
    )
    upper, lower = ring_finish("dp_1", first_a, more_a, part_a, boxes_a[1], boxes_a[3])
    for k in range(2):
        part_c[k] = upper[64 * k : 64 * k + 64]
        part_c[2 + k] = lower[64 * k : 64 * k + 64]
    first_c = ring_start("dp_0", part_c, boxes_c[0], boxes_c[1], send.at[2], recv.at[2])
    upper, lower = ring_finish("dp_0", first_b, more_b, part_b, boxes_b[1], boxes_b[3])
    for k in range(2):
        part_d[k] = upper[64 * k : 64 * k + 64]
        part_d[2 + k] = lower[64 * k : 64 * k + 64]
    first_d = ring_start("dp_1", part_d, boxes_d[0], boxes_d[1], send.at[3], recv.at[3])
    more_c = ring_relay(
        "dp_0", first_c, part_c, boxes_c[0], boxes_c[2], boxes_c[3], send.at[2], recv.at[2]
    )
    more_d = ring_relay(
        "dp_1", first_d, part_d, boxes_d[0], boxes_d[2], boxes_d[3], send.at[3], recv.at[3]
    )
    z_copies = []
    for k, (axis, first, more, part, boxes) in enumerate(
        [
            ("dp_0", first_c, more_c, part_c, boxes_c),
            ("dp_1", first_d, more_d, part_d, boxes_d),
        ]
    ):
        upper, lower = ring_finish(axis, first, more, part, boxes[1], boxes[3])
        last[k, 0] = upper
        last[k, 1] = lower
        c = remote(
            last.at[k, 1 - z], last_in.at[k], z_send.at[k], z_recv.at[k], "dp_2", 1 - z
        )
        c.start()
        z_copies.append(c)
    for k, c in enumerate(z_copies):
        c.wait_recv()
        both = last[k, z] + last_in[k]
        out[2 * k] = both[:, :512]
        out[2 * k + 1] = both[:, 512:]
    for c in [*pair, *z_copies]:
        c.wait_send()
    squares = jnp.sum(out[...] * out[...])
    row = lax.broadcasted_iota(jnp.int32, (8, 128), 0)
    value = jnp.where(row == 0, squares, loss_part[...])
    totals[...] = sum_over_all(value, inbox, sum_send, sum_recv)


def reduce_gradients(shaped, d_proj, packed, loss_part):
    core = lax.axis_index("dp_3")

    def split(values):
        rows = values.T.reshape(ROWS // 32, 2, 32, SEQ)
        own = lax.dynamic_index_in_dim(rows, core, 1, keepdims=False)
        other = lax.dynamic_index_in_dim(rows, 1 - core, 1, keepdims=False)
        return own.reshape(ROWS, SEQ), other.reshape(ROWS, SEQ)

    shaped_own, shaped_other = split(shaped)
    proj_own, proj_other = split(d_proj)
    vmem = pl.BlockSpec(memory_space=pltpu.VMEM)
    wire = jnp.float32

    def boxes(half):
        return [pltpu.VMEM((2, half, HALF), wire)] * 4

    return pl.pallas_call(
        reduce_kernel,
        out_shape=(
            jax.ShapeDtypeStruct((4, 32, 512), jnp.float32),
            jax.ShapeDtypeStruct((8, 128), jnp.float32),
        ),
        in_specs=[vmem] * 6,
        out_specs=(vmem, vmem),
        scratch_shapes=[
            pltpu.VMEM((ROWS, SEQ), jnp.bfloat16),
            pltpu.VMEM((ROWS, SEQ), jnp.bfloat16),
            pltpu.VMEM((SEQ, 2 * HALF), jnp.bfloat16),
            pltpu.VMEM((4, 256, HALF), jnp.float32),
            pltpu.VMEM((4, 256, HALF), jnp.float32),
            pltpu.VMEM((4, 64, HALF), jnp.float32),
            pltpu.VMEM((4, 64, HALF), jnp.float32),
            *boxes(128),
            *boxes(128),
            *boxes(32),
            *boxes(32),
            pltpu.VMEM((2, 2, 32, HALF), jnp.float32),
            pltpu.VMEM((2, 32, HALF), jnp.float32),
            pltpu.SemaphoreType.DMA((3,)),
            pltpu.SemaphoreType.DMA((3,)),
            pltpu.SemaphoreType.DMA((4, 6)),
            pltpu.SemaphoreType.DMA((4, 6)),
            pltpu.SemaphoreType.DMA((2,)),
            pltpu.SemaphoreType.DMA((2,)),
            pltpu.VMEM((4, 4, 8, 128), jnp.float32),
            pltpu.SemaphoreType.DMA((4, 3)),
            pltpu.SemaphoreType.DMA((4, 3)),
        ],
        compiler_params=pltpu.CompilerParams(
            collective_id=1, has_side_effects=True, vmem_limit_bytes=60 * 2**20
        ),
    )(shaped_own, shaped_other, proj_own, proj_other, packed, loss_part)


def swapped(values):
    return lax.ppermute(values, "mp", [(0, 1), (1, 0)])


def plan():
    grid = jnp.arange(TGRID + 1, dtype=jnp.float32)
    lamb = 6.0 - 12.0 * grid / TGRID
    return (jnp.sqrt(jax.nn.sigmoid(lamb)), jnp.sqrt(jax.nn.sigmoid(-lamb)))


def positions():
    index = jnp.arange(SEQ, dtype=jnp.float32)[:, None]
    half = D // 2
    freqs = jnp.exp(-math.log(10000.0) * jnp.arange(half, dtype=jnp.float32) / half)
    angles = index * freqs[None, :]
    return jnp.concatenate([jnp.sin(angles), jnp.cos(angles)], axis=1)


def normalize(values):
    center = values - jnp.mean(values, axis=-1, keepdims=True)
    inverse = lax.rsqrt(jnp.mean(center * center, axis=-1, keepdims=True) + LN_EPS)
    return (center * inverse, inverse)


def norm_back(upstream, normed, inverse):
    first_mean = jnp.mean(upstream, axis=-1, keepdims=True)
    second_mean = jnp.mean(upstream * normed, axis=-1, keepdims=True)
    return (upstream - first_mean - normed * second_mean) * inverse


def one_hot_rows(index, width):
    return (index[:, None] == jnp.arange(width, dtype=jnp.int32)[None, :]).astype(jnp.float32)


def per_device(
    clean_latent,
    noise_draw,
    timestep,
    bucket,
    bucket_weights,
    teacher_embed,
    teacher_final,
    teacher_mod,
    teacher_qkv,
    teacher_out,
    student_embed,
    student_final,
    student_mod,
    student_qkv,
    student_out,
    moment_qkv,
    second_qkv,
    moment_out,
    second_out,
):
    samples = clean_latent.shape[0]
    rows_all = samples * SEQ
    local_inner = teacher_out.shape[1]
    local_heads = local_inner // HS
    alphas, sigmas = plan()
    table = jnp.stack([alphas, sigmas], axis=1)

    def coefficients(tau):
        picked = jnp.dot(one_hot_rows(tau, TGRID + 1), table, precision=lax.Precision.HIGHEST)
        picked = jnp.repeat(picked, SEQ, axis=0)
        return (picked[:, 0:1], picked[:, 1:2])

    def modulation(mod_table, index, length):
        picked = jnp.dot(
            one_hot_rows(index, length),
            mod_table.reshape(length, 3 * D),
            precision=lax.Precision.HIGHEST,
        )
        return picked.reshape(samples, 3, D)

    def gate_rows(modrows):
        return jnp.repeat(modrows[:, 2], SEQ, axis=0)

    placed = positions()

    def front(latent, modrows, embed, w_qkv, w_out, other_out):
        hidden = (
            jnp.dot(latent, embed, precision=lax.Precision.HIGHEST).reshape(samples, SEQ, D)
            + placed[None]
        )
        normed, unused = normalize(hidden)
        shaped = (
            (normed * (1.0 + modrows[:, None, 1]) + modrows[:, None, 0])
            .astype(jnp.bfloat16)
            .reshape(rows_all, D)
        )
        hidden = hidden.reshape(rows_all, D)
        packed = jnp.dot(
            shaped, w_qkv.reshape(D, 3 * local_inner), preferred_element_type=jnp.float32
        )
        packed = packed.astype(jnp.bfloat16).reshape(samples, SEQ, 3, local_heads, HS)
        queries = packed[:, :, 0]
        keys_all = packed[:, :, 1]
        values = packed[:, :, 2]
        scores = jnp.einsum(
            "sqhd,skhd->shqk", queries, keys_all, preferred_element_type=jnp.float32
        ) / math.sqrt(HS)
        highest = jnp.max(scores, axis=-1, keepdims=True)
        expos = jnp.exp(scores - highest)
        weights = expos / jnp.sum(expos, axis=-1, keepdims=True)
        rounded = weights.astype(jnp.bfloat16)
        attended = jnp.einsum(
            "shqk,skhd->sqhd", rounded, values, preferred_element_type=jnp.float32
        )
        attended = attended.astype(jnp.bfloat16).reshape(rows_all, local_inner)
        contract = (((1,), (1,)), ((), ()))
        projected = lax.dot_general(
            attended, w_out, contract, preferred_element_type=jnp.float32
        ) + lax.dot_general(
            swapped(attended), other_out, contract, preferred_element_type=jnp.float32
        )
        return (hidden, shaped, queries, keys_all, values, weights, rounded, attended, projected)

    def tail(hidden, modrows, projected, final):
        mixed = hidden + gate_rows(modrows) * projected
        normed, inverse = normalize(mixed)
        predicted = lax.dot_general(
            normed, final, (((1,), (1,)), ((), ())), precision=lax.Precision.HIGHEST
        )
        return (predicted, normed, inverse)

    def teacher_eps(latent, modrows):
        parts = front(latent, modrows, teacher_embed, teacher_qkv, teacher_out, teacher_other)
        return tail(parts[0], modrows, parts[8], teacher_final)[0]

    teacher_other = swapped(teacher_out)
    flat = jnp.concatenate(
        [student_qkv.reshape(-1, 3 * local_inner), student_out, swapped(student_out)], axis=1
    )
    whole = lax.all_gather(flat, DP, axis=0, tiled=True)
    whole_qkv = whole[:, : 3 * local_inner]
    whole_out = whole[:, 3 * local_inner : 4 * local_inner]
    whole_other = whole[:, 4 * local_inner :]
    first = 2 * timestep
    middle = first - 1
    last = first - 2
    a_first, s_first = coefficients(first)
    a_middle, s_middle = coefficients(middle)
    a_last, s_last = coefficients(last)
    clean_rows = clean_latent.reshape(rows_all, PATCH_CH)
    noise_rows = noise_draw.reshape(rows_all, PATCH_CH)
    latent0 = a_first * clean_rows + s_first * noise_rows
    eps_zero = teacher_eps(latent0, modulation(teacher_mod, first - 1, TGRID))
    latent1 = a_middle * (latent0 - s_first * eps_zero) / a_first + s_middle * eps_zero
    eps_one = teacher_eps(latent1, modulation(teacher_mod, middle - 1, TGRID))
    latent2 = a_last * (latent1 - s_middle * eps_one) / a_middle + s_last * eps_one
    target = (latent0 - a_first / a_last * latent2) / (s_first - a_first * s_last / a_last)
    student_rows_mod = modulation(student_mod, timestep - 1, K)
    hidden, shaped, queries, keys_all, values, weights, rounded, attended, projected = front(
        latent0, student_rows_mod, student_embed, whole_qkv, whole_out, whole_other
    )
    predicted, normed, inverse = tail(hidden, student_rows_mod, projected, student_final)
    sample_weight = jnp.dot(
        one_hot_rows(bucket, NBUCKET), bucket_weights, precision=lax.Precision.HIGHEST
    )
    row_weight = jnp.repeat(sample_weight, SEQ, axis=0)[:, None]
    error = predicted - target
    loss_part = jnp.sum(row_weight * error * error)
    d_pred = 2.0 * row_weight * error
    d_normed = jnp.dot(d_pred, student_final, precision=lax.Precision.HIGHEST)
    d_mixed = norm_back(d_normed, normed, inverse)
    d_proj = (gate_rows(student_rows_mod) * d_mixed).astype(jnp.bfloat16)
    d_attn = jnp.dot(d_proj, whole_out, preferred_element_type=jnp.float32).astype(jnp.bfloat16)
    d_attn = d_attn.reshape(samples, SEQ, local_heads, HS)
    d_prob = jnp.einsum("sqhd,skhd->shqk", d_attn, values, preferred_element_type=jnp.float32)
    d_score = (
        weights * (d_prob - jnp.sum(weights * d_prob, axis=-1, keepdims=True)) / math.sqrt(HS)
    ).astype(jnp.bfloat16)
    d_query = jnp.einsum(
        "shqk,skhd->sqhd", d_score, keys_all, preferred_element_type=jnp.float32
    ).astype(jnp.bfloat16)
    d_key = jnp.einsum(
        "shqk,sqhd->skhd", d_score, queries, preferred_element_type=jnp.float32
    ).astype(jnp.bfloat16)
    d_value = jnp.einsum(
        "shqk,sqhd->skhd", rounded, d_attn, preferred_element_type=jnp.float32
    ).astype(jnp.bfloat16)
    packed = jnp.concatenate(
        [v.reshape(rows_all, local_inner) for v in (d_query, d_key, d_value, attended)], axis=1
    )
    grads, totals = reduce_gradients(
        shaped, d_proj, packed, jnp.full((8, 128), loss_part / lax.axis_size("mp"))
    )
    grad_qkv = jnp.moveaxis(grads[:3], 0, 1)
    grad_out = grads[3]
    squares, loss_sum = totals[0, 0], totals[1, 0]
    rms_value = jnp.sqrt(squares / (4 * D * INNER))
    factor = 1.0 / jnp.maximum(rms_value, 1.0)

    def adam(moment, second, grad):
        normed_grad = grad * factor
        new_moment = BETA_ONE * moment + (1.0 - BETA_ONE) * normed_grad
        new_second = BETA_TWO * second + (1.0 - BETA_TWO) * normed_grad * normed_grad
        return (new_moment, new_second, new_moment / (jnp.sqrt(new_second) + ADAM_EPS))

    mq, vq, uq = adam(moment_qkv, second_qkv, grad_qkv)
    mo, vo, uo = adam(moment_out, second_out, grad_out)
    loss = loss_sum / (samples * lax.axis_size(DP) * LATENT)
    return (mq, vq, uq, mo, vo, uo, loss)


def solution(mesh):
    torus = Mesh(
        mesh.devices.reshape(4, 4, 2, 2, mesh.shape["mp"]), ("dp_0", "dp_1", "dp_2", "dp_3", "mp")
    )
    in_specs = (
        P(DP, None),
        P(DP, None),
        P(DP),
        P(DP),
        P(),
        P(),
        P(),
        P(),
        P(None, None, "mp"),
        P(None, "mp"),
        P(),
        P(),
        P(),
        P(DP, None, "mp"),
        P(DP, "mp"),
        P(DP, None, "mp"),
        P(DP, None, "mp"),
        P(DP, "mp"),
        P(DP, "mp"),
    )
    out_specs = (
        P(DP, None, "mp"),
        P(DP, None, "mp"),
        P(DP, None, "mp"),
        P(DP, "mp"),
        P(DP, "mp"),
        P(DP, "mp"),
        P(),
    )
    return jax.shard_map(
        per_device, mesh=torus, in_specs=in_specs, out_specs=out_specs, check_vma=False
    )
```

```python
import math

import jax
import jax.numpy as jnp
from jax import lax
from jax.experimental import pallas as pl
from jax.experimental.pallas import tpu as pltpu
from jax.sharding import Mesh
from jax.sharding import PartitionSpec as P

D = 2048
HS = 64
INNER = 1024
PATCH_CH = 16
SEQ = 256
LATENT = 4096
K = 8
TGRID = 16
NBUCKET = 8
DP = ("dp_0", "dp_1", "dp_2", "dp_3")
DP_MP = ("dp_0", "dp_1", "dp_2", "dp_3", "mp")


LN_EPS = 0.01
BETA_ONE = 0.9
BETA_TWO = 0.99
ADAM_EPS = 1e-08


ROWS = 1024
HALF = 1024
AXES = ("dp_0", "dp_1", "dp_2", "dp_3", "mp")


def remote(src, dst, send, recv, axis, target):
    return pltpu.make_async_remote_copy(
        src_ref=src,
        dst_ref=dst,
        send_sem=send,
        recv_sem=recv,
        device_id={axis: target} if isinstance(axis, str) else dict(zip(axis, target)),
        device_id_type=pl.DeviceIdType.MESH,
    )


def greet(friends):
    barrier = pltpu.get_barrier_semaphore()
    for axis, target in friends:
        pl.semaphore_signal(
            barrier,
            inc=1,
            device_id={axis: target} if isinstance(axis, str) else dict(zip(axis, target)),
            device_id_type=pl.DeviceIdType.MESH,
        )
    pl.semaphore_wait(barrier, len(friends))


def all_places():
    y, x, z, core, mp = (lax.axis_index(a) for a in AXES)
    return [
        (core, [("dp_3", 1 - core)]),
        (2 * mp + z, [("dp_2", 1 - z), ("mp", 1 - mp), (("dp_2", "mp"), (1 - z, 1 - mp))]),
        (x, [("dp_1", lax.rem(x + k, 4)) for k in (1, 2, 3)]),
        (y, [("dp_0", lax.rem(y + k, 4)) for k in (1, 2, 3)]),
    ]


def sum_over_all(value, inbox, send, recv):
    for stage, (slot, partners) in enumerate(all_places()):
        inbox[stage, slot] = value
        copies = [
            remote(
                inbox.at[stage, slot],
                inbox.at[stage, slot],
                send.at[stage, k],
                recv.at[stage, k],
                axis,
                target,
            )
            for k, (axis, target) in enumerate(partners)
        ]
        for c in copies:
            c.start()
        for c in copies:
            c.wait_recv()
        value = inbox[stage, 0]
        for k in range(1, len(partners) + 1):
            value = value + inbox[stage, k]
        for c in copies:
            c.wait_send()
    return value


def ring_start(axis, part, relay, direct, send, recv):
    me = lax.axis_index(axis)
    right, left, far = (lax.rem(me + k, 4) for k in (1, 3, 2))
    half = part.shape[1] // 2
    top, low = pl.ds(0, half), pl.ds(half, half)
    copies = [
        remote(part.at[far, top], relay.at[0], send.at[0], recv.at[0], axis, right),
        remote(part.at[far, low], relay.at[1], send.at[1], recv.at[1], axis, left),
        remote(part.at[right, low], direct.at[0], send.at[2], recv.at[2], axis, right),
        remote(part.at[left, top], direct.at[1], send.at[3], recv.at[3], axis, left),
    ]
    for c in copies:
        c.start()
    return copies


def ring_relay(axis, copies, part, relay, passed, summed, send, recv):
    me = lax.axis_index(axis)
    right, left = (lax.rem(me + k, 4) for k in (1, 3))
    half = part.shape[1] // 2
    top, low = pl.ds(0, half), pl.ds(half, half)
    copies[0].wait_recv()
    passed[0] = relay[0] + part[right, top]
    first = remote(passed.at[0], summed.at[0], send.at[4], recv.at[4], axis, right)
    first.start()
    copies[1].wait_recv()
    passed[1] = relay[1] + part[left, low]
    second = remote(passed.at[1], summed.at[1], send.at[5], recv.at[5], axis, left)
    second.start()
    return [first, second]


def ring_finish(axis, copies, more, part, direct, summed):
    me = lax.axis_index(axis)
    half = part.shape[1] // 2
    copies[3].wait_recv()
    more[0].wait_recv()
    upper = part[me, pl.ds(0, half)] + direct[1] + summed[0]
    copies[2].wait_recv()
    more[1].wait_recv()
    lower = part[me, pl.ds(half, half)] + direct[0] + summed[1]
    for c in [*copies, *more]:
        c.wait_send()
    return upper, lower


def reduce_kernel(
    shaped,
    proj,
    packed,
    loss_part,
    out,
    totals,
    shaped_in,
    proj_in,
    packed_in,
    part_a,
    part_b,
    part_c,
    part_d,
    *rest,
):
    boxes_a, boxes_b, boxes_c, boxes_d = rest[0:4], rest[4:8], rest[8:12], rest[12:16]
    last, last_in, pair_send, pair_recv, send, recv, z_send, z_recv = rest[16:24]
    inbox, sum_send, sum_recv = rest[24:]
    y, x, z, core = (lax.axis_index(a) for a in AXES[:4])
    greet([friend for _, partners in all_places() for friend in partners])
    pair = [
        remote(a, b, pair_send.at[k], pair_recv.at[k], "dp_3", 1 - core)
        for k, (a, b) in enumerate(
            [(packed, packed_in), (shaped.at[:, 1 - core], shaped_in), (proj.at[:, 1 - core], proj_in)]
        )
    ]
    for c in pair:
        c.start()

    def products(s_ref, p_ref, b_ref, add):
        def step(k, carry):
            rows = pl.ds(pl.multiple_of(k * 8, 8), 8)
            s, p = (r[rows].reshape(256, SEQ) for r in (s_ref, p_ref))
            g = jnp.dot(s, b_ref[:, :HALF], preferred_element_type=jnp.float32)
            for j in range(4):
                block = g[64 * j : 64 * j + 64]
                spot = pl.ds(pl.multiple_of(k * 64, 64), 64)
                part_a[j, spot] = part_a[j, spot] + block if add else block
            h = jnp.dot(s, b_ref[:, HALF : HALF + 512], preferred_element_type=jnp.float32)
            part_b[k, :, 0:512] = part_b[k, :, 0:512] + h if add else h
            o = jnp.dot(p, b_ref[:, HALF + 512 :], preferred_element_type=jnp.float32)
            part_b[k, :, 512:1024] = part_b[k, :, 512:1024] + o if add else o
            return carry

        lax.fori_loop(0, 4, step, 0)

    products(shaped.at[:, core], proj.at[:, core], packed, False)
    for c in pair:
        c.wait_recv()
    products(shaped_in, proj_in, packed_in, True)

    first_a = ring_start("dp_1", part_a, boxes_a[0], boxes_a[1], send.at[0], recv.at[0])
    first_b = ring_start("dp_0", part_b, boxes_b[0], boxes_b[1], send.at[1], recv.at[1])
    more_a = ring_relay(
        "dp_1", first_a, part_a, boxes_a[0], boxes_a[2], boxes_a[3], send.at[0], recv.at[0]
    )
    more_b = ring_relay(
        "dp_0", first_b, part_b, boxes_b[0], boxes_b[2], boxes_b[3], send.at[1], recv.at[1]
    )
    upper, lower = ring_finish("dp_1", first_a, more_a, part_a, boxes_a[1], boxes_a[3])
    for k in range(2):
        part_c[k] = upper[64 * k : 64 * k + 64]
        part_c[2 + k] = lower[64 * k : 64 * k + 64]
    first_c = ring_start("dp_0", part_c, boxes_c[0], boxes_c[1], send.at[2], recv.at[2])
    upper, lower = ring_finish("dp_0", first_b, more_b, part_b, boxes_b[1], boxes_b[3])
    for k in range(2):
        part_d[k] = upper[64 * k : 64 * k + 64]
        part_d[2 + k] = lower[64 * k : 64 * k + 64]
    first_d = ring_start("dp_1", part_d, boxes_d[0], boxes_d[1], send.at[3], recv.at[3])
    more_c = ring_relay(
        "dp_0", first_c, part_c, boxes_c[0], boxes_c[2], boxes_c[3], send.at[2], recv.at[2]
    )
    more_d = ring_relay(
        "dp_1", first_d, part_d, boxes_d[0], boxes_d[2], boxes_d[3], send.at[3], recv.at[3]
    )
    z_copies = []
    for k, (axis, first, more, part, boxes) in enumerate(
        [
            ("dp_0", first_c, more_c, part_c, boxes_c),
            ("dp_1", first_d, more_d, part_d, boxes_d),
        ]
    ):
        upper, lower = ring_finish(axis, first, more, part, boxes[1], boxes[3])
        last[k, 0] = upper
        last[k, 1] = lower
        c = remote(
            last.at[k, 1 - z], last_in.at[k], z_send.at[k], z_recv.at[k], "dp_2", 1 - z
        )
        c.start()
        z_copies.append(c)
    for k, c in enumerate(z_copies):
        c.wait_recv()
        both = last[k, z] + last_in[k]
        out[2 * k] = both[:, :512]
        out[2 * k + 1] = both[:, 512:]
    for c in [*pair, *z_copies]:
        c.wait_send()
    squares = jnp.sum(out[...] * out[...])
    row = lax.broadcasted_iota(jnp.int32, (8, 128), 0)
    value = jnp.where(row == 0, squares, loss_part[...])
    totals[...] = sum_over_all(value, inbox, sum_send, sum_recv)


def reduce_gradients(shaped, proj, packed, loss_part):
    vmem = pl.BlockSpec(memory_space=pltpu.VMEM)
    wire = jnp.float32

    def boxes(half):
        return [pltpu.VMEM((2, half, HALF), wire)] * 4

    return pl.pallas_call(
        reduce_kernel,
        out_shape=(
            jax.ShapeDtypeStruct((4, 32, 512), jnp.float32),
            jax.ShapeDtypeStruct((8, 128), jnp.float32),
        ),
        in_specs=[vmem] * 4,
        out_specs=(vmem, vmem),
        scratch_shapes=[
            pltpu.VMEM((32, 32, SEQ), jnp.bfloat16),
            pltpu.VMEM((32, 32, SEQ), jnp.bfloat16),
            pltpu.VMEM((SEQ, 2 * HALF), jnp.bfloat16),
            pltpu.VMEM((4, 256, HALF), jnp.float32),
            pltpu.VMEM((4, 256, HALF), jnp.float32),
            pltpu.VMEM((4, 64, HALF), jnp.float32),
            pltpu.VMEM((4, 64, HALF), jnp.float32),
            *boxes(128),
            *boxes(128),
            *boxes(32),
            *boxes(32),
            pltpu.VMEM((2, 2, 32, HALF), jnp.float32),
            pltpu.VMEM((2, 32, HALF), jnp.float32),
            pltpu.SemaphoreType.DMA((3,)),
            pltpu.SemaphoreType.DMA((3,)),
            pltpu.SemaphoreType.DMA((4, 6)),
            pltpu.SemaphoreType.DMA((4, 6)),
            pltpu.SemaphoreType.DMA((2,)),
            pltpu.SemaphoreType.DMA((2,)),
            pltpu.VMEM((4, 4, 8, 128), jnp.float32),
            pltpu.SemaphoreType.DMA((4, 3)),
            pltpu.SemaphoreType.DMA((4, 3)),
        ],
        compiler_params=pltpu.CompilerParams(
            collective_id=1, has_side_effects=True, vmem_limit_bytes=60 * 2**20
        ),
    )(shaped, proj, packed, loss_part)


TOKENS = 256
WIDE = 256
NT = (((1,), (1,)), ((), ()))
TN = (((0,), (0,)), ((), ()))


def dot(a, b, dims=(((1,), (0,)), ((), ()))):
    return lax.dot_general(a, b, dims, preferred_element_type=jnp.float32)


def gather_stream(held, slabs, send, recv):
    y, x, z, core = (lax.axis_index(a) for a in AXES[:4])
    near = {"dp_0": [lax.rem(y + k, 4) for k in (1, 3)], "dp_1": [lax.rem(x + k, 4) for k in (1, 3)]}
    every = slice(None)
    live = []

    def go(spot, k, axis, target):
        ref = held.at[(slabs, *spot)]
        c = remote(ref, ref, send.at[k], recv.at[k], axis, target)
        c.start()
        live.append(c)
        return c

    def ring_direct(first):
        for half, axis in enumerate(("dp_1", "dp_0") if first else ("dp_0", "dp_1")):
            if first:
                spot = (y, x, every, core, half)
            elif half == 0:
                spot = (y, every, every, core, half)
            else:
                spot = (every, x, every, core, half)
            for side in range(2):
                k = (1 if first else 9) + 4 * half + side
                go(spot, k, axis, near[axis][side])

    def ring_relay(first):
        base = 1 if first else 9
        direct = live[-4:]
        for half, axis in enumerate(("dp_1", "dp_0") if first else ("dp_0", "dp_1")):
            for side in range(2):
                direct[2 * half + side].wait_recv()
                back = near[axis][1 - side]
                if first:
                    spot = (y, back) if axis == "dp_1" else (back, x)
                else:
                    spot = (every, back) if axis == "dp_1" else (back, every)
                go((*spot, side, core, half), base + 4 * half + 2 + side, axis, near[axis][side])

    def step(k):
        if k == 0:
            go((y, x, z, core), 0, "dp_2", 1 - z)
        elif k == 1:
            live[-1].wait_recv()
            ring_direct(True)
        elif k == 2:
            ring_relay(True)
        elif k == 3:
            for c in live[-4:]:
                c.wait_recv()
            ring_direct(False)
        elif k == 4:
            ring_relay(False)
        elif k == 5:
            for c in live[-4:]:
                c.wait_recv()
            go((every, every, every, core), 17, "dp_3", 1 - core)
        else:
            live[-1].wait_recv()
            for c in live:
                c.wait_send()

    return step


def three_terms(v8):
    high = v8.astype(jnp.bfloat16).astype(jnp.float32)
    rest = v8 - high
    middle = rest.astype(jnp.bfloat16).astype(jnp.float32)
    low = rest - middle
    group = lax.broadcasted_iota(jnp.int32, v8.shape, 1) // 16
    picked = jnp.where(
        (group == 0) | (group == 1) | (group == 3),
        high,
        jnp.where((group == 2) | (group == 5), middle, jnp.where(group == 4, low, 0.0)),
    )
    return picked.astype(jnp.bfloat16)


def step_kernel(
    coef,
    latent8,
    mods,
    placed,
    teacher_embed,
    teacher_final,
    student_embed,
    student_final,
    student_back,
    teacher_qkv,
    teacher_out,
    student_qkv,
    student_out,
    shaped_t,
    proj_t,
    packed,
    loss_part,
    held,
    near_qkv,
    hidden,
    hidden_s,
    mixed,
    shaped,
    shaped_s,
    qkv,
    heads,
    heads_in,
    weights,
    terms,
    inverses,
    d_attn,
    qkv_sem,
    swap_send,
    swap_recv,
    t_send,
    t_recv,
    s_send,
    s_recv,
):
    y, x, z, core, mp = (lax.axis_index(a) for a in AXES)
    load = pltpu.make_async_copy(teacher_qkv, near_qkv, qkv_sem)
    load.start()
    held[0:3, y, x, z, core] = student_qkv[...]
    held[3, y, x, z, core] = student_out[...]
    friends = [("dp_3", 1 - core), ("dp_2", 1 - z), ("mp", 1 - mp)]
    friends += [("dp_1", lax.rem(x + k, 4)) for k in (1, 3)]
    friends += [("dp_0", lax.rem(y + k, 4)) for k in (1, 3)]
    greet(friends)

    def swap(src, dst, k):
        c = remote(src, dst, swap_send.at[k], swap_recv.at[k], "mp", 1 - mp)
        c.start()
        return c

    spot = (y, x, z, core)
    swaps = [
        swap(teacher_out.at[spot], held.at[(5, *spot)], 0),
        swap(student_out, held.at[(4, *spot)], 1),
    ]
    t_step = gather_stream(held, pl.ds(5, 1), t_send, t_recv)
    s_step = gather_stream(held, pl.ds(0, 5), s_send, s_recv)

    def columns(k, width):
        return pl.ds(pl.multiple_of(k * width, width), width)

    def spread(v8, b_ref, out, base=None):
        terms8 = three_terms(v8)

        def body(n, carry):
            cols = columns(n, WIDE)
            h = dot(terms8, b_ref[:, cols])
            out[:, cols] = h if base is None else h + base[:, cols]
            return carry

        lax.fori_loop(0, D // WIDE, body, 0)

    def shape(hid, which, out):
        def body(n, carry):
            rows = columns(n, 16)
            v = hid[rows]
            c = v - jnp.mean(v, axis=-1, keepdims=True)
            inv = lax.rsqrt(jnp.mean(c * c, axis=-1, keepdims=True) + LN_EPS)
            s = c * inv * (1.0 + mods[which, 1:2]) + mods[which, 0:1]
            out[rows] = s.astype(jnp.bfloat16)
            return carry

        lax.fori_loop(0, TOKENS // 16, body, 0)

    def project(src, weight):
        def body(j, carry):
            qkv[j] = dot(src[...], weight(j)).astype(jnp.bfloat16)
            return carry

        lax.fori_loop(0, 3, body, 0)

    lane = lax.broadcasted_iota(jnp.int32, (1, 128), 1)
    low_f = jnp.where(lane < 64, 1.0, 0.0)
    sides = [low_f.astype(jnp.bfloat16), (1.0 - low_f).astype(jnp.bfloat16)]
    is_low = lax.broadcasted_iota(jnp.int32, (TOKENS, 128), 1) < 64

    def attend(out, keep):
        def body(hp, carry):
            cols = columns(hp, 128)
            q, k, v = qkv[0, :, cols], qkv[1, :, cols], qkv[2, :, cols]
            outs = []
            for h in range(2):
                s = dot(q * sides[h], k, NT) * 0.125
                e = jnp.exp(s - jnp.max(s, axis=-1, keepdims=True))
                w = e / jnp.sum(e, axis=-1, keepdims=True)
                if keep:
                    weights[2 * hp + h] = w
                outs.append(dot(w.astype(jnp.bfloat16), v))
            out[:, cols] = jnp.where(is_low, outs[0], outs[1]).astype(jnp.bfloat16)
            return carry

        lax.fori_loop(0, 4, body, 0)

    def mix(att, weight, which, base):
        def body(n, carry):
            cols = columns(n, 512)
            p = dot(att[...], weight(n), NT)
            mixed[:, cols] = base[:, cols] + mods[which, 2:3, cols] * p
            return carry

        lax.fori_loop(0, 4, body, 0)

    def predict(final, keep):
        def body(n, carry):
            rows = columns(n, 16)
            v = mixed[rows]
            c = v - jnp.mean(v, axis=-1, keepdims=True)
            inv = lax.rsqrt(jnp.mean(c * c, axis=-1, keepdims=True) + LN_EPS)
            u = c * inv
            if keep:
                mixed[rows] = u
                inverses[rows] = jnp.broadcast_to(inv, (16, 128))
            high = u.astype(jnp.bfloat16)
            rest = u - high.astype(jnp.float32)
            middle = rest.astype(jnp.bfloat16)
            terms[0, rows] = high
            terms[1, rows] = middle
            terms[2, rows] = (rest - middle.astype(jnp.float32)).astype(jnp.bfloat16)
            return carry

        lax.fori_loop(0, TOKENS // 16, body, 0)
        r = dot(terms[0], final[...], NT)
        m = dot(terms[1], final[0:256], NT)
        small = dot(terms[2], final[0:128], NT)
        return (
            r[:, 0:128]
            + (r[:, 128:256] + m[:, 0:128])
            + (r[:, 256:384] + m[:, 128:256] + small)
        )

    def other_rows(slab):
        return lambda n: held[slab, n].reshape(512, 512)

    a_f, s_f, a_m, s_m, a_l, s_l, row_weight = (coef[k] for k in range(7))

    lat0 = latent8[...]
    spread(lat0, teacher_embed, hidden, placed)
    shape(hidden, 0, shaped)
    for c in swaps:
        c.wait_recv()
    t_step(0)
    s_step(0)
    load.wait()
    project(shaped, lambda j: near_qkv[j])
    t_step(1)
    attend(heads.at[0], False)
    swaps.append(swap(heads.at[0], heads_in.at[0], 2))
    t_step(2)
    spread(lat0, student_embed, hidden_s, placed)
    t_step(3)
    s_step(1)
    shape(hidden_s, 2, shaped_s)
    t_step(4)
    s_step(2)
    mix(heads.at[0], lambda n: teacher_out[n].reshape(512, 512), 0, hidden)
    t_step(5)
    s_step(3)
    t_step(6)
    swaps[2].wait_recv()
    mix(heads_in.at[0], other_rows(5), 0, mixed)
    eps0 = predict(teacher_final, False)
    lat1 = a_m * (lat0 - s_f * eps0) / a_f + s_m * eps0

    spread(lat1, teacher_embed, hidden, placed)
    shape(hidden, 1, shaped)
    project(shaped, lambda j: near_qkv[j])
    attend(heads.at[1], False)
    swaps.append(swap(heads.at[1], heads_in.at[1], 3))
    s_step(4)
    mix(heads.at[1], lambda n: teacher_out[n].reshape(512, 512), 1, hidden)
    swaps[3].wait_recv()
    mix(heads_in.at[1], other_rows(5), 1, mixed)
    eps1 = predict(teacher_final, False)
    lat2 = a_l * (lat1 - s_m * eps1) / a_m + s_l * eps1
    target = (lat0 - a_f / a_l * lat2) / (s_f - a_f * s_l / a_l)

    s_step(5)

    def turn(src, out):
        def body(n, carry):
            t = src[:, columns(n, 128)].astype(jnp.float32).T.astype(jnp.bfloat16)
            out[pl.ds(2 * n, 2)] = t.reshape(2, 2, 32, TOKENS)
            return carry

        lax.fori_loop(0, D // 128, body, 0)

    turn(shaped_s, shaped_t)
    s_step(6)
    project(shaped_s, lambda j: held[j].reshape(D, 512))
    attend(heads.at[2], True)
    swaps.append(swap(heads.at[2], heads_in.at[2], 4))
    mix(heads.at[2], other_rows(3), 2, hidden_s)
    swaps[4].wait_recv()
    mix(heads_in.at[2], other_rows(4), 2, mixed)
    error = predict(student_final, True) - target
    lanes = lax.broadcasted_iota(jnp.int32, error.shape, 1)
    loss_part[...] = jnp.full(
        (8, 128), 0.5 * row_weight * jnp.sum(jnp.where(lanes < 16, error * error, 0.0))
    )

    spread(2.0 * row_weight * error, student_back, hidden)

    def back(n, carry):
        rows = columns(n, 16)
        up, u = hidden[rows], mixed[rows]
        first_mean = jnp.mean(up, axis=-1, keepdims=True)
        second_mean = jnp.mean(up * u, axis=-1, keepdims=True)
        d = (up - first_mean - u * second_mean) * inverses[rows, 0:1]
        shaped[rows] = (mods[2, 2:3] * d).astype(jnp.bfloat16)
        return carry

    lax.fori_loop(0, TOKENS // 16, back, 0)
    d_attn[...] = dot(shaped[...], held[3].reshape(D, 512)).astype(jnp.bfloat16)

    def back_heads(hp, carry):
        cols = columns(hp, 128)
        q, k, v, da = qkv[0, :, cols], qkv[1, :, cols], qkv[2, :, cols], d_attn[:, cols]
        outs = []
        for h in range(2):
            w = weights[2 * hp + h]
            dp = dot(da * sides[h], v, NT)
            ds = w * (dp - jnp.sum(w * dp, axis=-1, keepdims=True)) * 0.125
            ds = ds.astype(jnp.bfloat16)
            outs.append((dot(ds, k), dot(ds, q, TN), dot(w.astype(jnp.bfloat16), da, TN)))
        for j in range(3):
            spot = pl.ds(pl.multiple_of(j * 512 + hp * 128, 128), 128)
            both = jnp.where(is_low, outs[0][j], outs[1][j])
            packed[:, spot] = both.astype(jnp.bfloat16)
        packed[:, pl.ds(pl.multiple_of(1536 + hp * 128, 128), 128)] = heads[2, :, cols]
        return carry

    lax.fori_loop(0, 4, back_heads, 0)
    turn(shaped, proj_t)
    for c in swaps:
        c.wait_send()


def three_parts(values):
    high = lax.reduce_precision(values, 8, 7)
    rest = values - high
    middle = lax.reduce_precision(rest, 8, 7)
    return high, middle, rest - middle


def stacked(values):
    h, m, l = three_parts(values)
    zero = jnp.zeros_like(h)
    return jnp.concatenate([h, m, h, l, h, m, zero, zero], axis=0).astype(jnp.bfloat16)


def repeated(values):
    return jnp.concatenate([jnp.tile(t, (8, 1)) for t in three_parts(values)], axis=0).astype(
        jnp.bfloat16
    )


def whole_step(coef, latent8, mods, placed, teacher, student, qkv_t, out_t, qkv_s, out_s):
    vmem = pl.BlockSpec(memory_space=pltpu.VMEM)
    bf16, f32 = jnp.bfloat16, jnp.float32
    return pl.pallas_call(
        step_kernel,
        out_shape=(
            jax.ShapeDtypeStruct((32, 2, 32, TOKENS), bf16),
            jax.ShapeDtypeStruct((32, 2, 32, TOKENS), bf16),
            jax.ShapeDtypeStruct((TOKENS, D), bf16),
            jax.ShapeDtypeStruct((8, 128), f32),
        ),
        in_specs=[pl.BlockSpec(memory_space=pltpu.SMEM)]
        + [vmem] * 8
        + [pl.BlockSpec(memory_space=pl.ANY)]
        + [vmem] * 3,
        out_specs=(vmem,) * 4,
        scratch_shapes=[
            pltpu.VMEM((6, 4, 4, 2, 2, 2, 16, 512), bf16),
            pltpu.VMEM((3, D, 512), bf16),
            pltpu.VMEM((TOKENS, D), f32),
            pltpu.VMEM((TOKENS, D), f32),
            pltpu.VMEM((TOKENS, D), f32),
            pltpu.VMEM((TOKENS, D), bf16),
            pltpu.VMEM((TOKENS, D), bf16),
            pltpu.VMEM((3, TOKENS, 512), bf16),
            pltpu.VMEM((3, TOKENS, 512), bf16),
            pltpu.VMEM((3, TOKENS, 512), bf16),
            pltpu.VMEM((8, TOKENS, TOKENS), f32),
            pltpu.VMEM((3, TOKENS, D), bf16),
            pltpu.VMEM((TOKENS, 128), f32),
            pltpu.VMEM((TOKENS, 512), bf16),
            pltpu.SemaphoreType.DMA,
            pltpu.SemaphoreType.DMA((5,)),
            pltpu.SemaphoreType.DMA((5,)),
            pltpu.SemaphoreType.DMA((18,)),
            pltpu.SemaphoreType.DMA((18,)),
            pltpu.SemaphoreType.DMA((18,)),
            pltpu.SemaphoreType.DMA((18,)),
        ],
        compiler_params=pltpu.CompilerParams(
            collective_id=2, has_side_effects=True, vmem_limit_bytes=62 * 2**20
        ),
    )(
        coef,
        latent8,
        mods,
        placed,
        stacked(teacher[0]),
        repeated(teacher[1]),
        stacked(student[0]),
        repeated(student[1]),
        stacked(student[1]),
        jnp.moveaxis(qkv_t, 1, 0),
        out_t.reshape(4, 4, 2, 2, 2, 16, 512),
        jnp.moveaxis(qkv_s, 1, 0).reshape(3, 2, 16, 512),
        out_s.reshape(2, 16, 512),
    )


def plan():
    grid = jnp.arange(TGRID + 1, dtype=jnp.float32)
    lamb = 6.0 - 12.0 * grid / TGRID
    return (jnp.sqrt(jax.nn.sigmoid(lamb)), jnp.sqrt(jax.nn.sigmoid(-lamb)))


def positions():
    half = D // 2
    freqs = jnp.exp(-math.log(10000.0) * jnp.arange(half, dtype=jnp.float32) / half)
    steps = jnp.arange(16, dtype=jnp.float32)[:, None]
    coarse, fine = 16.0 * steps * freqs[None], steps * freqs[None]
    sin_a, cos_a = jnp.sin(coarse)[:, None], jnp.cos(coarse)[:, None]
    sin_b, cos_b = jnp.sin(fine)[None], jnp.cos(fine)[None]
    both = [sin_a * cos_b + cos_a * sin_b, cos_a * cos_b - sin_a * sin_b]
    return jnp.concatenate(both, axis=2).reshape(SEQ, D)


def one_hot_rows(index, width):
    return (index[:, None] == jnp.arange(width, dtype=jnp.int32)[None, :]).astype(jnp.float32)


def per_device(
    clean_latent,
    noise_draw,
    timestep,
    bucket,
    bucket_weights,
    teacher_embed,
    teacher_final,
    teacher_mod,
    teacher_qkv,
    teacher_out,
    student_embed,
    student_final,
    student_mod,
    student_qkv,
    student_out,
    moment_qkv,
    second_qkv,
    moment_out,
    second_out,
):
    samples = clean_latent.shape[0]
    alphas, sigmas = plan()
    table = jnp.stack([alphas, sigmas], axis=1)
    first = 2 * timestep
    taus = jnp.concatenate([first, first - 1, first - 2])
    picked = jnp.dot(one_hot_rows(taus, TGRID + 1), table, precision=lax.Precision.HIGHEST)
    weight = jnp.dot(
        one_hot_rows(bucket, NBUCKET), bucket_weights, precision=lax.Precision.HIGHEST
    )
    coef = jnp.concatenate([picked.reshape(-1), weight, jnp.zeros((1,), jnp.float32)])
    steps = one_hot_rows(jnp.concatenate([first - 1, first - 2]), TGRID)
    mods = jnp.concatenate(
        [
            jnp.dot(steps, teacher_mod.reshape(TGRID, 3 * D), precision=lax.Precision.HIGHEST),
            jnp.dot(
                one_hot_rows(timestep - 1, K),
                student_mod.reshape(K, 3 * D),
                precision=lax.Precision.HIGHEST,
            ),
        ]
    ).reshape(3, 3, D)
    latent0 = (coef[0] * clean_latent + coef[1] * noise_draw).reshape(SEQ, PATCH_CH)
    shaped, proj, packed, loss_part = whole_step(
        coef,
        jnp.tile(latent0, (1, 8)),
        mods,
        positions(),
        (teacher_embed, teacher_final),
        (student_embed, student_final),
        teacher_qkv,
        teacher_out,
        student_qkv,
        student_out,
    )
    grads, totals = reduce_gradients(shaped, proj, packed, loss_part)
    grad_qkv = jnp.moveaxis(grads[:3], 0, 1)
    grad_out = grads[3]
    squares, loss_sum = totals[0, 0], totals[1, 0]
    rms_value = jnp.sqrt(squares / (4 * D * INNER))
    factor = 1.0 / jnp.maximum(rms_value, 1.0)

    def adam(moment, second, grad):
        normed_grad = grad * factor
        new_moment = BETA_ONE * moment + (1.0 - BETA_ONE) * normed_grad
        new_second = BETA_TWO * second + (1.0 - BETA_TWO) * normed_grad * normed_grad
        return (new_moment, new_second, new_moment / (jnp.sqrt(new_second) + ADAM_EPS))

    mq, vq, uq = adam(moment_qkv, second_qkv, grad_qkv)
    mo, vo, uo = adam(moment_out, second_out, grad_out)
    loss = loss_sum / (samples * lax.axis_size(DP) * LATENT)
    return (mq, vq, uq, mo, vo, uo, loss)


def solution(mesh):
    torus = Mesh(
        mesh.devices.reshape(4, 4, 2, 2, mesh.shape["mp"]), ("dp_0", "dp_1", "dp_2", "dp_3", "mp")
    )
    in_specs = (
        P(DP, None),
        P(DP, None),
        P(DP),
        P(DP),
        P(),
        P(),
        P(),
        P(),
        P(None, None, "mp"),
        P(None, "mp"),
        P(),
        P(),
        P(),
        P(DP, None, "mp"),
        P(DP, "mp"),
        P(DP, None, "mp"),
        P(DP, None, "mp"),
        P(DP, "mp"),
        P(DP, "mp"),
    )
    out_specs = (
        P(DP, None, "mp"),
        P(DP, None, "mp"),
        P(DP, None, "mp"),
        P(DP, "mp"),
        P(DP, "mp"),
        P(DP, "mp"),
        P(),
    )
    return jax.shard_map(
        per_device, mesh=torus, in_specs=in_specs, out_specs=out_specs, check_vma=False
    )
```

```python
import math

import jax
import jax.numpy as jnp
import numpy as np
from jax import lax
from jax.experimental import pallas as pl
from jax.experimental.pallas import tpu as pltpu
from jax.sharding import Mesh
from jax.sharding import PartitionSpec as P

D = 2048
HS = 64
INNER = 1024
PATCH_CH = 16
SEQ = 256
LATENT = 4096
SAMPLES = 64
K = 8
TGRID = 16
NBUCKET = 8
DP = ("dp_0", "dp_1", "dp_2", "dp_3")
DP_MP = ("dp_0", "dp_1", "dp_2", "dp_3", "mp")


LN_EPS = 0.01
BETA_ONE = 0.9
BETA_TWO = 0.99
ADAM_EPS = 1e-08


ROWS = 1024
HALF = 1024
AXES = ("dp_0", "dp_1", "dp_2", "dp_3", "mp")


def remote(src, dst, send, recv, axis, target):
    return pltpu.make_async_remote_copy(
        src_ref=src,
        dst_ref=dst,
        send_sem=send,
        recv_sem=recv,
        device_id={axis: target} if isinstance(axis, str) else dict(zip(axis, target)),
        device_id_type=pl.DeviceIdType.MESH,
    )


def greet(friends):
    barrier = pltpu.get_barrier_semaphore()
    for axis, target in friends:
        pl.semaphore_signal(
            barrier,
            inc=1,
            device_id={axis: target} if isinstance(axis, str) else dict(zip(axis, target)),
            device_id_type=pl.DeviceIdType.MESH,
        )
    pl.semaphore_wait(barrier, len(friends))


def all_places():
    y, x, z, core, mp = (lax.axis_index(a) for a in AXES)
    return [
        (core, [("dp_3", 1 - core)]),
        (2 * mp + z, [("dp_2", 1 - z), ("mp", 1 - mp), (("dp_2", "mp"), (1 - z, 1 - mp))]),
        (x, [("dp_1", lax.rem(x + k, 4)) for k in (1, 2, 3)]),
        (y, [("dp_0", lax.rem(y + k, 4)) for k in (1, 2, 3)]),
    ]


def sum_over_all(value, inbox, send, recv):
    for stage, (slot, partners) in enumerate(all_places()):
        inbox[stage, slot] = value
        copies = [
            remote(
                inbox.at[stage, slot],
                inbox.at[stage, slot],
                send.at[stage, k],
                recv.at[stage, k],
                axis,
                target,
            )
            for k, (axis, target) in enumerate(partners)
        ]
        for c in copies:
            c.start()
        for c in copies:
            c.wait_recv()
        value = inbox[stage, 0]
        for k in range(1, len(partners) + 1):
            value = value + inbox[stage, k]
        for c in copies:
            c.wait_send()
    return value


def ring_start(axis, part, relay, direct, send, recv):
    me = lax.axis_index(axis)
    right, left, far = (lax.rem(me + k, 4) for k in (1, 3, 2))
    half = part.shape[1] // 2
    top, low = pl.ds(0, half), pl.ds(half, half)
    copies = [
        remote(part.at[far, top], relay.at[0], send.at[0], recv.at[0], axis, right),
        remote(part.at[far, low], relay.at[1], send.at[1], recv.at[1], axis, left),
        remote(part.at[right, low], direct.at[0], send.at[2], recv.at[2], axis, right),
        remote(part.at[left, top], direct.at[1], send.at[3], recv.at[3], axis, left),
    ]
    for c in copies:
        c.start()
    return copies


def ring_relay(axis, copies, part, relay, passed, summed, send, recv):
    me = lax.axis_index(axis)
    right, left = (lax.rem(me + k, 4) for k in (1, 3))
    half = part.shape[1] // 2
    top, low = pl.ds(0, half), pl.ds(half, half)
    copies[0].wait_recv()
    passed[0] = relay[0] + part[right, top]
    first = remote(passed.at[0], summed.at[0], send.at[4], recv.at[4], axis, right)
    first.start()
    copies[1].wait_recv()
    passed[1] = relay[1] + part[left, low]
    second = remote(passed.at[1], summed.at[1], send.at[5], recv.at[5], axis, left)
    second.start()
    return [first, second]


def ring_finish(axis, copies, more, part, direct, summed):
    me = lax.axis_index(axis)
    half = part.shape[1] // 2
    copies[3].wait_recv()
    more[0].wait_recv()
    upper = part[me, pl.ds(0, half)] + direct[1] + summed[0]
    copies[2].wait_recv()
    more[1].wait_recv()
    lower = part[me, pl.ds(half, half)] + direct[0] + summed[1]
    for c in [*copies, *more]:
        c.wait_send()
    return upper, lower


def reduce_kernel(
    shaped,
    proj,
    packed,
    loss_part,
    out,
    totals,
    shaped_in,
    proj_in,
    packed_in,
    part_a,
    part_b,
    part_c,
    part_d,
    *rest,
):
    boxes_a, boxes_b, boxes_c, boxes_d = rest[0:4], rest[4:8], rest[8:12], rest[12:16]
    last, last_in, pair_send, pair_recv, send, recv, z_send, z_recv = rest[16:24]
    inbox, sum_send, sum_recv = rest[24:]
    y, x, z, core = (lax.axis_index(a) for a in AXES[:4])
    greet([friend for _, partners in all_places() for friend in partners])
    pair = [
        remote(a, b, pair_send.at[k], pair_recv.at[k], "dp_3", 1 - core)
        for k, (a, b) in enumerate(
            [(packed, packed_in), (shaped.at[:, 1 - core], shaped_in), (proj.at[:, 1 - core], proj_in)]
        )
    ]
    for c in pair:
        c.start()

    def products(s_ref, p_ref, b_ref, add):
        def step(k, carry):
            rows = pl.ds(pl.multiple_of(k * 8, 8), 8)
            s, p = (r[rows].reshape(256, SEQ) for r in (s_ref, p_ref))
            g = jnp.dot(s, b_ref[:, :HALF], preferred_element_type=jnp.float32)
            for j in range(4):
                block = g[64 * j : 64 * j + 64]
                spot = pl.ds(pl.multiple_of(k * 64, 64), 64)
                part_a[j, spot] = part_a[j, spot] + block if add else block
            h = jnp.dot(s, b_ref[:, HALF : HALF + 512], preferred_element_type=jnp.float32)
            part_b[k, :, 0:512] = part_b[k, :, 0:512] + h if add else h
            o = jnp.dot(p, b_ref[:, HALF + 512 :], preferred_element_type=jnp.float32)
            part_b[k, :, 512:1024] = part_b[k, :, 512:1024] + o if add else o
            return carry

        lax.fori_loop(0, 4, step, 0)

    products(shaped.at[:, core], proj.at[:, core], packed, False)
    for c in pair:
        c.wait_recv()
    products(shaped_in, proj_in, packed_in, True)

    first_a = ring_start("dp_1", part_a, boxes_a[0], boxes_a[1], send.at[0], recv.at[0])
    first_b = ring_start("dp_0", part_b, boxes_b[0], boxes_b[1], send.at[1], recv.at[1])
    more_a = ring_relay(
        "dp_1", first_a, part_a, boxes_a[0], boxes_a[2], boxes_a[3], send.at[0], recv.at[0]
    )
    more_b = ring_relay(
        "dp_0", first_b, part_b, boxes_b[0], boxes_b[2], boxes_b[3], send.at[1], recv.at[1]
    )
    upper, lower = ring_finish("dp_1", first_a, more_a, part_a, boxes_a[1], boxes_a[3])
    for k in range(2):
        part_c[k] = upper[64 * k : 64 * k + 64]
        part_c[2 + k] = lower[64 * k : 64 * k + 64]
    first_c = ring_start("dp_0", part_c, boxes_c[0], boxes_c[1], send.at[2], recv.at[2])
    upper, lower = ring_finish("dp_0", first_b, more_b, part_b, boxes_b[1], boxes_b[3])
    for k in range(2):
        part_d[k] = upper[64 * k : 64 * k + 64]
        part_d[2 + k] = lower[64 * k : 64 * k + 64]
    first_d = ring_start("dp_1", part_d, boxes_d[0], boxes_d[1], send.at[3], recv.at[3])
    more_c = ring_relay(
        "dp_0", first_c, part_c, boxes_c[0], boxes_c[2], boxes_c[3], send.at[2], recv.at[2]
    )
    more_d = ring_relay(
        "dp_1", first_d, part_d, boxes_d[0], boxes_d[2], boxes_d[3], send.at[3], recv.at[3]
    )
    z_copies = []
    for k, (axis, first, more, part, boxes) in enumerate(
        [
            ("dp_0", first_c, more_c, part_c, boxes_c),
            ("dp_1", first_d, more_d, part_d, boxes_d),
        ]
    ):
        upper, lower = ring_finish(axis, first, more, part, boxes[1], boxes[3])
        last[k, 0] = upper
        last[k, 1] = lower
        c = remote(
            last.at[k, 1 - z], last_in.at[k], z_send.at[k], z_recv.at[k], "dp_2", 1 - z
        )
        c.start()
        z_copies.append(c)
    for k, c in enumerate(z_copies):
        c.wait_recv()
        both = last[k, z] + last_in[k]
        out[2 * k] = both[:, :512]
        out[2 * k + 1] = both[:, 512:]
    for c in [*pair, *z_copies]:
        c.wait_send()
    squares = jnp.sum(out[...] * out[...])
    row = lax.broadcasted_iota(jnp.int32, (8, 128), 0)
    value = jnp.where(row == 0, squares, loss_part[...])
    totals[...] = sum_over_all(value, inbox, sum_send, sum_recv)


def reduce_gradients(shaped, proj, packed, loss_part):
    vmem = pl.BlockSpec(memory_space=pltpu.VMEM)
    wire = jnp.float32

    def boxes(half):
        return [pltpu.VMEM((2, half, HALF), wire)] * 4

    return pl.pallas_call(
        reduce_kernel,
        out_shape=(
            jax.ShapeDtypeStruct((4, 32, 512), jnp.float32),
            jax.ShapeDtypeStruct((8, 128), jnp.float32),
        ),
        in_specs=[vmem] * 4,
        out_specs=(vmem, vmem),
        scratch_shapes=[
            pltpu.VMEM((32, 32, SEQ), jnp.bfloat16),
            pltpu.VMEM((32, 32, SEQ), jnp.bfloat16),
            pltpu.VMEM((SEQ, 2 * HALF), jnp.bfloat16),
            pltpu.VMEM((4, 256, HALF), jnp.float32),
            pltpu.VMEM((4, 256, HALF), jnp.float32),
            pltpu.VMEM((4, 64, HALF), jnp.float32),
            pltpu.VMEM((4, 64, HALF), jnp.float32),
            *boxes(128),
            *boxes(128),
            *boxes(32),
            *boxes(32),
            pltpu.VMEM((2, 2, 32, HALF), jnp.float32),
            pltpu.VMEM((2, 32, HALF), jnp.float32),
            pltpu.SemaphoreType.DMA((3,)),
            pltpu.SemaphoreType.DMA((3,)),
            pltpu.SemaphoreType.DMA((4, 6)),
            pltpu.SemaphoreType.DMA((4, 6)),
            pltpu.SemaphoreType.DMA((2,)),
            pltpu.SemaphoreType.DMA((2,)),
            pltpu.VMEM((4, 4, 8, 128), jnp.float32),
            pltpu.SemaphoreType.DMA((4, 3)),
            pltpu.SemaphoreType.DMA((4, 3)),
        ],
        compiler_params=pltpu.CompilerParams(
            collective_id=1, has_side_effects=True, vmem_limit_bytes=60 * 2**20
        ),
    )(shaped, proj, packed, loss_part)


TOKENS = 256
UNROLL = 4
WIDE = 256
NT = (((1,), (1,)), ((), ()))
TN = (((0,), (0,)), ((), ()))


def dot(a, b, dims=(((1,), (0,)), ((), ()))):
    return lax.dot_general(a, b, dims, preferred_element_type=jnp.float32)


def gather_stream(held, slabs, send, recv):
    y, x, z, core = (lax.axis_index(a) for a in AXES[:4])
    near = {"dp_0": [lax.rem(y + k, 4) for k in (1, 3)], "dp_1": [lax.rem(x + k, 4) for k in (1, 3)]}
    every = slice(None)
    live = []

    def go(spot, k, axis, target):
        ref = held.at[(slabs, *spot)]
        c = remote(ref, ref, send.at[k], recv.at[k], axis, target)
        c.start()
        live.append(c)
        return c

    def ring_direct(first):
        for half, axis in enumerate(("dp_1", "dp_0") if first else ("dp_0", "dp_1")):
            if first:
                spot = (y, x, every, core, half)
            elif half == 0:
                spot = (y, every, every, core, half)
            else:
                spot = (every, x, every, core, half)
            for side in range(2):
                k = (1 if first else 9) + 4 * half + side
                go(spot, k, axis, near[axis][side])

    def ring_relay(first):
        base = 1 if first else 9
        direct = live[-4:]
        for half, axis in enumerate(("dp_1", "dp_0") if first else ("dp_0", "dp_1")):
            for side in range(2):
                direct[2 * half + side].wait_recv()
                back = near[axis][1 - side]
                if first:
                    spot = (y, back) if axis == "dp_1" else (back, x)
                else:
                    spot = (every, back) if axis == "dp_1" else (back, every)
                go((*spot, side, core, half), base + 4 * half + 2 + side, axis, near[axis][side])

    def across(k, spot):
        go((*spot[:3], core, spot[3]), k, "dp_3", 1 - core)

    def step(k):
        if k == 0:
            go((y, x, z, core), 0, "dp_2", 1 - z)
        elif k == 1:
            live[-1].wait_recv()
            ring_direct(True)
        elif k == 2:
            ring_relay(True)
        elif k == 3:
            for c in live[-4:]:
                c.wait_recv()
            ring_direct(False)
        elif k == 4:
            ring_relay(False)
            relays.extend(live[-4:])
            across(17, (y, every, every, 0))
            across(18, (every, x, every, 1))
            for n in range(2):
                across(19 + 2 * n, (near["dp_0"][n], every, every, 0))
                across(20 + 2 * n, (every, near["dp_1"][n], every, 1))
        elif k == 5:
            for c in relays:
                c.wait_recv()
            across(23, (lax.rem(y + 2, 4), every, every, 0))
            across(24, (every, lax.rem(x + 2, 4), every, 1))
        else:
            for c in live[-8:]:
                c.wait_recv()
            for c in live:
                c.wait_send()

    relays = []
    return step


def gather_direct(held, slab, send, recv):
    y, x, z, core = (lax.axis_index(a) for a in AXES[:4])
    every = slice(None)
    live = []

    def ring(spots, base):
        for half, (axis, spot) in enumerate(spots):
            me = lax.axis_index(axis)
            for k in (1, 2, 3):
                ref = held.at[(slab, *spot, core, half)]
                n = base + 3 * half + k - 1
                c = remote(ref, ref, send.at[n], recv.at[n], axis, lax.rem(me + k, 4))
                c.start()
                live.append(c)

    def step(k):
        if k == 0:
            ring([("dp_1", (y, x, every)), ("dp_0", (y, x, every))], 0)
        elif k == 1:
            for c in live:
                c.wait_recv()
            ring([("dp_0", (y, every, every)), ("dp_1", (every, x, every))], 6)
        elif k == 2:
            for c in live[6:]:
                c.wait_recv()
            ref = held.at[slab, :, :, :, core]
            c = remote(ref, ref, send.at[12], recv.at[12], "dp_3", 1 - core)
            c.start()
            live.append(c)
        else:
            live[-1].wait_recv()
            for c in live:
                c.wait_send()

    return step


def three_terms(v8):
    high = v8.astype(jnp.bfloat16).astype(jnp.float32)
    rest = v8 - high
    middle = rest.astype(jnp.bfloat16).astype(jnp.float32)
    low = rest - middle
    group = lax.broadcasted_iota(jnp.int32, v8.shape, 1) // 16
    picked = jnp.where(
        (group == 0) | (group == 1) | (group == 3),
        high,
        jnp.where((group == 2) | (group == 5), middle, jnp.where(group == 4, low, 0.0)),
    )
    return picked.astype(jnp.bfloat16)


def picked_level(step, offset, values):
    out = jnp.float32(0.0)
    for k in range(1, K + 1):
        out = jnp.where(step == k, jnp.float32(values[2 * k + offset]), out)
    return out


def step_kernel(
    timestep,
    bucket,
    bucket_weights,
    clean8,
    noise8,
    tables,
    teacher_embed,
    teacher_final,
    teacher_mod,
    student_embed,
    student_final,
    student_mod,
    teacher_qkv,
    teacher_out,
    student_qkv,
    student_out,
    shaped_t,
    proj_t,
    packed,
    loss_part,
    held,
    near_qkv,
    placed,
    hidden,
    hidden_s,
    mixed,
    shaped,
    shaped_s,
    qkv,
    heads,
    heads_in,
    weights,
    terms,
    inverses,
    d_attn,
    embed_t,
    embed_s,
    back_s,
    final_t,
    final_s,
    qkv_sem,
    swap_send,
    swap_recv,
    t_send,
    t_recv,
    s_send,
    s_recv,
):
    y, x, z, core, mp = (lax.axis_index(a) for a in AXES)
    load = pltpu.make_async_copy(teacher_qkv, near_qkv, qkv_sem)
    load.start()
    held[0:3, y, x, z, core] = student_qkv[...]
    held[3, y, x, z, core] = student_out[...]
    both = ("dp_2", "mp")
    friends = [("dp_3", 1 - core), ("dp_2", 1 - z), ("mp", 1 - mp), (both, (1 - z, 1 - mp))]
    friends += [("dp_1", lax.rem(x + k, 4)) for k in (1, 2, 3)]
    friends += [("dp_0", lax.rem(y + k, 4)) for k in (1, 2, 3)]
    greet(friends)

    def swap(src, dst, k, axis="mp", target=None):
        target = 1 - mp if target is None else target
        return remote(src, dst, swap_send.at[k], swap_recv.at[k], axis, target)

    spot = (y, x, z, core)
    here = teacher_out.at[spot]
    swaps = [
        swap(here, held.at[(5, *spot)], 0),
        swap(here, held.at[(5, *spot)], 1, both, (1 - z, 1 - mp)),
        swap(student_out, held.at[(4, *spot)], 2),
    ]
    for c in swaps:
        c.start()
    t_step = gather_direct(held, 5, t_send, t_recv)
    s_step = gather_stream(held, pl.ds(0, 5), s_send, s_recv)

    step = timestep[0]
    a_f, a_m, a_l = (picked_level(step, -k, ALPHAS) for k in range(3))
    s_f, s_m, s_l = (picked_level(step, -k, SIGMAS) for k in range(3))
    row_weight = bucket_weights[jnp.clip(bucket[0], 0, NBUCKET - 1)]
    places = [
        (teacher_mod, jnp.clip(2 * step - 1, 0, TGRID - 1)),
        (teacher_mod, jnp.clip(2 * step - 2, 0, TGRID - 1)),
        (student_mod, jnp.clip(step - 1, 0, K - 1)),
    ]
    modrows = [[mod[j, pl.ds(at, 1), :] for j in range(3)] for mod, at in places]

    def split_rows(ref):
        v = ref[...]
        h = v.astype(jnp.bfloat16)
        rest = v - h.astype(jnp.float32)
        m = rest.astype(jnp.bfloat16)
        return h, m, (rest - m.astype(jnp.float32)).astype(jnp.bfloat16)

    def stack(parts, out):
        h, m, l = parts
        for k, v in enumerate([h, m, h, l, h, m, jnp.zeros_like(h), jnp.zeros_like(h)]):
            out[16 * k : 16 * k + 16] = v

    def repeat(parts, out):
        for k in range(24):
            out[16 * k : 16 * k + 16] = parts[k // 8]

    def columns(k, width):
        return pl.ds(pl.multiple_of(k * width, width), width)

    def spread(v8, b_ref, out, base=None):
        terms8 = three_terms(v8)

        def body(n, carry):
            cols = columns(n, WIDE)
            h = dot(terms8, b_ref[:, cols])
            out[:, cols] = h if base is None else h + base[:, cols]
            return carry

        lax.fori_loop(0, D // WIDE, body, 0)

    def centred(v):
        c = v - jnp.mean(v, axis=-1, keepdims=True)
        return c, lax.rsqrt(jnp.mean(c * c, axis=-1, keepdims=True) + LN_EPS)

    def by_rows(body):
        def group(n, carry):
            for u in range(UNROLL):
                body(pl.ds(pl.multiple_of(n * (16 * UNROLL) + 16 * u, 16), 16))
            return carry

        lax.fori_loop(0, TOKENS // (16 * UNROLL), group, 0)

    def shape(hid, which, out):
        shift, scale = modrows[which][0], 1.0 + modrows[which][1]

        def body(rows):
            c, inv = centred(hid[rows])
            out[rows] = (c * inv * scale + shift).astype(jnp.bfloat16)

        by_rows(body)

    def project(src, weight):
        def body(j, carry):
            qkv[j] = dot(src[...], weight(j)).astype(jnp.bfloat16)
            return carry

        lax.fori_loop(0, 3, body, 0)

    lane = lax.broadcasted_iota(jnp.int32, (1, 128), 1)
    low_f = jnp.where(lane < 64, 1.0, 0.0)
    sides = [low_f.astype(jnp.bfloat16), (1.0 - low_f).astype(jnp.bfloat16)]
    is_low = lax.broadcasted_iota(jnp.int32, (TOKENS, 128), 1) < 64

    def swap_pair(which, hp):
        cols = pl.ds(128 * hp, 128)
        return swap(heads.at[which, :, cols], heads_in.at[which, :, cols], 3 + 4 * which + hp)

    def attend(which, keep):
        for hp in range(4):
            cols = pl.ds(128 * hp, 128)
            q, k, v = qkv[0, :, cols], qkv[1, :, cols], qkv[2, :, cols]
            outs = []
            for h in range(2):
                s = dot(q * sides[h], k, NT) * 0.125
                e = jnp.exp(s - jnp.max(s, axis=-1, keepdims=True))
                w = e / jnp.sum(e, axis=-1, keepdims=True)
                if keep:
                    weights[2 * hp + h] = w
                outs.append(dot(w.astype(jnp.bfloat16), v))
            heads[which, :, cols] = jnp.where(is_low, outs[0], outs[1]).astype(jnp.bfloat16)
            if hp > 0:
                swap_pair(which, hp - 1).start()
        swap_pair(which, 3).start()

    def swapped(which):
        for hp in range(4):
            swap_pair(which, hp).wait_recv()

    def mix(att, weight, which, base):
        mod_ref, at = places[which]

        def body(n, carry):
            cols = columns(n, 512)
            p = dot(att[...], weight(n), NT)
            mixed[:, cols] = base[:, cols] + mod_ref[2, pl.ds(at, 1), cols] * p
            return carry

        lax.fori_loop(0, 4, body, 0)

    def predict(final, keep):
        def body(rows):
            c, inv = centred(mixed[rows])
            u = c * inv
            if keep:
                placed[rows] = u
                inverses[rows] = jnp.broadcast_to(inv, (16, 128))
            high = u.astype(jnp.bfloat16)
            rest = u - high.astype(jnp.float32)
            middle = rest.astype(jnp.bfloat16)
            terms[0, rows] = high
            terms[1, rows] = middle
            terms[2, rows] = (rest - middle.astype(jnp.float32)).astype(jnp.bfloat16)

        by_rows(body)
        r = dot(terms[0], final[...], NT)
        m = dot(terms[1], final[0:256], NT)
        small = dot(terms[2], final[0:128], NT)
        return (
            r[:, 0:128]
            + (r[:, 128:256] + m[:, 0:128])
            + (r[:, 256:384] + m[:, 128:256] + small)
        )

    def other_rows(slab):
        return lambda n: held[slab, n].reshape(512, 512)

    def near_rows(n):
        return teacher_out[n].reshape(512, 512)

    def turn(src, out):
        def body(n, carry):
            t = src[:, columns(n, 128)].astype(jnp.float32).T.astype(jnp.bfloat16)
            out[pl.ds(2 * n, 2)] = t.reshape(2, 2, 32, TOKENS)
            return carry

        lax.fori_loop(0, D // 128, body, 0)

    half = D // 2
    for k in range(16):
        sin_a, cos_a = tables[0, k : k + 1], tables[1, k : k + 1]
        rows = pl.ds(16 * k, 16)
        placed[rows, :half] = sin_a * tables[3] + cos_a * tables[2]
        placed[rows, half:] = cos_a * tables[3] - sin_a * tables[2]
    stack(split_rows(teacher_embed), embed_t)
    lat0 = a_f * clean8[...] + s_f * noise8[...]
    spread(lat0, embed_t, hidden, placed)
    swaps[0].wait_recv()
    swaps[1].wait_recv()
    t_step(0)
    swaps[2].wait_recv()
    s_step(0)
    shape(hidden, 0, shaped)
    load.wait()
    project(shaped, lambda j: near_qkv[j])
    t_step(1)
    s_step(1)
    attend(0, False)
    t_step(2)
    s_step(2)
    mix(heads.at[0], near_rows, 0, hidden)
    stack(split_rows(student_embed), embed_s)
    repeat(split_rows(teacher_final), final_t)
    spread(lat0, embed_s, hidden_s, placed)
    t_step(3)
    s_step(3)
    swapped(0)
    mix(heads_in.at[0], other_rows(5), 0, mixed)
    eps0 = predict(final_t, False)
    lat1 = a_m * (lat0 - s_f * eps0) / a_f + s_m * eps0

    spread(lat1, embed_t, hidden, placed)
    shape(hidden, 1, shaped)
    project(shaped, lambda j: near_qkv[j])
    attend(1, False)
    mix(heads.at[1], near_rows, 1, hidden)
    shape(hidden_s, 2, shaped_s)
    s_step(4)
    swapped(1)
    mix(heads_in.at[1], other_rows(5), 1, mixed)
    eps1 = predict(final_t, False)
    lat2 = a_l * (lat1 - s_m * eps1) / a_m + s_l * eps1
    target = (lat0 - a_f / a_l * lat2) / (s_f - a_f * s_l / a_l)

    s_step(5)
    turn(shaped_s, shaped_t)
    student_terms = split_rows(student_final)
    repeat(student_terms, final_s)
    stack(student_terms, back_s)
    s_step(6)
    project(shaped_s, lambda j: held[j].reshape(D, 512))
    attend(2, True)
    mix(heads.at[2], other_rows(3), 2, hidden_s)
    swapped(2)
    mix(heads_in.at[2], other_rows(4), 2, mixed)
    error = predict(final_s, True) - target
    lanes = lax.broadcasted_iota(jnp.int32, error.shape, 1)
    loss_part[...] = jnp.full(
        (8, 128), 0.5 * row_weight * jnp.sum(jnp.where(lanes < 16, error * error, 0.0))
    )

    spread(2.0 * row_weight * error, back_s, hidden)

    gate = modrows[2][2]

    def back(rows):
        up, u = hidden[rows], placed[rows]
        first_mean = jnp.mean(up, axis=-1, keepdims=True)
        second_mean = jnp.mean(up * u, axis=-1, keepdims=True)
        d = (up - first_mean - u * second_mean) * inverses[rows, 0:1]
        shaped[rows] = (gate * d).astype(jnp.bfloat16)

    by_rows(back)
    d_attn[...] = dot(shaped[...], held[3].reshape(D, 512)).astype(jnp.bfloat16)

    def back_heads(hp, carry):
        cols = columns(hp, 128)
        q, k, v, da = qkv[0, :, cols], qkv[1, :, cols], qkv[2, :, cols], d_attn[:, cols]
        outs = []
        for h in range(2):
            w = weights[2 * hp + h]
            dp = dot(da * sides[h], v, NT)
            ds = w * (dp - jnp.sum(w * dp, axis=-1, keepdims=True)) * 0.125
            ds = ds.astype(jnp.bfloat16)
            outs.append((dot(ds, k), dot(ds, q, TN), dot(w.astype(jnp.bfloat16), da, TN)))
        for j in range(3):
            spot = pl.ds(pl.multiple_of(j * 512 + hp * 128, 128), 128)
            both = jnp.where(is_low, outs[0][j], outs[1][j])
            packed[:, spot] = both.astype(jnp.bfloat16)
        packed[:, pl.ds(pl.multiple_of(1536 + hp * 128, 128), 128)] = heads[2, :, cols]
        return carry

    lax.fori_loop(0, 4, back_heads, 0)
    turn(shaped, proj_t)
    for c in swaps:
        c.wait_send()
    for which in range(3):
        for hp in range(4):
            swap_pair(which, hp).wait_send()


def levels():
    lamb = 6.0 - 12.0 * np.arange(TGRID + 1) / TGRID
    return [np.sqrt(1.0 / (1.0 + np.exp(sign * lamb))).astype(np.float32) for sign in (-1.0, 1.0)]


ALPHAS, SIGMAS = levels()


def position_tables():
    half = D // 2
    freqs = np.exp(-math.log(10000.0) * np.arange(half) / half)
    fine = np.arange(16)[:, None] * freqs[None]
    angles = (np.sin(16.0 * fine), np.cos(16.0 * fine), np.sin(fine), np.cos(fine))
    return np.stack(angles).astype(np.float32)


def whole_step(timestep, bucket, bucket_weights, clean, noise, teacher, student):
    vmem, smem = (pl.BlockSpec(memory_space=m) for m in (pltpu.VMEM, pltpu.SMEM))
    bf16, f32 = jnp.bfloat16, jnp.float32

    def tiled(v):
        return jnp.tile(v.reshape(SEQ, PATCH_CH), (1, 8))

    return pl.pallas_call(
        step_kernel,
        out_shape=(
            jax.ShapeDtypeStruct((32, 2, 32, TOKENS), bf16),
            jax.ShapeDtypeStruct((32, 2, 32, TOKENS), bf16),
            jax.ShapeDtypeStruct((TOKENS, D), bf16),
            jax.ShapeDtypeStruct((8, 128), f32),
        ),
        in_specs=[smem] * 3 + [vmem] * 9 + [pl.BlockSpec(memory_space=pl.ANY)] + [vmem] * 3,
        out_specs=(vmem,) * 4,
        scratch_shapes=[
            pltpu.VMEM((6, 4, 4, 2, 2, 2, 16, 512), bf16),
            pltpu.VMEM((3, D, 512), bf16),
            pltpu.VMEM((TOKENS, D), f32),
            pltpu.VMEM((TOKENS, D), f32),
            pltpu.VMEM((TOKENS, D), f32),
            pltpu.VMEM((TOKENS, D), f32),
            pltpu.VMEM((TOKENS, D), bf16),
            pltpu.VMEM((TOKENS, D), bf16),
            pltpu.VMEM((3, TOKENS, 512), bf16),
            pltpu.VMEM((3, TOKENS, 512), bf16),
            pltpu.VMEM((3, TOKENS, 512), bf16),
            pltpu.VMEM((8, TOKENS, TOKENS), f32),
            pltpu.VMEM((3, TOKENS, D), bf16),
            pltpu.VMEM((TOKENS, 128), f32),
            pltpu.VMEM((TOKENS, 512), bf16),
            pltpu.VMEM((128, D), bf16),
            pltpu.VMEM((128, D), bf16),
            pltpu.VMEM((128, D), bf16),
            pltpu.VMEM((384, D), bf16),
            pltpu.VMEM((384, D), bf16),
            pltpu.SemaphoreType.DMA,
            pltpu.SemaphoreType.DMA((15,)),
            pltpu.SemaphoreType.DMA((15,)),
            pltpu.SemaphoreType.DMA((13,)),
            pltpu.SemaphoreType.DMA((13,)),
            pltpu.SemaphoreType.DMA((25,)),
            pltpu.SemaphoreType.DMA((25,)),
        ],
        compiler_params=pltpu.CompilerParams(
            collective_id=2, has_side_effects=True, vmem_limit_bytes=62 * 2**20
        ),
    )(
        timestep,
        bucket,
        bucket_weights,
        tiled(clean),
        tiled(noise),
        jnp.asarray(position_tables()),
        teacher[0],
        teacher[1],
        jnp.moveaxis(teacher[2], 1, 0),
        student[0],
        student[1],
        jnp.moveaxis(student[2], 1, 0),
        jnp.moveaxis(teacher[3], 1, 0),
        teacher[4].reshape(4, 4, 2, 2, 2, 16, 512),
        jnp.moveaxis(student[3], 1, 0).reshape(3, 2, 16, 512),
        student[4].reshape(2, 16, 512),
    )


def adam_kernel(grads, totals, mq, vq, mo, vo, new_mq, new_vq, up_q, new_mo, new_vo, up_o, loss):
    rms = jnp.sqrt(totals[0:1, 0:1] / (4 * D * INNER))
    factor = 1.0 / jnp.maximum(rms, 1.0)

    def adam(grad, moment, second, new_moment, new_second, update):
        normed = grad * factor
        m = BETA_ONE * moment + (1.0 - BETA_ONE) * normed
        v = BETA_TWO * second + (1.0 - BETA_TWO) * normed * normed
        new_moment[...] = m
        new_second[...] = v
        update[...] = m / (jnp.sqrt(v) + ADAM_EPS)

    for j in range(3):
        adam(grads[j], mq[j], vq[j], new_mq.at[j], new_vq.at[j], up_q.at[j])
    adam(grads[3], mo[...], vo[...], new_mo, new_vo, up_o)
    loss[...] = totals[1:2, 0:1] / (SAMPLES * LATENT)


def adam_update(grads, totals, moment_qkv, second_qkv, moment_out, second_out):
    vmem = pl.BlockSpec(memory_space=pltpu.VMEM)
    mq, vq = (jnp.moveaxis(v, 1, 0) for v in (moment_qkv, second_qkv))
    qkv, out = (jax.ShapeDtypeStruct(v.shape, v.dtype) for v in (mq, moment_out))
    *news, loss = pl.pallas_call(
        adam_kernel,
        out_shape=(qkv, qkv, qkv, out, out, out, jax.ShapeDtypeStruct((1, 1), jnp.float32)),
        in_specs=[vmem] * 6,
        out_specs=(vmem,) * 7,
    )(grads, totals, mq, vq, moment_out, second_out)
    return (*(jnp.moveaxis(v, 0, 1) for v in news[:3]), *news[3:], loss.reshape(()))


def per_device(
    clean_latent,
    noise_draw,
    timestep,
    bucket,
    bucket_weights,
    teacher_embed,
    teacher_final,
    teacher_mod,
    teacher_qkv,
    teacher_out,
    student_embed,
    student_final,
    student_mod,
    student_qkv,
    student_out,
    moment_qkv,
    second_qkv,
    moment_out,
    second_out,
):
    shaped, proj, packed, loss_part = whole_step(
        timestep,
        bucket,
        bucket_weights,
        clean_latent,
        noise_draw,
        (teacher_embed, teacher_final, teacher_mod, teacher_qkv, teacher_out),
        (student_embed, student_final, student_mod, student_qkv, student_out),
    )
    grads, totals = reduce_gradients(shaped, proj, packed, loss_part)
    return adam_update(grads, totals, moment_qkv, second_qkv, moment_out, second_out)


def solution(mesh):
    torus = Mesh(
        mesh.devices.reshape(4, 4, 2, 2, mesh.shape["mp"]), ("dp_0", "dp_1", "dp_2", "dp_3", "mp")
    )
    in_specs = (
        P(DP, None),
        P(DP, None),
        P(DP),
        P(DP),
        P(),
        P(),
        P(),
        P(),
        P(None, None, "mp"),
        P(None, "mp"),
        P(),
        P(),
        P(),
        P(DP, None, "mp"),
        P(DP, "mp"),
        P(DP, None, "mp"),
        P(DP, None, "mp"),
        P(DP, "mp"),
        P(DP, "mp"),
    )
    out_specs = (
        P(DP, None, "mp"),
        P(DP, None, "mp"),
        P(DP, None, "mp"),
        P(DP, "mp"),
        P(DP, "mp"),
        P(DP, "mp"),
        P(),
    )
    return jax.shard_map(
        per_device, mesh=torus, in_specs=in_specs, out_specs=out_specs, check_vma=False
    )
```

```python
import math

import jax
import jax.numpy as jnp
import numpy as np
from jax import lax
from jax.experimental import pallas as pl
from jax.experimental.pallas import tpu as pltpu
from jax.sharding import Mesh
from jax.sharding import PartitionSpec as P

D = 2048
HS = 64
INNER = 1024
PATCH_CH = 16
SEQ = 256
LATENT = 4096
SAMPLES = 64
K = 8
TGRID = 16
NBUCKET = 8
DP = ("dp_0", "dp_1", "dp_2", "dp_3")
DP_MP = ("dp_0", "dp_1", "dp_2", "dp_3", "mp")


LN_EPS = 0.01
BETA_ONE = 0.9
BETA_TWO = 0.99
ADAM_EPS = 1e-08


ROWS = 1024
HALF = 1024
CODES = 32767.0
AXES = ("dp_0", "dp_1", "dp_2", "dp_3", "mp")


def remote(src, dst, send, recv, axis, target):
    return pltpu.make_async_remote_copy(
        src_ref=src,
        dst_ref=dst,
        send_sem=send,
        recv_sem=recv,
        device_id={axis: target} if isinstance(axis, str) else dict(zip(axis, target)),
        device_id_type=pl.DeviceIdType.MESH,
    )


def greet(friends):
    barrier = pltpu.get_barrier_semaphore()
    for axis, target in friends:
        pl.semaphore_signal(
            barrier,
            inc=1,
            device_id={axis: target} if isinstance(axis, str) else dict(zip(axis, target)),
            device_id_type=pl.DeviceIdType.MESH,
        )
    pl.semaphore_wait(barrier, len(friends))


def all_places():
    y, x, z, core, mp = (lax.axis_index(a) for a in AXES)
    axes, here = ("mp", "dp_2", "dp_3"), (mp, z, core)
    cube = []
    for k in range(1, 8):
        cube.append((axes, tuple(1 - h if k >> n & 1 else h for n, h in enumerate(here))))
    return [
        (4 * mp + 2 * z + core, cube),
        (x, [("dp_1", lax.rem(x + k, 4)) for k in (1, 2, 3)]),
        (y, [("dp_0", lax.rem(y + k, 4)) for k in (1, 2, 3)]),
    ]


def sum_over_all(value, inbox, send, recv):
    for stage, (slot, partners) in enumerate(all_places()):
        inbox[stage, slot] = value
        copies = [
            remote(
                inbox.at[stage, slot],
                inbox.at[stage, slot],
                send.at[stage, k],
                recv.at[stage, k],
                axis,
                target,
            )
            for k, (axis, target) in enumerate(partners)
        ]
        for c in copies:
            c.start()
        for c in copies:
            c.wait_recv()
        value = inbox[stage, 0]
        for k in range(1, len(partners) + 1):
            value = value + inbox[stage, k]
        for c in copies:
            c.wait_send()
    return value


def by_columns(body):
    def step(n, carry):
        body(pl.ds(pl.multiple_of(n * 256, 256), 256))
        return carry

    lax.fori_loop(0, HALF // 256, step, 0)


def ring_reduce(axis, part, codes, scales, boxes, box_scales, send, recv):
    me = lax.axis_index(axis)
    right, left, far = (lax.rem(me + k, 4) for k in (1, 3, 2))
    half = part.shape[1] // 2
    top, low = pl.ds(0, half), pl.ds(half, half)

    def decoded(k, cols):
        return boxes[k, :, cols].astype(jnp.int32).astype(jnp.float32) * box_scales[k, :, cols]

    def encode(k, value):
        def body(cols):
            v = value(cols)
            peak = jnp.maximum(jnp.max(jnp.abs(v), axis=0, keepdims=True), 1e-30)
            code = lax.round(v * (CODES / peak), lax.RoundingMethod.TO_NEAREST_EVEN)
            codes[k, :, cols] = code.astype(jnp.int32).astype(jnp.int16)
            scales[k, :, cols] = peak * (1.0 / CODES)

        by_columns(body)

    def message(k):
        target = left if k % 2 else right
        return [
            remote(codes.at[k], boxes.at[k], send.at[k, 0], recv.at[k, 0], axis, target),
            remote(scales.at[k], box_scales.at[k], send.at[k, 1], recv.at[k, 1], axis, target),
        ]

    def post(k, value):
        encode(k, value)
        for c in message(k):
            c.start()

    def arrived(*which):
        for k in which:
            for c in message(k):
                c.wait_recv()

    def start():
        post(0, lambda cols: part[far, top, cols])
        post(1, lambda cols: part[far, low, cols])
        post(2, lambda cols: part[right, low, cols])
        post(3, lambda cols: part[left, top, cols])

    def relay():
        arrived(0)
        post(4, lambda cols: part[right, top, cols] + decoded(0, cols))
        arrived(1)
        post(5, lambda cols: part[left, low, cols] + decoded(1, cols))

    def finish(store):
        arrived(3, 4)
        by_columns(lambda cols: store(0, cols, part[me, top, cols] + decoded(3, cols) + decoded(4, cols)))
        arrived(2, 5)
        by_columns(lambda cols: store(1, cols, part[me, low, cols] + decoded(2, cols) + decoded(5, cols)))
        for k in range(6):
            for c in message(k):
                c.wait_send()

    return start, relay, finish


def reduce_kernel(
    shaped,
    proj,
    packed,
    loss_part,
    out,
    totals,
    shaped_in,
    proj_in,
    packed_in,
    part_a,
    part_b,
    part_c,
    part_d,
    *rest,
):
    boxes = [rest[4 * k : 4 * k + 4] for k in range(4)]
    last, last_in, pair_send, pair_recv, send, recv, z_send, z_recv = rest[16:24]
    inbox, sum_send, sum_recv = rest[24:]
    y, x, z, core = (lax.axis_index(a) for a in AXES[:4])
    greet([friend for _, partners in all_places() for friend in partners])
    pair = [
        remote(a, b, pair_send.at[k], pair_recv.at[k], "dp_3", 1 - core)
        for k, (a, b) in enumerate(
            [(packed, packed_in), (shaped.at[:, 1 - core], shaped_in), (proj.at[:, 1 - core], proj_in)]
        )
    ]
    for c in pair:
        c.start()

    def products(s_ref, p_ref, b_ref, add):
        def step(k, carry):
            rows = pl.ds(pl.multiple_of(k * 8, 8), 8)
            s, p = (r[rows].reshape(256, SEQ) for r in (s_ref, p_ref))
            g = jnp.dot(s, b_ref[:, :HALF], preferred_element_type=jnp.float32)
            for j in range(4):
                block = g[64 * j : 64 * j + 64]
                spot = pl.ds(pl.multiple_of(k * 64, 64), 64)
                part_a[j, spot] = part_a[j, spot] + block if add else block
            h = jnp.dot(s, b_ref[:, HALF : HALF + 512], preferred_element_type=jnp.float32)
            part_b[k, :, 0:512] = part_b[k, :, 0:512] + h if add else h
            o = jnp.dot(p, b_ref[:, HALF + 512 :], preferred_element_type=jnp.float32)
            part_b[k, :, 512:1024] = part_b[k, :, 512:1024] + o if add else o
            return carry

        lax.fori_loop(0, 4, step, 0)

    products(shaped.at[:, core], proj.at[:, core], packed, False)
    for c in pair:
        c.wait_recv()
    products(shaped_in, proj_in, packed_in, True)

    rings = [
        ring_reduce(axis, part, *boxes[k], send.at[k], recv.at[k])
        for k, (axis, part) in enumerate(
            [("dp_1", part_a), ("dp_0", part_b), ("dp_0", part_c), ("dp_1", part_d)]
        )
    ]

    def into(part):
        def store(which, cols, value):
            part[2 * which, :, cols] = value[:64]
            part[2 * which + 1, :, cols] = value[64:]

        return store

    rings[0][0]()
    rings[1][0]()
    rings[0][1]()
    rings[1][1]()
    rings[0][2](into(part_c))
    rings[2][0]()
    rings[1][2](into(part_d))
    rings[3][0]()
    rings[2][1]()
    rings[3][1]()
    z_copies = []
    for k in range(2):

        def store(which, cols, value, k=k):
            last[k, which, :, cols] = value

        rings[2 + k][2](store)
        c = remote(
            last.at[k, 1 - z], last_in.at[k], z_send.at[k], z_recv.at[k], "dp_2", 1 - z
        )
        c.start()
        z_copies.append(c)
    for k, c in enumerate(z_copies):
        c.wait_recv()
        both = last[k, z] + last_in[k]
        out[2 * k] = both[:, :512]
        out[2 * k + 1] = both[:, 512:]
    for c in [*pair, *z_copies]:
        c.wait_send()
    squares = jnp.sum(out[...] * out[...])
    row = lax.broadcasted_iota(jnp.int32, (8, 128), 0)
    value = jnp.where(row == 0, squares, loss_part[...])
    totals[...] = sum_over_all(value, inbox, sum_send, sum_recv)


def reduce_gradients(shaped, proj, packed, loss_part):
    vmem = pl.BlockSpec(memory_space=pltpu.VMEM)

    def boxes(half):
        return [pltpu.VMEM((6, half, HALF), jnp.int16), pltpu.VMEM((6, 1, HALF), jnp.float32)] * 2

    return pl.pallas_call(
        reduce_kernel,
        out_shape=(
            jax.ShapeDtypeStruct((4, 32, 512), jnp.float32),
            jax.ShapeDtypeStruct((8, 128), jnp.float32),
        ),
        in_specs=[vmem] * 4,
        out_specs=(vmem, vmem),
        scratch_shapes=[
            pltpu.VMEM((32, 32, SEQ), jnp.bfloat16),
            pltpu.VMEM((32, 32, SEQ), jnp.bfloat16),
            pltpu.VMEM((SEQ, 2 * HALF), jnp.bfloat16),
            pltpu.VMEM((4, 256, HALF), jnp.float32),
            pltpu.VMEM((4, 256, HALF), jnp.float32),
            pltpu.VMEM((4, 64, HALF), jnp.float32),
            pltpu.VMEM((4, 64, HALF), jnp.float32),
            *boxes(128),
            *boxes(128),
            *boxes(32),
            *boxes(32),
            pltpu.VMEM((2, 2, 32, HALF), jnp.float32),
            pltpu.VMEM((2, 32, HALF), jnp.float32),
            pltpu.SemaphoreType.DMA((3,)),
            pltpu.SemaphoreType.DMA((3,)),
            pltpu.SemaphoreType.DMA((4, 6, 2)),
            pltpu.SemaphoreType.DMA((4, 6, 2)),
            pltpu.SemaphoreType.DMA((2,)),
            pltpu.SemaphoreType.DMA((2,)),
            pltpu.VMEM((3, 8, 8, 128), jnp.float32),
            pltpu.SemaphoreType.DMA((3, 7)),
            pltpu.SemaphoreType.DMA((3, 7)),
        ],
        compiler_params=pltpu.CompilerParams(
            collective_id=1, has_side_effects=True, vmem_limit_bytes=60 * 2**20
        ),
    )(shaped, proj, packed, loss_part)


TOKENS = 256
UNROLL = 4
WIDE = 256
NT = (((1,), (1,)), ((), ()))
TN = (((0,), (0,)), ((), ()))


def dot(a, b, dims=(((1,), (0,)), ((), ()))):
    return lax.dot_general(a, b, dims, preferred_element_type=jnp.float32)


def gather_stream(held, slabs, send, recv):
    y, x, z, core = (lax.axis_index(a) for a in AXES[:4])
    near = {"dp_0": [lax.rem(y + k, 4) for k in (1, 3)], "dp_1": [lax.rem(x + k, 4) for k in (1, 3)]}
    every = slice(None)
    live = []

    def go(spot, k, axis, target):
        ref = held.at[(slabs, *spot)]
        c = remote(ref, ref, send.at[k], recv.at[k], axis, target)
        c.start()
        live.append(c)
        return c

    def ring_direct(first):
        for half, axis in enumerate(("dp_1", "dp_0") if first else ("dp_0", "dp_1")):
            if first:
                spot = (y, x, every, core, half)
            elif half == 0:
                spot = (y, every, every, core, half)
            else:
                spot = (every, x, every, core, half)
            for side in range(2):
                k = (1 if first else 9) + 4 * half + side
                go(spot, k, axis, near[axis][side])

    def ring_relay(first):
        base = 1 if first else 9
        direct = live[-4:]
        for half, axis in enumerate(("dp_1", "dp_0") if first else ("dp_0", "dp_1")):
            for side in range(2):
                direct[2 * half + side].wait_recv()
                back = near[axis][1 - side]
                if first:
                    spot = (y, back) if axis == "dp_1" else (back, x)
                else:
                    spot = (every, back) if axis == "dp_1" else (back, every)
                go((*spot, side, core, half), base + 4 * half + 2 + side, axis, near[axis][side])

    def across(k, spot):
        go((*spot[:3], core, spot[3]), k, "dp_3", 1 - core)

    def step(k):
        if k == 0:
            go((y, x, z, core), 0, "dp_2", 1 - z)
        elif k == 1:
            live[-1].wait_recv()
            ring_direct(True)
        elif k == 2:
            ring_relay(True)
        elif k == 3:
            for c in live[-4:]:
                c.wait_recv()
            ring_direct(False)
        elif k == 4:
            ring_relay(False)
            relays.extend(live[-4:])
            across(17, (y, every, every, 0))
            across(18, (every, x, every, 1))
            for n in range(2):
                across(19 + 2 * n, (near["dp_0"][n], every, every, 0))
                across(20 + 2 * n, (every, near["dp_1"][n], every, 1))
        elif k == 5:
            for c in relays:
                c.wait_recv()
            across(23, (lax.rem(y + 2, 4), every, every, 0))
            across(24, (every, lax.rem(x + 2, 4), every, 1))
        else:
            for c in live[-8:]:
                c.wait_recv()
            for c in live:
                c.wait_send()

    relays = []
    return step


def gather_direct(held, slab, send, recv):
    y, x, z, core = (lax.axis_index(a) for a in AXES[:4])
    every = slice(None)
    live = []

    def ring(spots, base):
        for half, (axis, spot) in enumerate(spots):
            me = lax.axis_index(axis)
            for k in (1, 2, 3):
                ref = held.at[(slab, *spot, core, half)]
                n = base + 3 * half + k - 1
                c = remote(ref, ref, send.at[n], recv.at[n], axis, lax.rem(me + k, 4))
                c.start()
                live.append(c)

    def step(k):
        if k == 0:
            ring([("dp_1", (y, x, every)), ("dp_0", (y, x, every))], 0)
        elif k == 1:
            for c in live:
                c.wait_recv()
            ring([("dp_0", (y, every, every)), ("dp_1", (every, x, every))], 6)
        elif k == 2:
            for c in live[6:]:
                c.wait_recv()
            ref = held.at[slab, :, :, :, core]
            c = remote(ref, ref, send.at[12], recv.at[12], "dp_3", 1 - core)
            c.start()
            live.append(c)
        else:
            live[-1].wait_recv()
            for c in live:
                c.wait_send()

    return step


def three_terms(v8):
    high = v8.astype(jnp.bfloat16).astype(jnp.float32)
    rest = v8 - high
    middle = rest.astype(jnp.bfloat16).astype(jnp.float32)
    low = rest - middle
    group = lax.broadcasted_iota(jnp.int32, v8.shape, 1) // 16
    picked = jnp.where(
        (group == 0) | (group == 1) | (group == 3),
        high,
        jnp.where((group == 2) | (group == 5), middle, jnp.where(group == 4, low, 0.0)),
    )
    return picked.astype(jnp.bfloat16)


def picked_level(step, offset, values):
    out = jnp.float32(0.0)
    for k in range(1, K + 1):
        out = jnp.where(step == k, jnp.float32(values[2 * k + offset]), out)
    return out


def step_kernel(
    timestep,
    bucket,
    bucket_weights,
    clean8,
    noise8,
    tables,
    teacher_embed,
    teacher_final,
    teacher_mod,
    student_embed,
    student_final,
    student_mod,
    teacher_qkv,
    teacher_out,
    student_qkv,
    student_out,
    shaped_t,
    proj_t,
    packed,
    loss_part,
    held,
    near_qkv,
    placed,
    hidden,
    hidden_s,
    mixed,
    shaped,
    shaped_s,
    qkv,
    heads,
    heads_in,
    weights,
    terms,
    inverses,
    d_attn,
    embed_t,
    embed_s,
    back_s,
    final_t,
    final_s,
    qkv_sem,
    swap_send,
    swap_recv,
    t_send,
    t_recv,
    s_send,
    s_recv,
):
    y, x, z, core, mp = (lax.axis_index(a) for a in AXES)
    load = pltpu.make_async_copy(teacher_qkv, near_qkv, qkv_sem)
    load.start()
    held[0:3, y, x, z, core] = student_qkv[...]
    held[3, y, x, z, core] = student_out[...]
    both = ("dp_2", "mp")
    friends = [("dp_3", 1 - core), ("dp_2", 1 - z), ("mp", 1 - mp), (both, (1 - z, 1 - mp))]
    friends += [("dp_1", lax.rem(x + k, 4)) for k in (1, 2, 3)]
    friends += [("dp_0", lax.rem(y + k, 4)) for k in (1, 2, 3)]
    greet(friends)

    def swap(src, dst, k, axis="mp", target=None):
        target = 1 - mp if target is None else target
        return remote(src, dst, swap_send.at[k], swap_recv.at[k], axis, target)

    spot = (y, x, z, core)
    here = teacher_out.at[spot]
    swaps = [
        swap(here, held.at[(5, *spot)], 0),
        swap(here, held.at[(5, *spot)], 1, both, (1 - z, 1 - mp)),
        swap(student_out, held.at[(4, *spot)], 2),
    ]
    for c in swaps:
        c.start()
    t_step = gather_direct(held, 5, t_send, t_recv)
    s_step = gather_stream(held, pl.ds(0, 5), s_send, s_recv)

    step = timestep[0]
    a_f, a_m, a_l = (picked_level(step, -k, ALPHAS) for k in range(3))
    s_f, s_m, s_l = (picked_level(step, -k, SIGMAS) for k in range(3))
    row_weight = bucket_weights[jnp.clip(bucket[0], 0, NBUCKET - 1)]
    places = [
        (teacher_mod, jnp.clip(2 * step - 1, 0, TGRID - 1)),
        (teacher_mod, jnp.clip(2 * step - 2, 0, TGRID - 1)),
        (student_mod, jnp.clip(step - 1, 0, K - 1)),
    ]
    modrows = [[mod[j, pl.ds(at, 1), :] for j in range(3)] for mod, at in places]

    def split_rows(ref):
        v = ref[...]
        h = v.astype(jnp.bfloat16)
        rest = v - h.astype(jnp.float32)
        m = rest.astype(jnp.bfloat16)
        return h, m, (rest - m.astype(jnp.float32)).astype(jnp.bfloat16)

    def stack(parts, out):
        h, m, l = parts
        for k, v in enumerate([h, m, h, l, h, m, jnp.zeros_like(h), jnp.zeros_like(h)]):
            out[16 * k : 16 * k + 16] = v

    def repeat(parts, out):
        for k in range(24):
            out[16 * k : 16 * k + 16] = parts[k // 8]

    def columns(k, width):
        return pl.ds(pl.multiple_of(k * width, width), width)

    def spread(v8, b_ref, out, base=None):
        terms8 = three_terms(v8)

        def body(n, carry):
            cols = columns(n, WIDE)
            h = dot(terms8, b_ref[:, cols])
            out[:, cols] = h if base is None else h + base[:, cols]
            return carry

        lax.fori_loop(0, D // WIDE, body, 0)

    def centred(v):
        c = v - jnp.mean(v, axis=-1, keepdims=True)
        return c, lax.rsqrt(jnp.mean(c * c, axis=-1, keepdims=True) + LN_EPS)

    def by_rows(body):
        def group(n, carry):
            for u in range(UNROLL):
                body(pl.ds(pl.multiple_of(n * (16 * UNROLL) + 16 * u, 16), 16))
            return carry

        lax.fori_loop(0, TOKENS // (16 * UNROLL), group, 0)

    def shape(hid, which, out):
        shift, scale = modrows[which][0], 1.0 + modrows[which][1]

        def body(rows):
            c, inv = centred(hid[rows])
            out[rows] = (c * inv * scale + shift).astype(jnp.bfloat16)

        by_rows(body)

    def project(src, weight):
        def body(j, carry):
            qkv[j] = dot(src[...], weight(j)).astype(jnp.bfloat16)
            return carry

        lax.fori_loop(0, 3, body, 0)

    lane = lax.broadcasted_iota(jnp.int32, (1, 128), 1)
    low_f = jnp.where(lane < 64, 1.0, 0.0)
    sides = [low_f.astype(jnp.bfloat16), (1.0 - low_f).astype(jnp.bfloat16)]
    is_low = lax.broadcasted_iota(jnp.int32, (TOKENS, 128), 1) < 64

    def swap_pair(which, hp):
        cols = pl.ds(128 * hp, 128)
        return swap(heads.at[which, :, cols], heads_in.at[which, :, cols], 3 + 4 * which + hp)

    def attend(which, keep):
        for hp in range(4):
            cols = pl.ds(128 * hp, 128)
            q, k, v = qkv[0, :, cols], qkv[1, :, cols], qkv[2, :, cols]
            outs = []
            for h in range(2):
                s = dot(q * sides[h], k, NT) * 0.125
                e = jnp.exp(s - jnp.max(s, axis=-1, keepdims=True))
                w = e / jnp.sum(e, axis=-1, keepdims=True)
                if keep:
                    weights[2 * hp + h] = w
                outs.append(dot(w.astype(jnp.bfloat16), v))
            heads[which, :, cols] = jnp.where(is_low, outs[0], outs[1]).astype(jnp.bfloat16)
            if hp > 0:
                swap_pair(which, hp - 1).start()
        swap_pair(which, 3).start()

    def swapped(which):
        for hp in range(4):
            swap_pair(which, hp).wait_recv()

    def mix(att, weight, which, base):
        mod_ref, at = places[which]

        def body(n, carry):
            cols = columns(n, 512)
            p = dot(att[...], weight(n), NT)
            mixed[:, cols] = base[:, cols] + mod_ref[2, pl.ds(at, 1), cols] * p
            return carry

        lax.fori_loop(0, 4, body, 0)

    def predict(final, keep):
        def body(rows):
            c, inv = centred(mixed[rows])
            u = c * inv
            if keep:
                placed[rows] = u
                inverses[rows] = jnp.broadcast_to(inv, (16, 128))
            high = u.astype(jnp.bfloat16)
            rest = u - high.astype(jnp.float32)
            middle = rest.astype(jnp.bfloat16)
            terms[0, rows] = high
            terms[1, rows] = middle
            terms[2, rows] = (rest - middle.astype(jnp.float32)).astype(jnp.bfloat16)

        by_rows(body)
        r = dot(terms[0], final[...], NT)
        m = dot(terms[1], final[0:256], NT)
        small = dot(terms[2], final[0:128], NT)
        return (
            r[:, 0:128]
            + (r[:, 128:256] + m[:, 0:128])
            + (r[:, 256:384] + m[:, 128:256] + small)
        )

    def other_rows(slab):
        return lambda n: held[slab, n].reshape(512, 512)

    def near_rows(n):
        return teacher_out[n].reshape(512, 512)

    def turn(src, out):
        def body(n, carry):
            t = src[:, columns(n, 128)].astype(jnp.float32).T.astype(jnp.bfloat16)
            out[pl.ds(2 * n, 2)] = t.reshape(2, 2, 32, TOKENS)
            return carry

        lax.fori_loop(0, D // 128, body, 0)

    half = D // 2
    for k in range(16):
        sin_a, cos_a = tables[0, k : k + 1], tables[1, k : k + 1]
        rows = pl.ds(16 * k, 16)
        placed[rows, :half] = sin_a * tables[3] + cos_a * tables[2]
        placed[rows, half:] = cos_a * tables[3] - sin_a * tables[2]
    stack(split_rows(teacher_embed), embed_t)
    lat0 = a_f * clean8[...] + s_f * noise8[...]
    spread(lat0, embed_t, hidden, placed)
    swaps[0].wait_recv()
    swaps[1].wait_recv()
    t_step(0)
    swaps[2].wait_recv()
    s_step(0)
    shape(hidden, 0, shaped)
    load.wait()
    project(shaped, lambda j: near_qkv[j])
    t_step(1)
    s_step(1)
    attend(0, False)
    t_step(2)
    s_step(2)
    mix(heads.at[0], near_rows, 0, hidden)
    stack(split_rows(student_embed), embed_s)
    repeat(split_rows(teacher_final), final_t)
    spread(lat0, embed_s, hidden_s, placed)
    t_step(3)
    s_step(3)
    swapped(0)
    mix(heads_in.at[0], other_rows(5), 0, mixed)
    eps0 = predict(final_t, False)
    lat1 = a_m * (lat0 - s_f * eps0) / a_f + s_m * eps0

    spread(lat1, embed_t, hidden, placed)
    shape(hidden, 1, shaped)
    project(shaped, lambda j: near_qkv[j])
    attend(1, False)
    mix(heads.at[1], near_rows, 1, hidden)
    shape(hidden_s, 2, shaped_s)
    s_step(4)
    swapped(1)
    mix(heads_in.at[1], other_rows(5), 1, mixed)
    eps1 = predict(final_t, False)
    lat2 = a_l * (lat1 - s_m * eps1) / a_m + s_l * eps1
    target = (lat0 - a_f / a_l * lat2) / (s_f - a_f * s_l / a_l)

    s_step(5)
    turn(shaped_s, shaped_t)
    student_terms = split_rows(student_final)
    repeat(student_terms, final_s)
    stack(student_terms, back_s)
    s_step(6)
    project(shaped_s, lambda j: held[j].reshape(D, 512))
    attend(2, True)
    mix(heads.at[2], other_rows(3), 2, hidden_s)
    swapped(2)
    mix(heads_in.at[2], other_rows(4), 2, mixed)
    error = predict(final_s, True) - target
    lanes = lax.broadcasted_iota(jnp.int32, error.shape, 1)
    loss_part[...] = jnp.full(
        (8, 128), 0.5 * row_weight * jnp.sum(jnp.where(lanes < 16, error * error, 0.0))
    )

    spread(2.0 * row_weight * error, back_s, hidden)

    gate = modrows[2][2]

    def back(rows):
        up, u = hidden[rows], placed[rows]
        first_mean = jnp.mean(up, axis=-1, keepdims=True)
        second_mean = jnp.mean(up * u, axis=-1, keepdims=True)
        d = (up - first_mean - u * second_mean) * inverses[rows, 0:1]
        shaped[rows] = (gate * d).astype(jnp.bfloat16)

    by_rows(back)
    d_attn[...] = dot(shaped[...], held[3].reshape(D, 512)).astype(jnp.bfloat16)

    def back_heads(hp, carry):
        cols = columns(hp, 128)
        q, k, v, da = qkv[0, :, cols], qkv[1, :, cols], qkv[2, :, cols], d_attn[:, cols]
        outs = []
        for h in range(2):
            w = weights[2 * hp + h]
            dp = dot(da * sides[h], v, NT)
            ds = w * (dp - jnp.sum(w * dp, axis=-1, keepdims=True)) * 0.125
            ds = ds.astype(jnp.bfloat16)
            outs.append((dot(ds, k), dot(ds, q, TN), dot(w.astype(jnp.bfloat16), da, TN)))
        for j in range(3):
            spot = pl.ds(pl.multiple_of(j * 512 + hp * 128, 128), 128)
            both = jnp.where(is_low, outs[0][j], outs[1][j])
            packed[:, spot] = both.astype(jnp.bfloat16)
        packed[:, pl.ds(pl.multiple_of(1536 + hp * 128, 128), 128)] = heads[2, :, cols]
        return carry

    lax.fori_loop(0, 4, back_heads, 0)
    turn(shaped, proj_t)
    for c in swaps:
        c.wait_send()
    for which in range(3):
        for hp in range(4):
            swap_pair(which, hp).wait_send()


def levels():
    lamb = 6.0 - 12.0 * np.arange(TGRID + 1) / TGRID
    return [np.sqrt(1.0 / (1.0 + np.exp(sign * lamb))).astype(np.float32) for sign in (-1.0, 1.0)]


ALPHAS, SIGMAS = levels()


def position_tables():
    half = D // 2
    freqs = np.exp(-math.log(10000.0) * np.arange(half) / half)
    fine = np.arange(16)[:, None] * freqs[None]
    angles = (np.sin(16.0 * fine), np.cos(16.0 * fine), np.sin(fine), np.cos(fine))
    return np.stack(angles).astype(np.float32)


def whole_step(timestep, bucket, bucket_weights, clean, noise, teacher, student):
    vmem, smem = (pl.BlockSpec(memory_space=m) for m in (pltpu.VMEM, pltpu.SMEM))
    bf16, f32 = jnp.bfloat16, jnp.float32

    def tiled(v):
        return jnp.tile(v.reshape(SEQ, PATCH_CH), (1, 8))

    return pl.pallas_call(
        step_kernel,
        out_shape=(
            jax.ShapeDtypeStruct((32, 2, 32, TOKENS), bf16),
            jax.ShapeDtypeStruct((32, 2, 32, TOKENS), bf16),
            jax.ShapeDtypeStruct((TOKENS, D), bf16),
            jax.ShapeDtypeStruct((8, 128), f32),
        ),
        in_specs=[smem] * 3 + [vmem] * 9 + [pl.BlockSpec(memory_space=pl.ANY)] + [vmem] * 3,
        out_specs=(vmem,) * 4,
        scratch_shapes=[
            pltpu.VMEM((6, 4, 4, 2, 2, 2, 16, 512), bf16),
            pltpu.VMEM((3, D, 512), bf16),
            pltpu.VMEM((TOKENS, D), f32),
            pltpu.VMEM((TOKENS, D), f32),
            pltpu.VMEM((TOKENS, D), f32),
            pltpu.VMEM((TOKENS, D), f32),
            pltpu.VMEM((TOKENS, D), bf16),
            pltpu.VMEM((TOKENS, D), bf16),
            pltpu.VMEM((3, TOKENS, 512), bf16),
            pltpu.VMEM((3, TOKENS, 512), bf16),
            pltpu.VMEM((3, TOKENS, 512), bf16),
            pltpu.VMEM((8, TOKENS, TOKENS), f32),
            pltpu.VMEM((3, TOKENS, D), bf16),
            pltpu.VMEM((TOKENS, 128), f32),
            pltpu.VMEM((TOKENS, 512), bf16),
            pltpu.VMEM((128, D), bf16),
            pltpu.VMEM((128, D), bf16),
            pltpu.VMEM((128, D), bf16),
            pltpu.VMEM((384, D), bf16),
            pltpu.VMEM((384, D), bf16),
            pltpu.SemaphoreType.DMA,
            pltpu.SemaphoreType.DMA((15,)),
            pltpu.SemaphoreType.DMA((15,)),
            pltpu.SemaphoreType.DMA((13,)),
            pltpu.SemaphoreType.DMA((13,)),
            pltpu.SemaphoreType.DMA((25,)),
            pltpu.SemaphoreType.DMA((25,)),
        ],
        compiler_params=pltpu.CompilerParams(
            collective_id=2, has_side_effects=True, vmem_limit_bytes=62 * 2**20
        ),
    )(
        timestep,
        bucket,
        bucket_weights,
        tiled(clean),
        tiled(noise),
        jnp.asarray(position_tables()),
        teacher[0],
        teacher[1],
        jnp.moveaxis(teacher[2], 1, 0),
        student[0],
        student[1],
        jnp.moveaxis(student[2], 1, 0),
        jnp.moveaxis(teacher[3], 1, 0),
        teacher[4].reshape(4, 4, 2, 2, 2, 16, 512),
        jnp.moveaxis(student[3], 1, 0).reshape(3, 2, 16, 512),
        student[4].reshape(2, 16, 512),
    )


def adam_kernel(grads, totals, mq, vq, mo, vo, new_mq, new_vq, up_q, new_mo, new_vo, up_o, loss):
    rms = jnp.sqrt(totals[0:1, 0:1] / (4 * D * INNER))
    factor = 1.0 / jnp.maximum(rms, 1.0)

    def adam(grad, moment, second, new_moment, new_second, update):
        normed = grad * factor
        m = BETA_ONE * moment + (1.0 - BETA_ONE) * normed
        v = BETA_TWO * second + (1.0 - BETA_TWO) * normed * normed
        new_moment[...] = m
        new_second[...] = v
        update[...] = m / (jnp.sqrt(v) + ADAM_EPS)

    for j in range(3):
        adam(grads[j], mq[j], vq[j], new_mq.at[j], new_vq.at[j], up_q.at[j])
    adam(grads[3], mo[...], vo[...], new_mo, new_vo, up_o)
    loss[...] = totals[1:2, 0:1] / (SAMPLES * LATENT)


def adam_update(grads, totals, moment_qkv, second_qkv, moment_out, second_out):
    vmem = pl.BlockSpec(memory_space=pltpu.VMEM)
    mq, vq = (jnp.moveaxis(v, 1, 0) for v in (moment_qkv, second_qkv))
    qkv, out = (jax.ShapeDtypeStruct(v.shape, v.dtype) for v in (mq, moment_out))
    *news, loss = pl.pallas_call(
        adam_kernel,
        out_shape=(qkv, qkv, qkv, out, out, out, jax.ShapeDtypeStruct((1, 1), jnp.float32)),
        in_specs=[vmem] * 6,
        out_specs=(vmem,) * 7,
    )(grads, totals, mq, vq, moment_out, second_out)
    return (*(jnp.moveaxis(v, 0, 1) for v in news[:3]), *news[3:], loss.reshape(()))


def per_device(
    clean_latent,
    noise_draw,
    timestep,
    bucket,
    bucket_weights,
    teacher_embed,
    teacher_final,
    teacher_mod,
    teacher_qkv,
    teacher_out,
    student_embed,
    student_final,
    student_mod,
    student_qkv,
    student_out,
    moment_qkv,
    second_qkv,
    moment_out,
    second_out,
):
    shaped, proj, packed, loss_part = whole_step(
        timestep,
        bucket,
        bucket_weights,
        clean_latent,
        noise_draw,
        (teacher_embed, teacher_final, teacher_mod, teacher_qkv, teacher_out),
        (student_embed, student_final, student_mod, student_qkv, student_out),
    )
    grads, totals = reduce_gradients(shaped, proj, packed, loss_part)
    return adam_update(grads, totals, moment_qkv, second_qkv, moment_out, second_out)


def solution(mesh):
    torus = Mesh(
        mesh.devices.reshape(4, 4, 2, 2, mesh.shape["mp"]), ("dp_0", "dp_1", "dp_2", "dp_3", "mp")
    )
    in_specs = (
        P(DP, None),
        P(DP, None),
        P(DP),
        P(DP),
        P(),
        P(),
        P(),
        P(),
        P(None, None, "mp"),
        P(None, "mp"),
        P(),
        P(),
        P(),
        P(DP, None, "mp"),
        P(DP, "mp"),
        P(DP, None, "mp"),
        P(DP, None, "mp"),
        P(DP, "mp"),
        P(DP, "mp"),
    )
    out_specs = (
        P(DP, None, "mp"),
        P(DP, None, "mp"),
        P(DP, None, "mp"),
        P(DP, "mp"),
        P(DP, "mp"),
        P(DP, "mp"),
        P(),
    )
    return jax.shard_map(
        per_device, mesh=torus, in_specs=in_specs, out_specs=out_specs, check_vma=False
    )
```

```python
import math

import jax
import jax.numpy as jnp
import numpy as np
from jax import lax
from jax.experimental import pallas as pl
from jax.experimental.pallas import tpu as pltpu
from jax.sharding import Mesh
from jax.sharding import PartitionSpec as P

D = 2048
HS = 64
INNER = 1024
PATCH_CH = 16
SEQ = 256
LATENT = 4096
SAMPLES = 64
K = 8
TGRID = 16
NBUCKET = 8
DP = ("dp_0", "dp_1", "dp_2", "dp_3")
DP_MP = ("dp_0", "dp_1", "dp_2", "dp_3", "mp")


LN_EPS = 0.01
BETA_ONE = 0.9
BETA_TWO = 0.99
ADAM_EPS = 1e-08


ROWS = 1024
HALF = 1024
CODES = 32767.0
AXES = ("dp_0", "dp_1", "dp_2", "dp_3", "mp")


def remote(src, dst, send, recv, axis, target):
    return pltpu.make_async_remote_copy(
        src_ref=src,
        dst_ref=dst,
        send_sem=send,
        recv_sem=recv,
        device_id={axis: target} if isinstance(axis, str) else dict(zip(axis, target)),
        device_id_type=pl.DeviceIdType.MESH,
    )


def greet(friends):
    barrier = pltpu.get_barrier_semaphore()
    for axis, target in friends:
        pl.semaphore_signal(
            barrier,
            inc=1,
            device_id={axis: target} if isinstance(axis, str) else dict(zip(axis, target)),
            device_id_type=pl.DeviceIdType.MESH,
        )
    pl.semaphore_wait(barrier, len(friends))


def all_places():
    y, x, z, core, mp = (lax.axis_index(a) for a in AXES)
    axes, here = ("mp", "dp_2", "dp_3"), (mp, z, core)
    cube = []
    for k in range(1, 8):
        cube.append((axes, tuple(1 - h if k >> n & 1 else h for n, h in enumerate(here))))
    return [
        (4 * mp + 2 * z + core, cube),
        (x, [("dp_1", lax.rem(x + k, 4)) for k in (1, 2, 3)]),
        (y, [("dp_0", lax.rem(y + k, 4)) for k in (1, 2, 3)]),
    ]


def sum_over_all(value, inbox, send, recv):
    for stage, (slot, partners) in enumerate(all_places()):
        inbox[stage, slot] = value
        copies = [
            remote(
                inbox.at[stage, slot],
                inbox.at[stage, slot],
                send.at[stage, k],
                recv.at[stage, k],
                axis,
                target,
            )
            for k, (axis, target) in enumerate(partners)
        ]
        for c in copies:
            c.start()
        for c in copies:
            c.wait_recv()
        value = inbox[stage, 0]
        for k in range(1, len(partners) + 1):
            value = value + inbox[stage, k]
        for c in copies:
            c.wait_send()
    return value


def by_columns(body):
    def step(n, carry):
        body(pl.ds(pl.multiple_of(n * 256, 256), 256))
        return carry

    lax.fori_loop(0, HALF // 256, step, 0)


def ring_reduce(axis, part, codes, scales, boxes, box_scales, send, recv):
    me = lax.axis_index(axis)
    right, left, far = (lax.rem(me + k, 4) for k in (1, 3, 2))
    half = part.shape[1] // 2
    top, low = pl.ds(0, half), pl.ds(half, half)

    def decoded(k, cols):
        return boxes[k, :, cols].astype(jnp.int32).astype(jnp.float32) * box_scales[k, :, cols]

    def encode(k, value):
        def body(cols):
            v = value(cols)
            peak = jnp.maximum(jnp.max(jnp.abs(v), axis=0, keepdims=True), 1e-30)
            code = lax.round(v * (CODES / peak), lax.RoundingMethod.TO_NEAREST_EVEN)
            codes[k, :, cols] = code.astype(jnp.int32).astype(jnp.int16)
            scales[k, :, cols] = peak * (1.0 / CODES)

        by_columns(body)

    def message(k):
        target = left if k % 2 else right
        return [
            remote(codes.at[k], boxes.at[k], send.at[k, 0], recv.at[k, 0], axis, target),
            remote(scales.at[k], box_scales.at[k], send.at[k, 1], recv.at[k, 1], axis, target),
        ]

    def post(k, value):
        encode(k, value)
        for c in message(k):
            c.start()

    def arrived(*which):
        for k in which:
            for c in message(k):
                c.wait_recv()

    def start():
        post(0, lambda cols: part[far, top, cols])
        post(1, lambda cols: part[far, low, cols])
        post(2, lambda cols: part[right, low, cols])
        post(3, lambda cols: part[left, top, cols])

    def relay():
        arrived(0)
        post(4, lambda cols: part[right, top, cols] + decoded(0, cols))
        arrived(1)
        post(5, lambda cols: part[left, low, cols] + decoded(1, cols))

    def finish(store):
        arrived(3, 4)
        by_columns(lambda cols: store(0, cols, part[me, top, cols] + decoded(3, cols) + decoded(4, cols)))
        arrived(2, 5)
        by_columns(lambda cols: store(1, cols, part[me, low, cols] + decoded(2, cols) + decoded(5, cols)))
        for k in range(6):
            for c in message(k):
                c.wait_send()

    return start, relay, finish


TOKENS = 256
UNROLL = 4
WIDE = 256
NT = (((1,), (1,)), ((), ()))
TN = (((0,), (0,)), ((), ()))


def dot(a, b, dims=(((1,), (0,)), ((), ()))):
    return lax.dot_general(a, b, dims, preferred_element_type=jnp.float32)


def gather_stream(held, slabs, send, recv, short=False):
    y, x, z, core = (lax.axis_index(a) for a in AXES[:4])
    near = {"dp_0": [lax.rem(y + k, 4) for k in (1, 3)], "dp_1": [lax.rem(x + k, 4) for k in (1, 3)]}
    every = slice(None)
    live = []

    def go(spot, k, axis, target):
        ref = held.at[(slabs, *spot)]
        c = remote(ref, ref, send.at[k], recv.at[k], axis, target)
        c.start()
        live.append(c)
        return c

    def ring_direct(first):
        for half, axis in enumerate(("dp_1", "dp_0") if first else ("dp_0", "dp_1")):
            if first:
                spot = (y, x, every, core, half)
            elif half == 0:
                spot = (y, every, every, core, half)
            else:
                spot = (every, x, every, core, half)
            for side in range(2):
                k = (1 if first else 9) + 4 * half + side
                go(spot, k, axis, near[axis][side])

    def ring_relay(first):
        base = 1 if first else 9
        direct = live[-4:]
        for half, axis in enumerate(("dp_1", "dp_0") if first else ("dp_0", "dp_1")):
            for side in range(2):
                direct[2 * half + side].wait_recv()
                back = near[axis][1 - side]
                if first:
                    spot = (y, back) if axis == "dp_1" else (back, x)
                else:
                    spot = (every, back) if axis == "dp_1" else (back, every)
                go((*spot, side, core, half), base + 4 * half + 2 + side, axis, near[axis][side])

    def across(k, spot):
        go((*spot[:3], core, spot[3]), k, "dp_3", 1 - core)

    def ring_straight():
        for half, (axis, me) in enumerate([("dp_1", x), ("dp_0", y)]):
            for k in (1, 2, 3):
                go((y, x, every, core, half), 3 * half + k - 1, axis, lax.rem(me + k, 4))

    def step(k):
        if short:
            k = k + 2
        if k == 0:
            go((y, x, z, core), 0, "dp_2", 1 - z)
        elif k == 1:
            live[-1].wait_recv()
            ring_direct(True)
        elif k == 2:
            ring_straight() if short else ring_relay(True)
        elif k == 3:
            for c in live[-6:] if short else live[-4:]:
                c.wait_recv()
            ring_direct(False)
        elif k == 4:
            ring_relay(False)
            relays.extend(live[-4:])
            across(17, (y, every, every, 0))
            across(18, (every, x, every, 1))
            for n in range(2):
                across(19 + 2 * n, (near["dp_0"][n], every, every, 0))
                across(20 + 2 * n, (every, near["dp_1"][n], every, 1))
        elif k == 5:
            for c in relays:
                c.wait_recv()
            across(23, (lax.rem(y + 2, 4), every, every, 0))
            across(24, (every, lax.rem(x + 2, 4), every, 1))
        else:
            for c in live[-8:]:
                c.wait_recv()
            for c in live:
                c.wait_send()

    relays = []
    return step


def three_terms(v8):
    high = v8.astype(jnp.bfloat16).astype(jnp.float32)
    rest = v8 - high
    middle = rest.astype(jnp.bfloat16).astype(jnp.float32)
    low = rest - middle
    group = lax.broadcasted_iota(jnp.int32, v8.shape, 1) // 16
    picked = jnp.where(
        (group == 0) | (group == 1) | (group == 3),
        high,
        jnp.where((group == 2) | (group == 5), middle, jnp.where(group == 4, low, 0.0)),
    )
    return picked.astype(jnp.bfloat16)


def eightfold(rows):
    v = jnp.broadcast_to(rows[:, None], (32, 8, 128)).reshape(TOKENS, 128)
    token = lax.broadcasted_iota(jnp.int32, v.shape, 0) % 8
    lane = lax.broadcasted_iota(jnp.int32, v.shape, 1)
    v = jnp.where(lane // 16 == token, v, 0.0)
    across = lax.broadcasted_iota(jnp.int32, (128, 128), 1) % 16
    down = lax.broadcasted_iota(jnp.int32, (128, 128), 0) % 16
    spread = jnp.where(across == down, 1.0, 0.0).astype(jnp.bfloat16)
    high = v.astype(jnp.bfloat16)
    rest = v - high.astype(jnp.float32)
    middle = rest.astype(jnp.bfloat16)
    low = (rest - middle.astype(jnp.float32)).astype(jnp.bfloat16)
    return dot(high, spread) + dot(middle, spread) + dot(low, spread)


def picked_level(step, offset, values):
    out = jnp.float32(0.0)
    for k in range(1, K + 1):
        out = jnp.where(step == k, jnp.float32(values[2 * k + offset]), out)
    return out


def step_kernel(
    timestep,
    bucket,
    bucket_weights,
    clean,
    noise,
    tables,
    teacher_embed,
    teacher_final,
    teacher_mod,
    student_embed,
    student_final,
    student_mod,
    teacher_qkv,
    teacher_out_far,
    student_qkv,
    student_out,
    out,
    totals,
    held,
    near_qkv,
    teacher_out,
    wide,
    shaped,
    shaped_s,
    qkv,
    heads,
    heads_in,
    weights,
    terms,
    inverses,
    d_attn,
    embed_t,
    embed_s,
    final_b,
    lat_rows,
    shaped_t,
    proj_t,
    shaped_in,
    proj_in,
    packed_in,
    part_c,
    part_d,
    qkv_sem,
    out_sem,
    swap_send,
    swap_recv,
    t_send,
    t_recv,
    s_send,
    s_recv,
    o_send,
    o_recv,
    *rest,
):
    boxes = [rest[4 * k : 4 * k + 4] for k in range(4)]
    last, last_in, pair_send, pair_recv, send, recv, z_send, z_recv = rest[16:24]
    inbox, sum_send, sum_recv = rest[24:]
    hidden, hidden_s, mixed, placed = (wide.at[k] for k in range(4))
    part_a, part_b = (wide.at[:, :, pl.ds(HALF * k, HALF)] for k in range(2))
    packed = near_qkv.at[0, pl.ds(0, 4 * TOKENS)]
    y, x, z, core, mp = (lax.axis_index(a) for a in AXES)
    load_out = pltpu.make_async_copy(teacher_out_far, teacher_out, out_sem)
    load_out.start()
    load = pltpu.make_async_copy(teacher_qkv, near_qkv, qkv_sem)
    load.start()
    held[0:3, y, x, z, core] = student_qkv[...]
    held[3, y, x, z, core] = student_out[...]
    both = ("dp_2", "mp")
    greet([friend for _, partners in all_places() for friend in partners])

    def swap(src, dst, k, axis="mp", target=None):
        target = 1 - mp if target is None else target
        return remote(src, dst, swap_send.at[k], swap_recv.at[k], axis, target)

    load_out.wait()
    spot = (y, x, z, core)
    here = teacher_out.at[spot]
    swaps = [
        swap(here, held.at[(5, *spot)], 0),
        swap(here, held.at[(5, *spot)], 1, both, (1 - z, 1 - mp)),
        swap(student_out, held.at[(4, *spot)], 15),
        swap(student_out, held.at[(4, *spot)], 16, both, (1 - z, 1 - mp)),
    ]
    for c in swaps:
        c.start()
    t_step = gather_stream(held, pl.ds(5, 1), t_send, t_recv, short=True)
    s_step = gather_stream(held, pl.ds(0, 4), s_send, s_recv)
    o_step = gather_stream(held, pl.ds(4, 1), o_send, o_recv, short=True)
    s_step(0)

    step = timestep[0]
    a_f, a_m, a_l = (picked_level(step, -k, ALPHAS) for k in range(3))
    s_f, s_m, s_l = (picked_level(step, -k, SIGMAS) for k in range(3))
    row_weight = bucket_weights[jnp.clip(bucket[0], 0, NBUCKET - 1)]
    places = [
        (teacher_mod, jnp.clip(2 * step - 1, 0, TGRID - 1)),
        (teacher_mod, jnp.clip(2 * step - 2, 0, TGRID - 1)),
        (student_mod, jnp.clip(step - 1, 0, K - 1)),
    ]
    modrows = [[mod[j, pl.ds(at, 1), :] for j in range(3)] for mod, at in places]

    def split_rows(ref):
        v = ref[...]
        h = v.astype(jnp.bfloat16)
        rest = v - h.astype(jnp.float32)
        m = rest.astype(jnp.bfloat16)
        return h, m, (rest - m.astype(jnp.float32)).astype(jnp.bfloat16)

    def stack(parts, out):
        h, m, l = parts
        for k, v in enumerate([h, m, h, l, h, m, jnp.zeros_like(h), jnp.zeros_like(h)]):
            out[16 * k : 16 * k + 16] = v

    def repeat(parts, out):
        for k in range(24):
            out[16 * k : 16 * k + 16] = parts[k // 8]

    def columns(k, width):
        return pl.ds(pl.multiple_of(k * width, width), width)

    def spread(v8, b_ref, out, base=None):
        terms8 = three_terms(v8)

        def body(n, carry):
            cols = columns(n, WIDE)
            h = dot(terms8, b_ref[:, cols])
            out[:, cols] = h if base is None else h + base[:, cols]
            return carry

        lax.fori_loop(0, D // WIDE, body, 0)

    def centred(v):
        mean = jnp.mean(v, axis=-1, keepdims=True)
        c = v - mean
        return c, lax.rsqrt(jnp.mean(c * c, axis=-1, keepdims=True) + LN_EPS), mean

    def by_rows(body):
        def group(n, carry):
            for u in range(UNROLL):
                body(pl.ds(pl.multiple_of(n * (16 * UNROLL) + 16 * u, 16), 16))
            return carry

        lax.fori_loop(0, TOKENS // (16 * UNROLL), group, 0)

    def shape(hid, which, out):
        shift, scale = modrows[which][0], 1.0 + modrows[which][1]

        def body(rows):
            c, inv, _ = centred(hid[rows])
            out[rows] = (c * inv * scale + shift).astype(jnp.bfloat16)

        by_rows(body)

    def project(src, weight):
        def body(j, carry):
            qkv[j] = dot(src[...], weight(j)).astype(jnp.bfloat16)
            return carry

        lax.fori_loop(0, 3, body, 0)

    lane = lax.broadcasted_iota(jnp.int32, (1, 128), 1)
    low_f = jnp.where(lane < 64, 1.0, 0.0)
    sides = [low_f.astype(jnp.bfloat16), (1.0 - low_f).astype(jnp.bfloat16)]
    is_low = lax.broadcasted_iota(jnp.int32, (TOKENS, 128), 1) < 64

    def swap_pair(which, hp):
        cols = pl.ds(128 * hp, 128)
        return swap(heads.at[which, :, cols], heads_in.at[which, :, cols], 3 + 4 * which + hp)

    def attend(which, keep):
        for hp in range(4):
            cols = pl.ds(128 * hp, 128)
            q, k, v = qkv[0, :, cols], qkv[1, :, cols], qkv[2, :, cols]
            outs = []
            for h in range(2):
                s = dot(q * sides[h], k, NT) * 0.125
                e = jnp.exp(s - jnp.max(s, axis=-1, keepdims=True))
                w = e / jnp.sum(e, axis=-1, keepdims=True)
                if keep:
                    weights[2 * hp + h] = w
                outs.append(dot(w.astype(jnp.bfloat16), v))
            heads[which, :, cols] = jnp.where(is_low, outs[0], outs[1]).astype(jnp.bfloat16)
            if hp > 0:
                swap_pair(which, hp - 1).start()
        swap_pair(which, 3).start()

    def swapped(which):
        for hp in range(4):
            swap_pair(which, hp).wait_recv()

    def mix(att, weight, which, base):
        mod_ref, at = places[which]

        def body(n, carry):
            cols = columns(n, 512)
            p = dot(att[...], weight(n), NT)
            mixed[:, cols] = base[:, cols] + mod_ref[2, pl.ds(at, 1), cols] * p
            return carry

        lax.fori_loop(0, 4, body, 0)

    def predict(final, keep):
        def body(rows):
            c, inv, mean = centred(mixed[rows])
            u = c * inv
            if keep:
                inverses[0, rows] = jnp.broadcast_to(inv, (16, 128))
                inverses[1, rows] = jnp.broadcast_to(mean, (16, 128))
            high = u.astype(jnp.bfloat16)
            rest = u - high.astype(jnp.float32)
            middle = rest.astype(jnp.bfloat16)
            terms[0, rows] = high
            terms[1, rows] = middle
            terms[2, rows] = (rest - middle.astype(jnp.float32)).astype(jnp.bfloat16)

        by_rows(body)
        r = dot(terms[0], final[...], NT)
        m = dot(terms[1], final[0:256], NT)
        small = dot(terms[2], final[0:128], NT)
        return (
            r[:, 0:128]
            + (r[:, 128:256] + m[:, 0:128])
            + (r[:, 256:384] + m[:, 128:256] + small)
        )

    def other_rows(slab):
        return lambda n: held[slab, n].reshape(512, 512)

    def near_rows(n):
        return teacher_out[n].reshape(512, 512)

    def turn(src, out):
        def body(n, carry):
            t = src[:, columns(n, 128)].astype(jnp.float32).T.astype(jnp.bfloat16)
            out[pl.ds(2 * n, 2)] = t.reshape(2, 2, 32, TOKENS)
            return carry

        lax.fori_loop(0, D // 128, body, 0)

    def pair(k):
        if k < 2:
            src, dst = ((shaped_t, shaped_in), (proj_t, proj_in))[k]
            src = src.at[:, 1 - core]
        else:
            cols = pl.ds(128 * (k - 2), 128)
            src, dst = packed.at[:, cols], packed_in.at[:, cols]
        return remote(src, dst, pair_send.at[k], pair_recv.at[k], "dp_3", 1 - core)

    half = D // 2
    for k in range(16):
        sin_a, cos_a = tables[0, k : k + 1], tables[1, k : k + 1]
        rows = pl.ds(16 * k, 16)
        placed[rows, :half] = sin_a * tables[3] + cos_a * tables[2]
        placed[rows, half:] = cos_a * tables[3] - sin_a * tables[2]
    stack(split_rows(teacher_embed), embed_t)
    latents = a_f * clean[...] + s_f * noise[...]
    for k in range(32):
        lat_rows[k : k + 1] = latents[:, 128 * k : 128 * k + 128]
    lat0 = eightfold(lat_rows[...])
    spread(lat0, embed_t, hidden, placed)
    shape(hidden, 0, shaped)
    swaps[0].wait_recv()
    swaps[1].wait_recv()
    t_step(0)
    s_step(1)
    load.wait()
    project(shaped, lambda j: near_qkv[j])
    t_step(1)
    attend(0, False)
    s_step(2)
    t_step(2)
    mix(heads.at[0], near_rows, 0, hidden)
    s_step(3)
    stack(split_rows(student_embed), embed_s)
    repeat(split_rows(teacher_final), final_b)
    spread(lat0, embed_s, hidden_s, placed)
    t_step(3)
    shape(hidden_s, 2, shaped_s)
    turn(shaped_s, shaped_t)
    t_step(4)
    swapped(0)
    mix(heads_in.at[0], other_rows(5), 0, mixed)
    eps0 = predict(final_b, False)
    lat1 = a_m * (lat0 - s_f * eps0) / a_f + s_m * eps0

    spread(lat1, embed_t, hidden, placed)
    shape(hidden, 1, shaped)
    project(shaped, lambda j: near_qkv[j])
    s_step(4)
    swaps[2].wait_recv()
    swaps[3].wait_recv()
    o_step(0)
    attend(1, False)
    mix(heads.at[1], near_rows, 1, hidden)
    swapped(1)
    mix(heads_in.at[1], other_rows(5), 1, mixed)
    s_step(5)
    o_step(1)
    eps1 = predict(final_b, False)
    lat2 = a_l * (lat1 - s_m * eps1) / a_m + s_l * eps1
    target = (lat0 - a_f / a_l * lat2) / (s_f - a_f * s_l / a_l)

    pair(0).start()
    student_terms = split_rows(student_final)
    repeat(student_terms, final_b)
    stack(student_terms, embed_t)
    s_step(6)
    project(shaped_s, lambda j: held[j].reshape(D, 512))
    o_step(2)
    attend(2, True)
    mix(heads.at[2], other_rows(3), 2, hidden_s)
    o_step(3)
    o_step(4)
    swapped(2)
    mix(heads_in.at[2], other_rows(4), 2, mixed)
    error = predict(final_b, True) - target
    lanes = lax.broadcasted_iota(jnp.int32, error.shape, 1)
    loss_part = (
        0.5 * row_weight * jnp.sum(jnp.where(lanes < 16, error * error, 0.0))
    )

    spread(2.0 * row_weight * error, embed_t, hidden)

    gate = modrows[2][2]

    def back(rows):
        inv, mean = inverses[0, rows, 0:1], inverses[1, rows, 0:1]
        up, u = hidden[rows], (mixed[rows] - mean) * inv
        first_mean = jnp.mean(up, axis=-1, keepdims=True)
        second_mean = jnp.mean(up * u, axis=-1, keepdims=True)
        d = (up - first_mean - u * second_mean) * inv
        shaped[rows] = (gate * d).astype(jnp.bfloat16)

    by_rows(back)
    turn(shaped, proj_t)
    d_attn[...] = dot(shaped[...], held[3].reshape(D, 512)).astype(jnp.bfloat16)
    pair(1).start()
    for hp in range(4):
        cols = pl.ds(128 * hp, 128)
        q, k, v, da = qkv[0, :, cols], qkv[1, :, cols], qkv[2, :, cols], d_attn[:, cols]
        outs = []
        for h in range(2):
            w = weights[2 * hp + h]
            dp = dot(da * sides[h], v, NT)
            ds = w * (dp - jnp.sum(w * dp, axis=-1, keepdims=True)) * 0.125
            ds = ds.astype(jnp.bfloat16)
            outs.append((dot(ds, k), dot(ds, q, TN), dot(w.astype(jnp.bfloat16), da, TN)))
        for j in range(3):
            joined = jnp.where(is_low, outs[0][j], outs[1][j]).astype(jnp.bfloat16)
            packed[TOKENS * j : TOKENS * (j + 1), cols] = joined
        packed[3 * TOKENS :, cols] = heads[2, :, cols]
        if hp > 0:
            pair(1 + hp).start()
    pair(5).start()

    def products(s_ref, p_ref, b_ref, add):
        def body(k, carry):
            rows = pl.ds(pl.multiple_of(k * 8, 8), 8)
            s, p = (r[rows].reshape(256, TOKENS) for r in (s_ref, p_ref))
            spot = pl.ds(pl.multiple_of(k * 64, 64), 64)
            for j in range(4):
                g = dot(p if j == 3 else s, b_ref[TOKENS * j : TOKENS * (j + 1)])
                cols = pl.ds(512 * (j % 2), 512)
                if j < 2:
                    for i in range(4):
                        block = g[64 * i : 64 * i + 64]
                        part_a[i, spot, cols] = part_a[i, spot, cols] + block if add else block
                else:
                    part_b[k, :, cols] = part_b[k, :, cols] + g if add else g
            return carry

        lax.fori_loop(0, 4, body, 0)

    products(shaped_t.at[:, core], proj_t.at[:, core], packed, False)
    for k in range(6):
        pair(k).wait_recv()
    products(shaped_in, proj_in, packed_in, True)
    rings = [
        ring_reduce(axis, part, *boxes[k], send.at[k], recv.at[k])
        for k, (axis, part) in enumerate(
            [("dp_1", part_a), ("dp_0", part_b), ("dp_0", part_c), ("dp_1", part_d)]
        )
    ]

    def into(part):
        def store(which, cols, value):
            part[2 * which, :, cols] = value[:64]
            part[2 * which + 1, :, cols] = value[64:]

        return store

    rings[0][0]()
    rings[1][0]()
    rings[0][1]()
    rings[1][1]()
    rings[0][2](into(part_c))
    rings[2][0]()
    rings[1][2](into(part_d))
    rings[3][0]()
    rings[2][1]()
    rings[3][1]()
    z_copies = []
    for k in range(2):

        def store(which, cols, value, k=k):
            last[k, which, :, cols] = value

        rings[2 + k][2](store)
        c = remote(
            last.at[k, 1 - z], last_in.at[k], z_send.at[k], z_recv.at[k], "dp_2", 1 - z
        )
        c.start()
        z_copies.append(c)
    for k, c in enumerate(z_copies):
        c.wait_recv()
        both = last[k, z] + last_in[k]
        out[2 * k] = both[:, :512]
        out[2 * k + 1] = both[:, 512:]
    for c in z_copies:
        c.wait_send()
    squares = jnp.sum(out[...] * out[...])
    row = lax.broadcasted_iota(jnp.int32, (8, 128), 0)
    value = jnp.where(row == 0, squares, loss_part)
    totals[...] = sum_over_all(value, inbox, sum_send, sum_recv)
    for c in swaps:
        c.wait_send()
    for k in range(6):
        pair(k).wait_send()
    for which in range(3):
        for hp in range(4):
            swap_pair(which, hp).wait_send()


def levels():
    lamb = 6.0 - 12.0 * np.arange(TGRID + 1) / TGRID
    return [np.sqrt(1.0 / (1.0 + np.exp(sign * lamb))).astype(np.float32) for sign in (-1.0, 1.0)]


ALPHAS, SIGMAS = levels()


def position_tables():
    half = D // 2
    freqs = np.exp(-math.log(10000.0) * np.arange(half) / half)
    fine = np.arange(16)[:, None] * freqs[None]
    angles = (np.sin(16.0 * fine), np.cos(16.0 * fine), np.sin(fine), np.cos(fine))
    return np.stack(angles).astype(np.float32)


def whole_step(timestep, bucket, bucket_weights, clean, noise, teacher, student):
    vmem, smem = (pl.BlockSpec(memory_space=m) for m in (pltpu.VMEM, pltpu.SMEM))
    bf16, f32 = jnp.bfloat16, jnp.float32

    def boxes(half):
        return [pltpu.VMEM((6, half, HALF), jnp.int16), pltpu.VMEM((6, 1, HALF), f32)] * 2

    def semaphores(*shape):
        return [pltpu.SemaphoreType.DMA(shape)] * 2

    return pl.pallas_call(
        step_kernel,
        out_shape=(
            jax.ShapeDtypeStruct((4, 32, 512), f32),
            jax.ShapeDtypeStruct((8, 128), f32),
        ),
        in_specs=[smem] * 3 + [vmem] * 9 + [pl.BlockSpec(memory_space=pl.ANY)] * 2 + [vmem] * 2,
        out_specs=(vmem,) * 2,
        scratch_shapes=[
            pltpu.VMEM((6, 4, 4, 2, 2, 2, 16, 512), bf16),
            pltpu.VMEM((3, D, 512), bf16),
            pltpu.VMEM((4, 4, 2, 2, 2, 16, 512), bf16),
            pltpu.VMEM((4, TOKENS, D), f32),
            pltpu.VMEM((TOKENS, D), bf16),
            pltpu.VMEM((TOKENS, D), bf16),
            pltpu.VMEM((3, TOKENS, 512), bf16),
            pltpu.VMEM((3, TOKENS, 512), bf16),
            pltpu.VMEM((3, TOKENS, 512), bf16),
            pltpu.VMEM((8, TOKENS, TOKENS), f32),
            pltpu.VMEM((3, TOKENS, D), bf16),
            pltpu.VMEM((2, TOKENS, 128), f32),
            pltpu.VMEM((TOKENS, 512), bf16),
            pltpu.VMEM((128, D), bf16),
            pltpu.VMEM((128, D), bf16),
            pltpu.VMEM((384, D), bf16),
            pltpu.VMEM((32, 128), f32),
            pltpu.VMEM((32, 2, 32, TOKENS), bf16),
            pltpu.VMEM((32, 2, 32, TOKENS), bf16),
            pltpu.VMEM((32, 32, TOKENS), bf16),
            pltpu.VMEM((32, 32, TOKENS), bf16),
            pltpu.VMEM((4 * TOKENS, 512), bf16),
            pltpu.VMEM((4, 64, HALF), f32),
            pltpu.VMEM((4, 64, HALF), f32),
            pltpu.SemaphoreType.DMA,
            pltpu.SemaphoreType.DMA,
            *semaphores(17),
            *semaphores(25),
            *semaphores(25),
            *semaphores(25),
            *boxes(128),
            *boxes(128),
            *boxes(32),
            *boxes(32),
            pltpu.VMEM((2, 2, 32, HALF), f32),
            pltpu.VMEM((2, 32, HALF), f32),
            *semaphores(6),
            *semaphores(4, 6, 2),
            *semaphores(2),
            pltpu.VMEM((3, 8, 8, 128), f32),
            *semaphores(3, 7),
        ],
        compiler_params=pltpu.CompilerParams(
            collective_id=2, has_side_effects=True, vmem_limit_bytes=63 * 2**20
        ),
    )(
        timestep,
        bucket,
        bucket_weights,
        clean,
        noise,
        jnp.asarray(position_tables()),
        teacher[0],
        teacher[1],
        jnp.moveaxis(teacher[2], 1, 0),
        student[0],
        student[1],
        jnp.moveaxis(student[2], 1, 0),
        jnp.moveaxis(teacher[3], 1, 0),
        teacher[4].reshape(4, 4, 2, 2, 2, 16, 512),
        jnp.moveaxis(student[3], 1, 0).reshape(3, 2, 16, 512),
        student[4].reshape(2, 16, 512),
    )


def adam_kernel(grads, totals, mq, vq, mo, vo, new_mq, new_vq, up_q, new_mo, new_vo, up_o, loss):
    rms = jnp.sqrt(totals[0:1, 0:1] / (4 * D * INNER))
    factor = 1.0 / jnp.maximum(rms, 1.0)

    def adam(grad, moment, second, new_moment, new_second, update):
        normed = grad * factor
        m = BETA_ONE * moment + (1.0 - BETA_ONE) * normed
        v = BETA_TWO * second + (1.0 - BETA_TWO) * normed * normed
        new_moment[...] = m
        new_second[...] = v
        update[...] = m / (jnp.sqrt(v) + ADAM_EPS)

    for j in range(3):
        adam(grads[j], mq[j], vq[j], new_mq.at[j], new_vq.at[j], up_q.at[j])
    adam(grads[3], mo[...], vo[...], new_mo, new_vo, up_o)
    loss[...] = totals[1:2, 0:1] / (SAMPLES * LATENT)


def adam_update(grads, totals, moment_qkv, second_qkv, moment_out, second_out):
    vmem = pl.BlockSpec(memory_space=pltpu.VMEM)
    mq, vq = (jnp.moveaxis(v, 1, 0) for v in (moment_qkv, second_qkv))
    qkv, out = (jax.ShapeDtypeStruct(v.shape, v.dtype) for v in (mq, moment_out))
    *news, loss = pl.pallas_call(
        adam_kernel,
        out_shape=(qkv, qkv, qkv, out, out, out, jax.ShapeDtypeStruct((1, 1), jnp.float32)),
        in_specs=[vmem] * 6,
        out_specs=(vmem,) * 7,
    )(grads, totals, mq, vq, moment_out, second_out)
    return (*(jnp.moveaxis(v, 0, 1) for v in news[:3]), *news[3:], loss.reshape(()))


def per_device(
    clean_latent,
    noise_draw,
    timestep,
    bucket,
    bucket_weights,
    teacher_embed,
    teacher_final,
    teacher_mod,
    teacher_qkv,
    teacher_out,
    student_embed,
    student_final,
    student_mod,
    student_qkv,
    student_out,
    moment_qkv,
    second_qkv,
    moment_out,
    second_out,
):
    grads, totals = whole_step(
        timestep,
        bucket,
        bucket_weights,
        clean_latent,
        noise_draw,
        (teacher_embed, teacher_final, teacher_mod, teacher_qkv, teacher_out),
        (student_embed, student_final, student_mod, student_qkv, student_out),
    )
    return adam_update(grads, totals, moment_qkv, second_qkv, moment_out, second_out)


def solution(mesh):
    torus = Mesh(
        mesh.devices.reshape(4, 4, 2, 2, mesh.shape["mp"]), ("dp_0", "dp_1", "dp_2", "dp_3", "mp")
    )
    in_specs = (
        P(DP, None),
        P(DP, None),
        P(DP),
        P(DP),
        P(),
        P(),
        P(),
        P(),
        P(None, None, "mp"),
        P(None, "mp"),
        P(),
        P(),
        P(),
        P(DP, None, "mp"),
        P(DP, "mp"),
        P(DP, None, "mp"),
        P(DP, None, "mp"),
        P(DP, "mp"),
        P(DP, "mp"),
    )
    out_specs = (
        P(DP, None, "mp"),
        P(DP, None, "mp"),
        P(DP, None, "mp"),
        P(DP, "mp"),
        P(DP, "mp"),
        P(DP, "mp"),
        P(),
    )
    return jax.shard_map(
        per_device, mesh=torus, in_specs=in_specs, out_specs=out_specs, check_vma=False
    )
```

```python
import math

import jax
import jax.numpy as jnp
import numpy as np
from jax import lax
from jax.experimental import pallas as pl
from jax.experimental.pallas import tpu as pltpu
from jax.sharding import Mesh
from jax.sharding import PartitionSpec as P

D = 2048
HS = 64
INNER = 1024
PATCH_CH = 16
SEQ = 256
LATENT = 4096
SAMPLES = 64
K = 8
TGRID = 16
NBUCKET = 8
DP = ("dp_0", "dp_1", "dp_2", "dp_3")
DP_MP = ("dp_0", "dp_1", "dp_2", "dp_3", "mp")


LN_EPS = 0.01
BETA_ONE = 0.9
BETA_TWO = 0.99
ADAM_EPS = 1e-08


ROWS = 1024
HALF = 1024
CODES = 32767.0
AXES = ("dp_0", "dp_1", "dp_2", "dp_3", "mp")


def remote(src, dst, send, recv, axis, target):
    return pltpu.make_async_remote_copy(
        src_ref=src,
        dst_ref=dst,
        send_sem=send,
        recv_sem=recv,
        device_id={axis: target} if isinstance(axis, str) else dict(zip(axis, target)),
        device_id_type=pl.DeviceIdType.MESH,
    )


def greet(friends):
    barrier = pltpu.get_barrier_semaphore()
    for axis, target in friends:
        pl.semaphore_signal(
            barrier,
            inc=1,
            device_id={axis: target} if isinstance(axis, str) else dict(zip(axis, target)),
            device_id_type=pl.DeviceIdType.MESH,
        )
    pl.semaphore_wait(barrier, len(friends))


def all_places():
    y, x, z, core, mp = (lax.axis_index(a) for a in AXES)
    axes, here = ("mp", "dp_2", "dp_3"), (mp, z, core)
    cube = []
    for k in range(1, 8):
        cube.append((axes, tuple(1 - h if k >> n & 1 else h for n, h in enumerate(here))))
    plane = []
    for k in range(1, 16):
        plane.append((("dp_0", "dp_1"), (lax.rem(y + k // 4, 4), lax.rem(x + k % 4, 4))))
    return [(4 * mp + 2 * z + core, cube), (4 * y + x, plane)]


def sum_over_all(value, inbox, send, recv):
    for stage, (slot, partners) in enumerate(all_places()):
        inbox[stage, slot] = value
        copies = [
            remote(
                inbox.at[stage, slot],
                inbox.at[stage, slot],
                send.at[stage, k],
                recv.at[stage, k],
                axis,
                target,
            )
            for k, (axis, target) in enumerate(partners)
        ]
        for c in copies:
            c.start()
        for c in copies:
            c.wait_recv()
        value = inbox[stage, 0]
        for k in range(1, len(partners) + 1):
            value = value + inbox[stage, k]
        for c in copies:
            c.wait_send()
    return value


def by_columns(body, width):
    def step(n, carry):
        body(pl.ds(pl.multiple_of(n * 256, 256), 256))
        return carry

    lax.fori_loop(0, width // 256, step, 0)


def coder(codes, scales, boxes, box_scales):
    def encode(k, value):
        def body(cols):
            v = value(cols)
            peak = jnp.maximum(jnp.max(jnp.abs(v), axis=0, keepdims=True), 1e-30)
            code = lax.round(v * (CODES / peak), lax.RoundingMethod.TO_NEAREST_EVEN)
            codes[k, :, cols] = code.astype(jnp.int32).astype(jnp.int16)
            scales[k, :, cols] = peak * (1.0 / CODES)

        by_columns(body, codes.shape[2])

    def decoded(k, cols):
        return boxes[k, :, cols].astype(jnp.int32).astype(jnp.float32) * box_scales[k, :, cols]

    return encode, decoded


def ring_reduce(axis, part, codes, scales, boxes, box_scales, send, recv):
    me = lax.axis_index(axis)
    right, left, far = (lax.rem(me + k, 4) for k in (1, 3, 2))
    half, width = part.shape[1] // 2, part.shape[2]
    top, low = pl.ds(0, half), pl.ds(half, half)

    encode, decoded = coder(codes, scales, boxes, box_scales)

    def message(k):
        target = left if k % 2 else right
        return [
            remote(codes.at[k], boxes.at[k], send.at[k, 0], recv.at[k, 0], axis, target),
            remote(scales.at[k], box_scales.at[k], send.at[k, 1], recv.at[k, 1], axis, target),
        ]

    def post(k, value):
        encode(k, value)
        for c in message(k):
            c.start()

    def arrived(*which):
        for k in which:
            for c in message(k):
                c.wait_recv()

    def start():
        post(0, lambda cols: part[far, top, cols])
        post(1, lambda cols: part[far, low, cols])
        post(2, lambda cols: part[right, low, cols])
        post(3, lambda cols: part[left, top, cols])

    def relay():
        arrived(0)
        post(4, lambda cols: part[right, top, cols] + decoded(0, cols))
        arrived(1)
        post(5, lambda cols: part[left, low, cols] + decoded(1, cols))

    def finish(store):
        arrived(3, 4)
        by_columns(
            lambda cols: store(0, cols, part[me, top, cols] + decoded(3, cols) + decoded(4, cols)),
            width,
        )
        arrived(2, 5)
        by_columns(
            lambda cols: store(1, cols, part[me, low, cols] + decoded(2, cols) + decoded(5, cols)),
            width,
        )
        for k in range(6):
            for c in message(k):
                c.wait_send()

    return start, relay, finish


TOKENS = 256
UNROLL = 4
WIDE = 256
NT = (((1,), (1,)), ((), ()))
TN = (((0,), (0,)), ((), ()))


def dot(a, b, dims=(((1,), (0,)), ((), ()))):
    return lax.dot_general(a, b, dims, preferred_element_type=jnp.float32)


def gather_stream(held, slabs, send, recv, short=False):
    y, x, z, core = (lax.axis_index(a) for a in AXES[:4])
    near = {"dp_0": [lax.rem(y + k, 4) for k in (1, 3)], "dp_1": [lax.rem(x + k, 4) for k in (1, 3)]}
    every = slice(None)
    live = []

    def go(spot, k, axis, target):
        ref = held.at[(slabs, *spot)]
        c = remote(ref, ref, send.at[k], recv.at[k], axis, target)
        c.start()
        live.append(c)
        return c

    def ring_direct(first):
        for half, axis in enumerate(("dp_1", "dp_0") if first else ("dp_0", "dp_1")):
            if first:
                spot = (y, x, every, core, half)
            elif half == 0:
                spot = (y, every, every, core, half)
            else:
                spot = (every, x, every, core, half)
            for side in range(2):
                k = (1 if first else 9) + 4 * half + side
                go(spot, k, axis, near[axis][side])

    def ring_relay(first):
        base = 1 if first else 9
        direct = live[-4:]
        for half, axis in enumerate(("dp_1", "dp_0") if first else ("dp_0", "dp_1")):
            for side in range(2):
                direct[2 * half + side].wait_recv()
                back = near[axis][1 - side]
                if first:
                    spot = (y, back) if axis == "dp_1" else (back, x)
                else:
                    spot = (every, back) if axis == "dp_1" else (back, every)
                go((*spot, side, core, half), base + 4 * half + 2 + side, axis, near[axis][side])

    def across(k, spot):
        go((*spot[:3], core, spot[3]), k, "dp_3", 1 - core)

    def ring_straight():
        for half, (axis, me) in enumerate([("dp_1", x), ("dp_0", y)]):
            for k in (1, 2, 3):
                go((y, x, every, core, half), 3 * half + k - 1, axis, lax.rem(me + k, 4))

    def step(k):
        if short:
            k = k + 2
        if k == 0:
            go((y, x, z, core), 0, "dp_2", 1 - z)
        elif k == 1:
            live[-1].wait_recv()
            ring_direct(True)
        elif k == 2:
            ring_straight() if short else ring_relay(True)
        elif k == 3:
            for c in live[-6:] if short else live[-4:]:
                c.wait_recv()
            ring_direct(False)
        elif k == 4:
            ring_relay(False)
            relays.extend(live[-4:])
            across(17, (y, every, every, 0))
            across(18, (every, x, every, 1))
            for n in range(2):
                across(19 + 2 * n, (near["dp_0"][n], every, every, 0))
                across(20 + 2 * n, (every, near["dp_1"][n], every, 1))
        elif k == 5:
            for c in relays:
                c.wait_recv()
            across(23, (lax.rem(y + 2, 4), every, every, 0))
            across(24, (every, lax.rem(x + 2, 4), every, 1))
        else:
            for c in live[-8:]:
                c.wait_recv()
            for c in live:
                c.wait_send()

    relays = []
    return step


def three_terms(v8):
    high = v8.astype(jnp.bfloat16).astype(jnp.float32)
    rest = v8 - high
    middle = rest.astype(jnp.bfloat16).astype(jnp.float32)
    low = rest - middle
    group = lax.broadcasted_iota(jnp.int32, v8.shape, 1) // 16
    picked = jnp.where(
        (group == 0) | (group == 1) | (group == 3),
        high,
        jnp.where((group == 2) | (group == 5), middle, jnp.where(group == 4, low, 0.0)),
    )
    return picked.astype(jnp.bfloat16)


def eightfold(rows):
    v = jnp.broadcast_to(rows[:, None], (32, 8, 128)).reshape(TOKENS, 128)
    token = lax.broadcasted_iota(jnp.int32, v.shape, 0) % 8
    lane = lax.broadcasted_iota(jnp.int32, v.shape, 1)
    v = jnp.where(lane // 16 == token, v, 0.0)
    across = lax.broadcasted_iota(jnp.int32, (128, 128), 1) % 16
    down = lax.broadcasted_iota(jnp.int32, (128, 128), 0) % 16
    spread = jnp.where(across == down, 1.0, 0.0).astype(jnp.bfloat16)
    high = v.astype(jnp.bfloat16)
    rest = v - high.astype(jnp.float32)
    middle = rest.astype(jnp.bfloat16)
    low = (rest - middle.astype(jnp.float32)).astype(jnp.bfloat16)
    return dot(high, spread) + dot(middle, spread) + dot(low, spread)


def picked_level(step, offset, values):
    out = jnp.float32(0.0)
    for k in range(1, K + 1):
        out = jnp.where(step == k, jnp.float32(values[2 * k + offset]), out)
    return out


def step_kernel(
    timestep,
    bucket,
    bucket_weights,
    clean,
    noise,
    tables,
    teacher_embed,
    teacher_final,
    teacher_mod,
    student_embed,
    student_final,
    student_mod,
    teacher_qkv,
    teacher_out_far,
    student_qkv,
    student_out,
    out_far,
    totals,
    out,
    held,
    near_qkv,
    teacher_out,
    wide,
    shaped,
    shaped_s,
    qkv,
    heads,
    heads_in,
    weights,
    terms,
    inverses,
    d_attn,
    embed_t,
    embed_s,
    final_b,
    lat_rows,
    shaped_t,
    proj_t,
    shaped_in,
    proj_in,
    packed_in,
    part_c,
    part_d,
    qkv_sem,
    out_sem,
    grads_sem,
    swap_send,
    swap_recv,
    t_send,
    t_recv,
    s_send,
    s_recv,
    o_send,
    o_recv,
    *rest,
):
    boxes = [rest[4 * k : 4 * k + 4] for k in range(10)]
    last, pair_send, pair_recv, send, recv, z_send, z_recv = rest[40:47]
    inbox, sum_send, sum_recv = rest[47:]
    hidden, hidden_s, mixed, placed = (wide.at[k] for k in range(4))
    packed = near_qkv.at[0, pl.ds(0, 3 * TOKENS)]
    y, x, z, core, mp = (lax.axis_index(a) for a in AXES)
    load_out = pltpu.make_async_copy(teacher_out_far, teacher_out, out_sem)
    load_out.start()
    load = pltpu.make_async_copy(teacher_qkv, near_qkv, qkv_sem)
    load.start()
    held[0:3, y, x, z, core] = student_qkv[...]
    held[3, y, x, z, core] = student_out[...]
    both = ("dp_2", "mp")
    greet([friend for _, partners in all_places() for friend in partners])

    def swap(src, dst, k, axis="mp", target=None):
        target = 1 - mp if target is None else target
        return remote(src, dst, swap_send.at[k], swap_recv.at[k], axis, target)

    load_out.wait()
    spot = (y, x, z, core)
    here = teacher_out.at[spot]
    swaps = [
        swap(here, held.at[(5, *spot)], 0),
        swap(here, held.at[(5, *spot)], 1, both, (1 - z, 1 - mp)),
        swap(student_out, held.at[(4, *spot)], 15),
        swap(student_out, held.at[(4, *spot)], 16, both, (1 - z, 1 - mp)),
    ]
    for c in swaps:
        c.start()
    t_step = gather_stream(held, pl.ds(5, 1), t_send, t_recv, short=True)
    s_step = gather_stream(held, pl.ds(0, 4), s_send, s_recv)
    o_step = gather_stream(held, pl.ds(4, 1), o_send, o_recv, short=True)
    s_step(0)

    step = timestep[0]
    a_f, a_m, a_l = (picked_level(step, -k, ALPHAS) for k in range(3))
    s_f, s_m, s_l = (picked_level(step, -k, SIGMAS) for k in range(3))
    row_weight = bucket_weights[jnp.clip(bucket[0], 0, NBUCKET - 1)]
    places = [
        (teacher_mod, jnp.clip(2 * step - 1, 0, TGRID - 1)),
        (teacher_mod, jnp.clip(2 * step - 2, 0, TGRID - 1)),
        (student_mod, jnp.clip(step - 1, 0, K - 1)),
    ]
    modrows = [[mod[j, pl.ds(at, 1), :] for j in range(3)] for mod, at in places]

    def split_rows(ref):
        v = ref[...]
        h = v.astype(jnp.bfloat16)
        rest = v - h.astype(jnp.float32)
        m = rest.astype(jnp.bfloat16)
        return h, m, (rest - m.astype(jnp.float32)).astype(jnp.bfloat16)

    def stack(parts, out):
        h, m, l = parts
        for k, v in enumerate([h, m, h, l, h, m, jnp.zeros_like(h), jnp.zeros_like(h)]):
            out[16 * k : 16 * k + 16] = v

    def repeat(parts, out):
        for k in range(24):
            out[16 * k : 16 * k + 16] = parts[k // 8]

    def columns(k, width):
        return pl.ds(pl.multiple_of(k * width, width), width)

    def spread(v8, b_ref, out, base=None):
        terms8 = three_terms(v8)

        for n in range(D // WIDE):
            cols = pl.ds(n * WIDE, WIDE)
            h = dot(terms8, b_ref[:, cols])
            out[:, cols] = h if base is None else h + base[:, cols]

    def centred(v):
        mean = jnp.mean(v, axis=-1, keepdims=True)
        c = v - mean
        return c, lax.rsqrt(jnp.mean(c * c, axis=-1, keepdims=True) + LN_EPS), mean

    def by_rows(body):
        def group(n, carry):
            for u in range(UNROLL):
                body(pl.ds(pl.multiple_of(n * (16 * UNROLL) + 16 * u, 16), 16))
            return carry

        lax.fori_loop(0, TOKENS // (16 * UNROLL), group, 0)

    def shape(hid, which, out):
        shift, scale = modrows[which][0], 1.0 + modrows[which][1]

        def body(rows):
            c, inv, _ = centred(hid[rows])
            out[rows] = (c * inv * scale + shift).astype(jnp.bfloat16)

        by_rows(body)

    def project(src, weight):
        def body(j, carry):
            qkv[j] = dot(src[...], weight(j)).astype(jnp.bfloat16)
            return carry

        lax.fori_loop(0, 3, body, 0)

    lane = lax.broadcasted_iota(jnp.int32, (1, 128), 1)
    low_f = jnp.where(lane < 64, 1.0, 0.0)
    sides = [low_f.astype(jnp.bfloat16), (1.0 - low_f).astype(jnp.bfloat16)]
    is_low = lax.broadcasted_iota(jnp.int32, (TOKENS, 128), 1) < 64

    def swap_pair(which, hp):
        cols = pl.ds(128 * hp, 128)
        return swap(heads.at[which, :, cols], heads_in.at[which, :, cols], 3 + 4 * which + hp)

    def attend(which, keep):
        for hp in range(4):
            cols = pl.ds(128 * hp, 128)
            q, k, v = qkv[0, :, cols], qkv[1, :, cols], qkv[2, :, cols]
            outs = []
            for h in range(2):
                s = dot(q * sides[h], k, NT) * 0.125
                e = jnp.exp(s - jnp.max(s, axis=-1, keepdims=True))
                w = e / jnp.sum(e, axis=-1, keepdims=True)
                if keep:
                    weights[2 * hp + h] = w
                outs.append(dot(w.astype(jnp.bfloat16), v))
            heads[which, :, cols] = jnp.where(is_low, outs[0], outs[1]).astype(jnp.bfloat16)
            if hp > 0:
                swap_pair(which, hp - 1).start()
        swap_pair(which, 3).start()

    def swapped(which):
        for hp in range(4):
            swap_pair(which, hp).wait_recv()

    def mix(att, weight, which, base):
        mod_ref, at = places[which]

        for n in range(4):
            cols = pl.ds(n * 512, 512)
            p = dot(att[...], weight(n), NT)
            mixed[:, cols] = base[:, cols] + mod_ref[2, pl.ds(at, 1), cols] * p

    def predict(final, keep):
        def body(rows):
            c, inv, mean = centred(mixed[rows])
            u = c * inv
            if keep:
                inverses[0, rows] = jnp.broadcast_to(inv, (16, 128))
                inverses[1, rows] = jnp.broadcast_to(mean, (16, 128))
            high = u.astype(jnp.bfloat16)
            rest = u - high.astype(jnp.float32)
            middle = rest.astype(jnp.bfloat16)
            terms[0, rows] = high
            terms[1, rows] = middle
            terms[2, rows] = (rest - middle.astype(jnp.float32)).astype(jnp.bfloat16)

        by_rows(body)
        r = dot(terms[0], final[...], NT)
        m = dot(terms[1], final[0:256], NT)
        small = dot(terms[2], final[0:128], NT)
        return (
            r[:, 0:128]
            + (r[:, 128:256] + m[:, 0:128])
            + (r[:, 256:384] + m[:, 128:256] + small)
        )

    def other_rows(slab):
        return lambda n: held[slab, n].reshape(512, 512)

    def near_rows(n):
        return teacher_out[n].reshape(512, 512)

    def turn(src, out):
        def body(n, carry):
            t = src[:, columns(n, 128)].astype(jnp.float32).T.astype(jnp.bfloat16)
            out[pl.ds(2 * n, 2)] = t.reshape(2, 2, 32, TOKENS)
            return carry

        lax.fori_loop(0, D // 128, body, 0)

    def pair(k):
        if k < 2:
            src, dst = ((shaped_t, shaped_in), (proj_t, proj_in))[k]
            src = src.at[:, 1 - core]
        elif k == 2:
            src, dst = heads.at[2], packed_in.at[pl.ds(3 * TOKENS, TOKENS)]
        else:
            cols = pl.ds(128 * (k - 3), 128)
            src, dst = packed.at[:, cols], packed_in.at[pl.ds(0, 3 * TOKENS), cols]
        return remote(src, dst, pair_send.at[k], pair_recv.at[k], "dp_3", 1 - core)

    half = D // 2
    for k in range(16):
        sin_a, cos_a = tables[0, k : k + 1], tables[1, k : k + 1]
        rows = pl.ds(16 * k, 16)
        placed[rows, :half] = sin_a * tables[3] + cos_a * tables[2]
        placed[rows, half:] = cos_a * tables[3] - sin_a * tables[2]
    stack(split_rows(teacher_embed), embed_t)
    latents = a_f * clean[...] + s_f * noise[...]
    for k in range(32):
        lat_rows[k : k + 1] = latents[:, 128 * k : 128 * k + 128]
    lat0 = eightfold(lat_rows[...])
    spread(lat0, embed_t, hidden, placed)
    shape(hidden, 0, shaped)
    swaps[0].wait_recv()
    swaps[1].wait_recv()
    t_step(0)
    s_step(1)
    load.wait()
    project(shaped, lambda j: near_qkv[j])
    t_step(1)
    attend(0, False)
    s_step(2)
    t_step(2)
    mix(heads.at[0], near_rows, 0, hidden)
    s_step(3)
    stack(split_rows(student_embed), embed_s)
    repeat(split_rows(teacher_final), final_b)
    spread(lat0, embed_s, hidden_s, placed)
    t_step(3)
    shape(hidden_s, 2, shaped_s)
    turn(shaped_s, shaped_t)
    t_step(4)
    swapped(0)
    mix(heads_in.at[0], other_rows(5), 0, mixed)
    eps0 = predict(final_b, False)
    lat1 = a_m * (lat0 - s_f * eps0) / a_f + s_m * eps0

    spread(lat1, embed_t, hidden, placed)
    shape(hidden, 1, shaped)
    project(shaped, lambda j: near_qkv[j])
    s_step(4)
    swaps[2].wait_recv()
    swaps[3].wait_recv()
    o_step(0)
    attend(1, False)
    mix(heads.at[1], near_rows, 1, hidden)
    swapped(1)
    mix(heads_in.at[1], other_rows(5), 1, mixed)
    s_step(5)
    o_step(1)
    eps1 = predict(final_b, False)
    lat2 = a_l * (lat1 - s_m * eps1) / a_m + s_l * eps1
    target = (lat0 - a_f / a_l * lat2) / (s_f - a_f * s_l / a_l)

    pair(0).start()
    student_terms = split_rows(student_final)
    repeat(student_terms, final_b)
    stack(student_terms, embed_t)
    s_step(6)
    project(shaped_s, lambda j: held[j].reshape(D, 512))
    o_step(2)
    attend(2, True)
    mix(heads.at[2], other_rows(3), 2, hidden_s)
    o_step(3)
    swapped(2)
    o_step(4)
    mix(heads_in.at[2], other_rows(4), 2, mixed)
    error = predict(final_b, True) - target
    lanes = lax.broadcasted_iota(jnp.int32, error.shape, 1)
    loss_part = (
        0.5 * row_weight * jnp.sum(jnp.where(lanes < 16, error * error, 0.0))
    )

    spread(2.0 * row_weight * error, embed_t, hidden)

    gate = modrows[2][2]

    def back(rows):
        inv, mean = inverses[0, rows, 0:1], inverses[1, rows, 0:1]
        up, u = hidden[rows], (mixed[rows] - mean) * inv
        first_mean = jnp.mean(up, axis=-1, keepdims=True)
        second_mean = jnp.mean(up * u, axis=-1, keepdims=True)
        d = (up - first_mean - u * second_mean) * inv
        shaped[rows] = (gate * d).astype(jnp.bfloat16)

    by_rows(back)
    turn(shaped, proj_t)
    pair(2).start()
    d_attn[...] = dot(shaped[...], held[3].reshape(D, 512)).astype(jnp.bfloat16)
    pair(1).start()

    extents = [(0, 3 * WIDE), (3 * WIDE, WIDE)]

    def products(s_ref, b_ref, first, count, add):
        def body(k, carry):
            lhs = s_ref[pl.ds(pl.multiple_of(k * 8, 8), 8)].reshape(256, TOKENS)
            spot = pl.ds(pl.multiple_of(k * 64, 64), 64)
            for j in range(count):
                g = dot(lhs, b_ref[TOKENS * j : TOKENS * (j + 1)])
                cols = pl.ds(WIDE * (first + j), WIDE)
                for i in range(4):
                    block = g[64 * i : 64 * i + 64, :WIDE]
                    wide[i, spot, cols] = wide[i, spot, cols] + block if add else block
                cols = pl.ds(HALF + WIDE * (first + j), WIDE)
                right = g[:, WIDE:]
                wide[k, :, cols] = wide[k, :, cols] + right if add else right
            return carry

        lax.fori_loop(0, 4, body, 0)

    rings = []
    for which, (offset, width) in enumerate(extents):
        for way in range(2):
            for stage in range(2):
                n = len(rings)
                if stage == 0:
                    part = wide.at[:, :, pl.ds(HALF * way + offset, width)]
                else:
                    part = (part_c, part_d)[way].at[:, :, pl.ds(offset, width)]
                axis = ("dp_1", "dp_0")[(way + stage) % 2]
                rings.append(ring_reduce(axis, part, *boxes[n], send.at[n], recv.at[n]))

    def ring_step(which, stage, step):
        offset, width = extents[which]
        for way in range(2):

            def into(half, cols, value, way=way):
                if stage == 0:
                    part = (part_c, part_d)[way].at[:, :, pl.ds(offset, width)]
                    part[2 * half, :, cols] = value[:64]
                    part[2 * half + 1, :, cols] = value[64:]
                else:
                    last.at[way, half, :, pl.ds(offset, width)][:, cols] = value

            do = rings[4 * which + 2 * way + stage][step]
            do(into) if step == 2 else do()

    def z_copies(which):
        codes, scales, codes_in, scales_in = boxes[8 + which]
        return [
            remote(a, b, z_send.at[2 * which + k], z_recv.at[2 * which + k], "dp_2", 1 - z)
            for k, (a, b) in enumerate([(codes, codes_in), (scales, scales_in)])
        ]

    def z_start(which):
        encode, _ = coder(*boxes[8 + which])
        offset, width = extents[which]
        for way in range(2):
            encode(way, lambda cols, way=way: last.at[way, 1 - z, :, pl.ds(offset, width)][:, cols])
        for c in z_copies(which):
            c.start()

    products(proj_t.at[:, core], heads.at[2], 3, 1, False)
    pair(1).wait_recv()
    pair(2).wait_recv()
    products(proj_in, packed_in.at[pl.ds(3 * TOKENS, TOKENS)], 3, 1, True)
    ring_step(1, 0, 0)
    for hp in range(4):
        cols = pl.ds(128 * hp, 128)
        q, k, v, da = qkv[0, :, cols], qkv[1, :, cols], qkv[2, :, cols], d_attn[:, cols]
        outs = []
        for h in range(2):
            w = weights[2 * hp + h]
            dp = dot(da * sides[h], v, NT)
            ds = w * (dp - jnp.sum(w * dp, axis=-1, keepdims=True)) * 0.125
            ds = ds.astype(jnp.bfloat16)
            outs.append((dot(ds, k), dot(ds, q, TN), dot(w.astype(jnp.bfloat16), da, TN)))
        for j in range(3):
            joined = jnp.where(is_low, outs[0][j], outs[1][j]).astype(jnp.bfloat16)
            packed[TOKENS * j : TOKENS * (j + 1), cols] = joined
        if hp > 0:
            pair(2 + hp).start()
    pair(6).start()
    ring_step(1, 0, 1)
    products(shaped_t.at[:, core], packed, 0, 3, False)
    for k in (0, 3, 4, 5, 6):
        pair(k).wait_recv()
    products(shaped_in, packed_in, 0, 3, True)
    ring_step(0, 0, 0)
    ring_step(1, 0, 2)
    ring_step(0, 0, 1)
    ring_step(0, 0, 2)
    ring_step(0, 1, 0)
    ring_step(1, 1, 0)
    ring_step(0, 1, 1)
    ring_step(1, 1, 1)
    ring_step(0, 1, 2)
    z_start(0)
    ring_step(1, 1, 2)
    z_start(1)
    for which, (offset, width) in enumerate(extents):
        _, decoded = coder(*boxes[8 + which])
        for c in z_copies(which):
            c.wait_recv()
        for way in range(2):
            for j in range(offset // WIDE, (offset + width) // WIDE):
                cols, near = pl.ds(WIDE * j, WIDE), pl.ds(WIDE * j - offset, WIDE)
                out[j, :, pl.ds(WIDE * way, WIDE)] = last[way, z, :, cols] + decoded(way, near)
    leave = pltpu.make_async_copy(out, out_far, grads_sem)
    leave.start()
    squares = jnp.sum(out[...] * out[...])
    row = lax.broadcasted_iota(jnp.int32, (8, 128), 0)
    value = jnp.where(row == 0, squares, loss_part)
    totals[...] = sum_over_all(value, inbox, sum_send, sum_recv)
    leave.wait()
    for c in [*z_copies(0), *z_copies(1)]:
        c.wait_send()
    for c in swaps:
        c.wait_send()
    for k in range(7):
        pair(k).wait_send()
    for which in range(3):
        for hp in range(4):
            swap_pair(which, hp).wait_send()


def levels():
    lamb = 6.0 - 12.0 * np.arange(TGRID + 1) / TGRID
    return [np.sqrt(1.0 / (1.0 + np.exp(sign * lamb))).astype(np.float32) for sign in (-1.0, 1.0)]


ALPHAS, SIGMAS = levels()


def position_tables():
    half = D // 2
    freqs = np.exp(-math.log(10000.0) * np.arange(half) / half)
    fine = np.arange(16)[:, None] * freqs[None]
    angles = (np.sin(16.0 * fine), np.cos(16.0 * fine), np.sin(fine), np.cos(fine))
    return np.stack(angles).astype(np.float32)


def whole_step(timestep, bucket, bucket_weights, clean, noise, teacher, student):
    vmem, smem = (pl.BlockSpec(memory_space=m) for m in (pltpu.VMEM, pltpu.SMEM))
    bf16, f32 = jnp.bfloat16, jnp.float32

    def boxes(width):
        return [
            scratch
            for half in (128, 32, 128, 32)
            for scratch in [pltpu.VMEM((6, half, width), jnp.int16), pltpu.VMEM((6, 1, width), f32)] * 2
        ]

    def last_boxes(width):
        return [pltpu.VMEM((2, 32, width), jnp.int16), pltpu.VMEM((2, 1, width), f32)] * 2

    def semaphores(*shape):
        return [pltpu.SemaphoreType.DMA(shape)] * 2

    return pl.pallas_call(
        step_kernel,
        out_shape=(
            jax.ShapeDtypeStruct((4, 32, 512), f32),
            jax.ShapeDtypeStruct((8, 128), f32),
        ),
        in_specs=[smem] * 3 + [vmem] * 9 + [pl.BlockSpec(memory_space=pl.ANY)] * 2 + [vmem] * 2,
        out_specs=(pl.BlockSpec(memory_space=pl.ANY), vmem),
        scratch_shapes=[
            pltpu.VMEM((4, 32, 512), f32),
            pltpu.VMEM((6, 4, 4, 2, 2, 2, 16, 512), bf16),
            pltpu.VMEM((3, D, 512), bf16),
            pltpu.VMEM((4, 4, 2, 2, 2, 16, 512), bf16),
            pltpu.VMEM((4, TOKENS, D), f32),
            pltpu.VMEM((TOKENS, D), bf16),
            pltpu.VMEM((TOKENS, D), bf16),
            pltpu.VMEM((3, TOKENS, 512), bf16),
            pltpu.VMEM((3, TOKENS, 512), bf16),
            pltpu.VMEM((3, TOKENS, 512), bf16),
            pltpu.VMEM((8, TOKENS, TOKENS), f32),
            pltpu.VMEM((3, TOKENS, D), bf16),
            pltpu.VMEM((2, TOKENS, 128), f32),
            pltpu.VMEM((TOKENS, 512), bf16),
            pltpu.VMEM((128, D), bf16),
            pltpu.VMEM((128, D), bf16),
            pltpu.VMEM((384, D), bf16),
            pltpu.VMEM((32, 128), f32),
            pltpu.VMEM((32, 2, 32, TOKENS), bf16),
            pltpu.VMEM((32, 2, 32, TOKENS), bf16),
            pltpu.VMEM((32, 32, TOKENS), bf16),
            pltpu.VMEM((32, 32, TOKENS), bf16),
            pltpu.VMEM((4 * TOKENS, 512), bf16),
            pltpu.VMEM((4, 64, HALF), f32),
            pltpu.VMEM((4, 64, HALF), f32),
            pltpu.SemaphoreType.DMA,
            pltpu.SemaphoreType.DMA,
            pltpu.SemaphoreType.DMA,
            *semaphores(17),
            *semaphores(25),
            *semaphores(25),
            *semaphores(25),
            *boxes(3 * WIDE),
            *boxes(WIDE),
            *last_boxes(3 * WIDE),
            *last_boxes(WIDE),
            pltpu.VMEM((2, 2, 32, HALF), f32),
            *semaphores(7),
            *semaphores(8, 6, 2),
            *semaphores(4),
            pltpu.VMEM((2, 16, 8, 128), f32),
            *semaphores(2, 15),
        ],
        compiler_params=pltpu.CompilerParams(
            collective_id=2, has_side_effects=True, vmem_limit_bytes=63 * 2**20
        ),
    )(
        timestep,
        bucket,
        bucket_weights,
        clean,
        noise,
        jnp.asarray(position_tables()),
        teacher[0],
        teacher[1],
        jnp.moveaxis(teacher[2], 1, 0),
        student[0],
        student[1],
        jnp.moveaxis(student[2], 1, 0),
        jnp.moveaxis(teacher[3], 1, 0),
        teacher[4].reshape(4, 4, 2, 2, 2, 16, 512),
        jnp.moveaxis(student[3], 1, 0).reshape(3, 2, 16, 512),
        student[4].reshape(2, 16, 512),
    )


def adam_kernel(grads, totals, mq, vq, mo, vo, new_mq, new_vq, up_q, new_mo, new_vo, up_o, loss):
    rms = jnp.sqrt(totals[0:1, 0:1] / (4 * D * INNER))
    factor = 1.0 / jnp.maximum(rms, 1.0)

    def adam(grad, moment, second, new_moment, new_second, update):
        normed = grad * factor
        m = BETA_ONE * moment + (1.0 - BETA_ONE) * normed
        v = BETA_TWO * second + (1.0 - BETA_TWO) * normed * normed
        new_moment[...] = m
        new_second[...] = v
        update[...] = m / (jnp.sqrt(v) + ADAM_EPS)

    for j in range(3):
        adam(grads[j], mq[j], vq[j], new_mq.at[j], new_vq.at[j], up_q.at[j])
    adam(grads[3], mo[...], vo[...], new_mo, new_vo, up_o)
    loss[...] = totals[1:2, 0:1] / (SAMPLES * LATENT)


def adam_update(grads, totals, moment_qkv, second_qkv, moment_out, second_out):
    vmem = pl.BlockSpec(memory_space=pltpu.VMEM)
    mq, vq = (jnp.moveaxis(v, 1, 0) for v in (moment_qkv, second_qkv))
    qkv, out = (jax.ShapeDtypeStruct(v.shape, v.dtype) for v in (mq, moment_out))
    *news, loss = pl.pallas_call(
        adam_kernel,
        out_shape=(qkv, qkv, qkv, out, out, out, jax.ShapeDtypeStruct((1, 1), jnp.float32)),
        in_specs=[vmem] * 6,
        out_specs=(vmem,) * 7,
    )(grads, totals, mq, vq, moment_out, second_out)
    return (*(jnp.moveaxis(v, 0, 1) for v in news[:3]), *news[3:], loss.reshape(()))


def per_device(
    clean_latent,
    noise_draw,
    timestep,
    bucket,
    bucket_weights,
    teacher_embed,
    teacher_final,
    teacher_mod,
    teacher_qkv,
    teacher_out,
    student_embed,
    student_final,
    student_mod,
    student_qkv,
    student_out,
    moment_qkv,
    second_qkv,
    moment_out,
    second_out,
):
    grads, totals = whole_step(
        timestep,
        bucket,
        bucket_weights,
        clean_latent,
        noise_draw,
        (teacher_embed, teacher_final, teacher_mod, teacher_qkv, teacher_out),
        (student_embed, student_final, student_mod, student_qkv, student_out),
    )
    return adam_update(grads, totals, moment_qkv, second_qkv, moment_out, second_out)


def solution(mesh):
    torus = Mesh(
        mesh.devices.reshape(4, 4, 2, 2, mesh.shape["mp"]), ("dp_0", "dp_1", "dp_2", "dp_3", "mp")
    )
    in_specs = (
        P(DP, None),
        P(DP, None),
        P(DP),
        P(DP),
        P(),
        P(),
        P(),
        P(),
        P(None, None, "mp"),
        P(None, "mp"),
        P(),
        P(),
        P(),
        P(DP, None, "mp"),
        P(DP, "mp"),
        P(DP, None, "mp"),
        P(DP, None, "mp"),
        P(DP, "mp"),
        P(DP, "mp"),
    )
    out_specs = (
        P(DP, None, "mp"),
        P(DP, None, "mp"),
        P(DP, None, "mp"),
        P(DP, "mp"),
        P(DP, "mp"),
        P(DP, "mp"),
        P(),
    )
    return jax.shard_map(
        per_device, mesh=torus, in_specs=in_specs, out_specs=out_specs, check_vma=False
    )
```

```python
import math

import jax
import jax.numpy as jnp
import numpy as np
from jax import lax
from jax.experimental import pallas as pl
from jax.experimental.pallas import tpu as pltpu
from jax.sharding import Mesh
from jax.sharding import PartitionSpec as P

D = 2048
HS = 64
INNER = 1024
PATCH_CH = 16
SEQ = 256
LATENT = 4096
SAMPLES = 64
K = 8
TGRID = 16
NBUCKET = 8
DP = ("dp_0", "dp_1", "dp_2", "dp_3")
DP_MP = ("dp_0", "dp_1", "dp_2", "dp_3", "mp")


LN_EPS = 0.01
BETA_ONE = 0.9
BETA_TWO = 0.99
ADAM_EPS = 1e-08


ROWS = 1024
HALF = 1024
CODES = 32767.0
AXES = ("dp_0", "dp_1", "dp_2", "dp_3", "mp")


def remote(src, dst, send, recv, axis, target):
    return pltpu.make_async_remote_copy(
        src_ref=src,
        dst_ref=dst,
        send_sem=send,
        recv_sem=recv,
        device_id={axis: target} if isinstance(axis, str) else dict(zip(axis, target)),
        device_id_type=pl.DeviceIdType.MESH,
    )


def greet(friends):
    barrier = pltpu.get_barrier_semaphore()
    for axis, target in friends:
        pl.semaphore_signal(
            barrier,
            inc=1,
            device_id={axis: target} if isinstance(axis, str) else dict(zip(axis, target)),
            device_id_type=pl.DeviceIdType.MESH,
        )
    pl.semaphore_wait(barrier, len(friends))


def all_places():
    y, x, z, core, mp = (lax.axis_index(a) for a in AXES)
    axes, here = ("mp", "dp_2", "dp_3"), (mp, z, core)
    cube = []
    for k in range(1, 8):
        cube.append((axes, tuple(1 - h if k >> n & 1 else h for n, h in enumerate(here))))
    plane = []
    for k in range(1, 16):
        plane.append((("dp_0", "dp_1"), (lax.rem(y + k // 4, 4), lax.rem(x + k % 4, 4))))
    return [(4 * mp + 2 * z + core, cube), (4 * y + x, plane)]


def sum_over_all(value, inbox, send, recv):
    for stage, (slot, partners) in enumerate(all_places()):
        inbox[stage, slot] = value
        copies = [
            remote(
                inbox.at[stage, slot],
                inbox.at[stage, slot],
                send.at[stage, k],
                recv.at[stage, k],
                axis,
                target,
            )
            for k, (axis, target) in enumerate(partners)
        ]
        for c in copies:
            c.start()
        for c in copies:
            c.wait_recv()
        value = inbox[stage, 0]
        for k in range(1, len(partners) + 1):
            value = value + inbox[stage, k]
        for c in copies:
            c.wait_send()
    return value


def by_columns(body, width):
    def step(n, carry):
        body(pl.ds(pl.multiple_of(n * 256, 256), 256))
        return carry

    lax.fori_loop(0, width // 256, step, 0)


def coder(codes, scales, boxes, box_scales):
    def encode(k, value):
        def body(cols):
            v = value(cols)
            peak = jnp.maximum(jnp.max(jnp.abs(v), axis=0, keepdims=True), 1e-30)
            code = lax.round(v * (CODES / peak), lax.RoundingMethod.TO_NEAREST_EVEN)
            codes[k, :, cols] = code.astype(jnp.int32).astype(jnp.int16)
            scales[k, :, cols] = peak * (1.0 / CODES)

        by_columns(body, codes.shape[2])

    def decoded(k, cols):
        return boxes[k, :, cols].astype(jnp.int32).astype(jnp.float32) * box_scales[k, :, cols]

    return encode, decoded


def ring_reduce(axis, part, codes, scales, boxes, box_scales, send, recv):
    me = lax.axis_index(axis)
    right, left, far = (lax.rem(me + k, 4) for k in (1, 3, 2))
    half, width = part.shape[1] // 2, part.shape[2]
    top, low = pl.ds(0, half), pl.ds(half, half)

    encode, decoded = coder(codes, scales, boxes, box_scales)

    def message(k):
        target = left if k % 2 else right
        return [
            remote(codes.at[k], boxes.at[k], send.at[k, 0], recv.at[k, 0], axis, target),
            remote(scales.at[k], box_scales.at[k], send.at[k, 1], recv.at[k, 1], axis, target),
        ]

    def post(k, value):
        encode(k, value)
        for c in message(k):
            c.start()

    def arrived(*which):
        for k in which:
            for c in message(k):
                c.wait_recv()

    def start():
        post(0, lambda cols: part[far, top, cols])
        post(1, lambda cols: part[far, low, cols])
        post(2, lambda cols: part[right, low, cols])
        post(3, lambda cols: part[left, top, cols])

    def relay():
        arrived(0)
        post(4, lambda cols: part[right, top, cols] + decoded(0, cols))
        arrived(1)
        post(5, lambda cols: part[left, low, cols] + decoded(1, cols))

    def finish(store):
        arrived(3, 4)
        by_columns(
            lambda cols: store(0, cols, part[me, top, cols] + decoded(3, cols) + decoded(4, cols)),
            width,
        )
        arrived(2, 5)
        by_columns(
            lambda cols: store(1, cols, part[me, low, cols] + decoded(2, cols) + decoded(5, cols)),
            width,
        )
        for k in range(6):
            for c in message(k):
                c.wait_send()

    return start, relay, finish


TOKENS = 256
UNROLL = 4
WIDE = 256
NT = (((1,), (1,)), ((), ()))
TN = (((0,), (0,)), ((), ()))


def dot(a, b, dims=(((1,), (0,)), ((), ()))):
    return lax.dot_general(a, b, dims, preferred_element_type=jnp.float32)


def gather_stream(held, slabs, send, recv, short=False):
    y, x, z, core = (lax.axis_index(a) for a in AXES[:4])
    near = {"dp_0": [lax.rem(y + k, 4) for k in (1, 3)], "dp_1": [lax.rem(x + k, 4) for k in (1, 3)]}
    every = slice(None)
    live = []

    def go(spot, k, axis, target):
        ref = held.at[(slabs, *spot)]
        c = remote(ref, ref, send.at[k], recv.at[k], axis, target)
        c.start()
        live.append(c)
        return c

    def ring_direct(first):
        for half, axis in enumerate(("dp_1", "dp_0") if first else ("dp_0", "dp_1")):
            if first:
                spot = (y, x, every, core, half)
            elif half == 0:
                spot = (y, every, every, core, half)
            else:
                spot = (every, x, every, core, half)
            for side in range(2):
                k = (1 if first else 9) + 4 * half + side
                go(spot, k, axis, near[axis][side])

    def ring_relay(first):
        base = 1 if first else 9
        direct = live[-4:]
        for half, axis in enumerate(("dp_1", "dp_0") if first else ("dp_0", "dp_1")):
            for side in range(2):
                direct[2 * half + side].wait_recv()
                back = near[axis][1 - side]
                if first:
                    spot = (y, back) if axis == "dp_1" else (back, x)
                else:
                    spot = (every, back) if axis == "dp_1" else (back, every)
                go((*spot, side, core, half), base + 4 * half + 2 + side, axis, near[axis][side])

    def across(k, spot):
        go((*spot[:3], core, spot[3]), k, "dp_3", 1 - core)

    def ring_straight():
        for half, (axis, me) in enumerate([("dp_1", x), ("dp_0", y)]):
            for k in (1, 2, 3):
                go((y, x, every, core, half), 3 * half + k - 1, axis, lax.rem(me + k, 4))

    def step(k):
        if short:
            k = k + 2
        if k == 0:
            go((y, x, z, core), 0, "dp_2", 1 - z)
        elif k == 1:
            live[-1].wait_recv()
            ring_direct(True)
        elif k == 2:
            ring_straight() if short else ring_relay(True)
        elif k == 3:
            for c in live[-6:] if short else live[-4:]:
                c.wait_recv()
            ring_direct(False)
        elif k == 4:
            ring_relay(False)
            relays.extend(live[-4:])
            across(17, (y, every, every, 0))
            across(18, (every, x, every, 1))
            for n in range(2):
                across(19 + 2 * n, (near["dp_0"][n], every, every, 0))
                across(20 + 2 * n, (every, near["dp_1"][n], every, 1))
        elif k == 5:
            for c in relays:
                c.wait_recv()
            across(23, (lax.rem(y + 2, 4), every, every, 0))
            across(24, (every, lax.rem(x + 2, 4), every, 1))
        else:
            for c in live[-8:]:
                c.wait_recv()
            for c in live:
                c.wait_send()

    relays = []
    return step


def three_terms(v8):
    high = v8.astype(jnp.bfloat16).astype(jnp.float32)
    rest = v8 - high
    middle = rest.astype(jnp.bfloat16).astype(jnp.float32)
    low = rest - middle
    group = lax.broadcasted_iota(jnp.int32, v8.shape, 1) // 16
    picked = jnp.where(
        (group == 0) | (group == 1) | (group == 3),
        high,
        jnp.where((group == 2) | (group == 5), middle, jnp.where(group == 4, low, 0.0)),
    )
    return picked.astype(jnp.bfloat16)


def eightfold(rows):
    v = jnp.broadcast_to(rows[:, None], (32, 8, 128)).reshape(TOKENS, 128)
    token = lax.broadcasted_iota(jnp.int32, v.shape, 0) % 8
    lane = lax.broadcasted_iota(jnp.int32, v.shape, 1)
    v = jnp.where(lane // 16 == token, v, 0.0)
    across = lax.broadcasted_iota(jnp.int32, (128, 128), 1) % 16
    down = lax.broadcasted_iota(jnp.int32, (128, 128), 0) % 16
    spread = jnp.where(across == down, 1.0, 0.0).astype(jnp.bfloat16)
    high = v.astype(jnp.bfloat16)
    rest = v - high.astype(jnp.float32)
    middle = rest.astype(jnp.bfloat16)
    low = (rest - middle.astype(jnp.float32)).astype(jnp.bfloat16)
    return dot(high, spread) + dot(middle, spread) + dot(low, spread)


def picked_level(step, offset, values):
    out = jnp.float32(0.0)
    for k in range(1, K + 1):
        out = jnp.where(step == k, jnp.float32(values[2 * k + offset]), out)
    return out


def step_kernel(
    timestep,
    bucket,
    bucket_weights,
    clean,
    noise,
    tables,
    teacher_embed,
    teacher_final,
    teacher_mod,
    student_embed,
    student_final,
    student_mod,
    teacher_qkv,
    teacher_out_far,
    student_qkv,
    student_out,
    out_far,
    totals,
    out,
    held,
    near_qkv,
    teacher_out,
    wide,
    shaped,
    shaped_s,
    qkv,
    heads,
    heads_in,
    weights,
    terms,
    inverses,
    d_attn,
    embed_t,
    embed_s,
    final_b,
    lat_rows,
    shaped_t,
    proj_t,
    shaped_in,
    proj_in,
    packed_in,
    part_c,
    part_d,
    qkv_sem,
    out_sem,
    grads_sem,
    swap_send,
    swap_recv,
    t_send,
    t_recv,
    s_send,
    s_recv,
    o_send,
    o_recv,
    *rest,
):
    boxes = [rest[4 * k : 4 * k + 4] for k in range(10)]
    last, pair_send, pair_recv, send, recv, z_send, z_recv = rest[40:47]
    inbox, sum_send, sum_recv = rest[47:]
    hidden, hidden_s, mixed, placed = (wide.at[k] for k in range(4))
    packed = near_qkv.at[0, pl.ds(0, 3 * TOKENS)]
    y, x, z, core, mp = (lax.axis_index(a) for a in AXES)
    load_out = pltpu.make_async_copy(teacher_out_far, teacher_out, out_sem)
    load_out.start()
    load = pltpu.make_async_copy(teacher_qkv, near_qkv, qkv_sem)
    load.start()
    held[0:3, y, x, z, core] = student_qkv[...]
    held[3, y, x, z, core] = student_out[...]
    both = ("dp_2", "mp")
    greet([friend for _, partners in all_places() for friend in partners])

    def swap(src, dst, k, axis="mp", target=None):
        target = 1 - mp if target is None else target
        return remote(src, dst, swap_send.at[k], swap_recv.at[k], axis, target)

    load_out.wait()
    spot = (y, x, z, core)
    here = teacher_out.at[spot]
    swaps = [
        swap(here, held.at[(5, *spot)], 0),
        swap(here, held.at[(5, *spot)], 1, both, (1 - z, 1 - mp)),
        swap(student_out, held.at[(4, *spot)], 15),
        swap(student_out, held.at[(4, *spot)], 16, both, (1 - z, 1 - mp)),
    ]
    for c in swaps:
        c.start()
    t_step = gather_stream(held, pl.ds(5, 1), t_send, t_recv, short=True)
    s_step = gather_stream(held, pl.ds(0, 4), s_send, s_recv)
    o_step = gather_stream(held, pl.ds(4, 1), o_send, o_recv, short=True)
    s_step(0)

    step = timestep[0]
    a_f, a_m, a_l = (picked_level(step, -k, ALPHAS) for k in range(3))
    s_f, s_m, s_l = (picked_level(step, -k, SIGMAS) for k in range(3))
    row_weight = bucket_weights[jnp.clip(bucket[0], 0, NBUCKET - 1)]
    places = [
        (teacher_mod, jnp.clip(2 * step - 1, 0, TGRID - 1)),
        (teacher_mod, jnp.clip(2 * step - 2, 0, TGRID - 1)),
        (student_mod, jnp.clip(step - 1, 0, K - 1)),
    ]
    modrows = [[mod[j, pl.ds(at, 1), :] for j in range(3)] for mod, at in places]

    def split_rows(ref):
        v = ref[...]
        h = v.astype(jnp.bfloat16)
        rest = v - h.astype(jnp.float32)
        m = rest.astype(jnp.bfloat16)
        return h, m, (rest - m.astype(jnp.float32)).astype(jnp.bfloat16)

    def stack(parts, out):
        h, m, l = parts
        for k, v in enumerate([h, m, h, l, h, m, jnp.zeros_like(h), jnp.zeros_like(h)]):
            out[16 * k : 16 * k + 16] = v

    def repeat(parts, out):
        for k in range(24):
            out[16 * k : 16 * k + 16] = parts[k // 8]

    def columns(k, width):
        return pl.ds(pl.multiple_of(k * width, width), width)

    def spread(v8, b_ref, out, base=None):
        terms8 = three_terms(v8)

        for n in range(D // WIDE):
            cols = pl.ds(n * WIDE, WIDE)
            h = dot(terms8, b_ref[:, cols])
            out[:, cols] = h if base is None else h + base[:, cols]

    def centred(v):
        mean = jnp.mean(v, axis=-1, keepdims=True)
        c = v - mean
        return c, lax.rsqrt(jnp.mean(c * c, axis=-1, keepdims=True) + LN_EPS), mean

    def by_rows(body):
        def group(n, carry):
            for u in range(UNROLL):
                body(pl.ds(pl.multiple_of(n * (16 * UNROLL) + 16 * u, 16), 16))
            return carry

        lax.fori_loop(0, TOKENS // (16 * UNROLL), group, 0)

    def shape(hid, which, out):
        shift, scale = modrows[which][0], 1.0 + modrows[which][1]

        def body(rows):
            c, inv, _ = centred(hid[rows])
            out[rows] = (c * inv * scale + shift).astype(jnp.bfloat16)

        by_rows(body)

    def project(src, weight):
        def body(j, carry):
            qkv[j] = dot(src[...], weight(j)).astype(jnp.bfloat16)
            return carry

        lax.fori_loop(0, 3, body, 0)

    lane = lax.broadcasted_iota(jnp.int32, (1, 128), 1)
    low_f = jnp.where(lane < 64, 1.0, 0.0)
    sides = [low_f.astype(jnp.bfloat16), (1.0 - low_f).astype(jnp.bfloat16)]
    is_low = lax.broadcasted_iota(jnp.int32, (TOKENS, 128), 1) < 64

    def swap_pair(which, hp):
        cols = pl.ds(128 * hp, 128)
        return swap(heads.at[which, :, cols], heads_in.at[which, :, cols], 3 + 4 * which + hp)

    def attend(which, keep):
        for hp in range(4):
            cols = pl.ds(128 * hp, 128)
            q, k, v = qkv[0, :, cols], qkv[1, :, cols], qkv[2, :, cols]
            outs = []
            for h in range(2):
                s = dot(q * sides[h], k, NT) * 0.125
                e = jnp.exp(s - jnp.max(s, axis=-1, keepdims=True))
                w = e / jnp.sum(e, axis=-1, keepdims=True)
                if keep:
                    weights[2 * hp + h] = w
                outs.append(dot(w.astype(jnp.bfloat16), v))
            heads[which, :, cols] = jnp.where(is_low, outs[0], outs[1]).astype(jnp.bfloat16)
            if hp > 0:
                swap_pair(which, hp - 1).start()
        swap_pair(which, 3).start()

    def swapped(which):
        for hp in range(4):
            swap_pair(which, hp).wait_recv()

    def mix(att, weight, which, base):
        mod_ref, at = places[which]

        for n in range(4):
            cols = pl.ds(n * 512, 512)
            p = dot(att[...], weight(n), NT)
            mixed[:, cols] = base[:, cols] + mod_ref[2, pl.ds(at, 1), cols] * p

    def predict(final, keep):
        def body(rows):
            c, inv, mean = centred(mixed[rows])
            u = c * inv
            if keep:
                inverses[0, rows] = jnp.broadcast_to(inv, (16, 128))
                inverses[1, rows] = jnp.broadcast_to(mean, (16, 128))
            high = u.astype(jnp.bfloat16)
            rest = u - high.astype(jnp.float32)
            middle = rest.astype(jnp.bfloat16)
            terms[0, rows] = high
            terms[1, rows] = middle
            terms[2, rows] = (rest - middle.astype(jnp.float32)).astype(jnp.bfloat16)

        by_rows(body)
        r = dot(terms[0], final[...], NT)
        m = dot(terms[1], final[0:256], NT)
        small = dot(terms[2], final[0:128], NT)
        return (
            r[:, 0:128]
            + (r[:, 128:256] + m[:, 0:128])
            + (r[:, 256:384] + m[:, 128:256] + small)
        )

    def other_rows(slab):
        return lambda n: held[slab, n].reshape(512, 512)

    def near_rows(n):
        return teacher_out[n].reshape(512, 512)

    def turn(src, out):
        def body(n, carry):
            t = src[:, columns(n, 128)].astype(jnp.float32).T.astype(jnp.bfloat16)
            out[pl.ds(2 * n, 2)] = t.reshape(2, 2, 32, TOKENS)
            return carry

        lax.fori_loop(0, D // 128, body, 0)

    def pair(k):
        if k < 2:
            src, dst = ((shaped_t, shaped_in), (proj_t, proj_in))[k]
            src = src.at[:, 1 - core]
        elif k == 2:
            src, dst = heads.at[2], packed_in.at[pl.ds(3 * TOKENS, TOKENS)]
        elif k == 3:
            rows = pl.ds(2 * TOKENS, TOKENS)
            src, dst = packed.at[rows], packed_in.at[rows]
        else:
            rows, cols = pl.ds(0, 2 * TOKENS), pl.ds(128 * (k - 4), 128)
            src, dst = packed.at[rows, cols], packed_in.at[rows, cols]
        return remote(src, dst, pair_send.at[k], pair_recv.at[k], "dp_3", 1 - core)

    half = D // 2
    for k in range(16):
        sin_a, cos_a = tables[0, k : k + 1], tables[1, k : k + 1]
        rows = pl.ds(16 * k, 16)
        placed[rows, :half] = sin_a * tables[3] + cos_a * tables[2]
        placed[rows, half:] = cos_a * tables[3] - sin_a * tables[2]
    stack(split_rows(teacher_embed), embed_t)
    latents = a_f * clean[...] + s_f * noise[...]
    for k in range(32):
        lat_rows[k : k + 1] = latents[:, 128 * k : 128 * k + 128]
    lat0 = eightfold(lat_rows[...])
    spread(lat0, embed_t, hidden, placed)
    shape(hidden, 0, shaped)
    swaps[0].wait_recv()
    swaps[1].wait_recv()
    t_step(0)
    s_step(1)
    load.wait()
    project(shaped, lambda j: near_qkv[j])
    t_step(1)
    attend(0, False)
    s_step(2)
    t_step(2)
    mix(heads.at[0], near_rows, 0, hidden)
    s_step(3)
    repeat(split_rows(teacher_final), final_b)
    t_step(3)
    t_step(4)
    swapped(0)
    mix(heads_in.at[0], other_rows(5), 0, mixed)
    eps0 = predict(final_b, False)
    lat1 = a_m * (lat0 - s_f * eps0) / a_f + s_m * eps0

    spread(lat1, embed_t, hidden, placed)
    shape(hidden, 1, shaped)
    project(shaped, lambda j: near_qkv[j])
    s_step(4)
    swaps[2].wait_recv()
    swaps[3].wait_recv()
    o_step(0)
    attend(1, False)
    mix(heads.at[1], near_rows, 1, hidden)
    stack(split_rows(student_embed), embed_s)
    spread(lat0, embed_s, hidden_s, placed)
    shape(hidden_s, 2, shaped_s)
    swapped(1)
    mix(heads_in.at[1], other_rows(5), 1, mixed)
    s_step(5)
    o_step(1)
    eps1 = predict(final_b, False)
    lat2 = a_l * (lat1 - s_m * eps1) / a_m + s_l * eps1
    target = (lat0 - a_f / a_l * lat2) / (s_f - a_f * s_l / a_l)

    student_terms = split_rows(student_final)
    repeat(student_terms, final_b)
    stack(student_terms, embed_t)
    s_step(6)
    project(shaped_s, lambda j: held[j].reshape(D, 512))
    o_step(2)
    attend(2, True)
    mix(heads.at[2], other_rows(3), 2, hidden_s)
    o_step(3)
    turn(shaped_s, shaped_t)
    swapped(2)
    o_step(4)
    mix(heads_in.at[2], other_rows(4), 2, mixed)
    pair(0).start()
    error = predict(final_b, True) - target
    lanes = lax.broadcasted_iota(jnp.int32, error.shape, 1)
    loss_part = (
        0.5 * row_weight * jnp.sum(jnp.where(lanes < 16, error * error, 0.0))
    )

    spread(2.0 * row_weight * error, embed_t, hidden)

    gate = modrows[2][2]

    def back(rows):
        inv, mean = inverses[0, rows, 0:1], inverses[1, rows, 0:1]
        up, u = hidden[rows], (mixed[rows] - mean) * inv
        first_mean = jnp.mean(up, axis=-1, keepdims=True)
        second_mean = jnp.mean(up * u, axis=-1, keepdims=True)
        d = (up - first_mean - u * second_mean) * inv
        shaped[rows] = (gate * d).astype(jnp.bfloat16)

    by_rows(back)
    turn(shaped, proj_t)
    pair(2).start()
    d_attn[...] = dot(shaped[...], held[3].reshape(D, 512)).astype(jnp.bfloat16)
    pair(1).start()

    extents = [(0, 2 * WIDE), (2 * WIDE, 2 * WIDE)]

    def products(s_ref, b_ref, first, count, add):
        def body(k, carry):
            lhs = s_ref[pl.ds(pl.multiple_of(k * 8, 8), 8)].reshape(256, TOKENS)
            spot = pl.ds(pl.multiple_of(k * 64, 64), 64)
            for j in range(count):
                g = dot(lhs, b_ref[TOKENS * j : TOKENS * (j + 1)])
                cols = pl.ds(WIDE * (first + j), WIDE)
                for i in range(4):
                    block = g[64 * i : 64 * i + 64, :WIDE]
                    wide[i, spot, cols] = wide[i, spot, cols] + block if add else block
                cols = pl.ds(HALF + WIDE * (first + j), WIDE)
                right = g[:, WIDE:]
                wide[k, :, cols] = wide[k, :, cols] + right if add else right
            return carry

        lax.fori_loop(0, 4, body, 0)

    rings = []
    for which, (offset, width) in enumerate(extents):
        for way in range(2):
            for stage in range(2):
                n = len(rings)
                if stage == 0:
                    part = wide.at[:, :, pl.ds(HALF * way + offset, width)]
                else:
                    part = (part_c, part_d)[way].at[:, :, pl.ds(offset, width)]
                axis = ("dp_1", "dp_0")[(way + stage) % 2]
                rings.append(ring_reduce(axis, part, *boxes[n], send.at[n], recv.at[n]))

    def ring_step(which, stage, step):
        offset, width = extents[which]
        for way in range(2):

            def into(half, cols, value, way=way):
                if stage == 0:
                    part = (part_c, part_d)[way].at[:, :, pl.ds(offset, width)]
                    part[2 * half, :, cols] = value[:64]
                    part[2 * half + 1, :, cols] = value[64:]
                else:
                    last.at[way, half, :, pl.ds(offset, width)][:, cols] = value

            do = rings[4 * which + 2 * way + stage][step]
            do(into) if step == 2 else do()

    def z_copies(which):
        codes, scales, codes_in, scales_in = boxes[8 + which]
        return [
            remote(a, b, z_send.at[2 * which + k], z_recv.at[2 * which + k], "dp_2", 1 - z)
            for k, (a, b) in enumerate([(codes, codes_in), (scales, scales_in)])
        ]

    def z_start(which):
        encode, _ = coder(*boxes[8 + which])
        offset, width = extents[which]
        for way in range(2):
            encode(way, lambda cols, way=way: last.at[way, 1 - z, :, pl.ds(offset, width)][:, cols])
        for c in z_copies(which):
            c.start()

    for hp in range(4):
        cols = pl.ds(128 * hp, 128)
        da = d_attn[:, cols]
        outs = [dot(weights[2 * hp + h].astype(jnp.bfloat16), da, TN) for h in range(2)]
        packed[2 * TOKENS :, cols] = jnp.where(is_low, outs[0], outs[1]).astype(jnp.bfloat16)
    products(proj_t.at[:, core], heads.at[2], 3, 1, False)
    pair(3).start()
    pair(1).wait_recv()
    pair(2).wait_recv()
    products(proj_in, packed_in.at[pl.ds(3 * TOKENS, TOKENS)], 3, 1, True)
    products(shaped_t.at[:, core], packed.at[pl.ds(2 * TOKENS, TOKENS)], 2, 1, False)
    pair(0).wait_recv()
    pair(3).wait_recv()
    products(shaped_in, packed_in.at[pl.ds(2 * TOKENS, TOKENS)], 2, 1, True)
    ring_step(1, 0, 0)
    for hp in range(4):
        cols = pl.ds(128 * hp, 128)
        q, k, v, da = qkv[0, :, cols], qkv[1, :, cols], qkv[2, :, cols], d_attn[:, cols]
        outs = []
        for h in range(2):
            w = weights[2 * hp + h]
            dp = dot(da * sides[h], v, NT)
            ds = w * (dp - jnp.sum(w * dp, axis=-1, keepdims=True)) * 0.125
            ds = ds.astype(jnp.bfloat16)
            outs.append((dot(ds, k), dot(ds, q, TN)))
        for j in range(2):
            joined = jnp.where(is_low, outs[0][j], outs[1][j]).astype(jnp.bfloat16)
            packed[TOKENS * j : TOKENS * (j + 1), cols] = joined
        if hp > 0:
            pair(3 + hp).start()
    pair(7).start()
    products(shaped_t.at[:, core], packed, 0, 2, False)
    ring_step(1, 0, 1)
    for k in (4, 5, 6, 7):
        pair(k).wait_recv()
    products(shaped_in, packed_in, 0, 2, True)
    ring_step(0, 0, 0)
    ring_step(1, 0, 2)
    ring_step(0, 0, 1)
    ring_step(0, 0, 2)
    ring_step(0, 1, 0)
    ring_step(1, 1, 0)
    ring_step(0, 1, 1)
    ring_step(1, 1, 1)
    ring_step(0, 1, 2)
    z_start(0)
    ring_step(1, 1, 2)
    z_start(1)
    for which, (offset, width) in enumerate(extents):
        _, decoded = coder(*boxes[8 + which])
        for c in z_copies(which):
            c.wait_recv()
        for way in range(2):
            for j in range(offset // WIDE, (offset + width) // WIDE):
                cols, near = pl.ds(WIDE * j, WIDE), pl.ds(WIDE * j - offset, WIDE)
                out[j, :, pl.ds(WIDE * way, WIDE)] = last[way, z, :, cols] + decoded(way, near)
    leave = pltpu.make_async_copy(out, out_far, grads_sem)
    leave.start()
    squares = jnp.sum(out[...] * out[...])
    row = lax.broadcasted_iota(jnp.int32, (8, 128), 0)
    value = jnp.where(row == 0, squares, loss_part)
    totals[...] = sum_over_all(value, inbox, sum_send, sum_recv)
    leave.wait()
    for c in [*z_copies(0), *z_copies(1)]:
        c.wait_send()
    for c in swaps:
        c.wait_send()
    for k in range(8):
        pair(k).wait_send()
    for which in range(3):
        for hp in range(4):
            swap_pair(which, hp).wait_send()


def levels():
    lamb = 6.0 - 12.0 * np.arange(TGRID + 1) / TGRID
    return [np.sqrt(1.0 / (1.0 + np.exp(sign * lamb))).astype(np.float32) for sign in (-1.0, 1.0)]


ALPHAS, SIGMAS = levels()


def position_tables():
    half = D // 2
    freqs = np.exp(-math.log(10000.0) * np.arange(half) / half)
    fine = np.arange(16)[:, None] * freqs[None]
    angles = (np.sin(16.0 * fine), np.cos(16.0 * fine), np.sin(fine), np.cos(fine))
    return np.stack(angles).astype(np.float32)


def whole_step(timestep, bucket, bucket_weights, clean, noise, teacher, student):
    vmem, smem = (pl.BlockSpec(memory_space=m) for m in (pltpu.VMEM, pltpu.SMEM))
    bf16, f32 = jnp.bfloat16, jnp.float32

    def boxes(width):
        return [
            scratch
            for half in (128, 32, 128, 32)
            for scratch in [pltpu.VMEM((6, half, width), jnp.int16), pltpu.VMEM((6, 1, width), f32)] * 2
        ]

    def last_boxes(width):
        return [pltpu.VMEM((2, 32, width), jnp.int16), pltpu.VMEM((2, 1, width), f32)] * 2

    def semaphores(*shape):
        return [pltpu.SemaphoreType.DMA(shape)] * 2

    return pl.pallas_call(
        step_kernel,
        out_shape=(
            jax.ShapeDtypeStruct((4, 32, 512), f32),
            jax.ShapeDtypeStruct((8, 128), f32),
        ),
        in_specs=[smem] * 3 + [vmem] * 9 + [pl.BlockSpec(memory_space=pl.ANY)] * 2 + [vmem] * 2,
        out_specs=(pl.BlockSpec(memory_space=pl.ANY), vmem),
        scratch_shapes=[
            pltpu.VMEM((4, 32, 512), f32),
            pltpu.VMEM((6, 4, 4, 2, 2, 2, 16, 512), bf16),
            pltpu.VMEM((3, D, 512), bf16),
            pltpu.VMEM((4, 4, 2, 2, 2, 16, 512), bf16),
            pltpu.VMEM((4, TOKENS, D), f32),
            pltpu.VMEM((TOKENS, D), bf16),
            pltpu.VMEM((TOKENS, D), bf16),
            pltpu.VMEM((3, TOKENS, 512), bf16),
            pltpu.VMEM((3, TOKENS, 512), bf16),
            pltpu.VMEM((3, TOKENS, 512), bf16),
            pltpu.VMEM((8, TOKENS, TOKENS), f32),
            pltpu.VMEM((3, TOKENS, D), bf16),
            pltpu.VMEM((2, TOKENS, 128), f32),
            pltpu.VMEM((TOKENS, 512), bf16),
            pltpu.VMEM((128, D), bf16),
            pltpu.VMEM((128, D), bf16),
            pltpu.VMEM((384, D), bf16),
            pltpu.VMEM((32, 128), f32),
            pltpu.VMEM((32, 2, 32, TOKENS), bf16),
            pltpu.VMEM((32, 2, 32, TOKENS), bf16),
            pltpu.VMEM((32, 32, TOKENS), bf16),
            pltpu.VMEM((32, 32, TOKENS), bf16),
            pltpu.VMEM((4 * TOKENS, 512), bf16),
            pltpu.VMEM((4, 64, HALF), f32),
            pltpu.VMEM((4, 64, HALF), f32),
            pltpu.SemaphoreType.DMA,
            pltpu.SemaphoreType.DMA,
            pltpu.SemaphoreType.DMA,
            *semaphores(17),
            *semaphores(25),
            *semaphores(25),
            *semaphores(25),
            *boxes(2 * WIDE),
            *boxes(2 * WIDE),
            *last_boxes(2 * WIDE),
            *last_boxes(2 * WIDE),
            pltpu.VMEM((2, 2, 32, HALF), f32),
            *semaphores(8),
            *semaphores(8, 6, 2),
            *semaphores(4),
            pltpu.VMEM((2, 16, 8, 128), f32),
            *semaphores(2, 15),
        ],
        compiler_params=pltpu.CompilerParams(
            collective_id=2, has_side_effects=True, vmem_limit_bytes=63 * 2**20
        ),
    )(
        timestep,
        bucket,
        bucket_weights,
        clean,
        noise,
        jnp.asarray(position_tables()),
        teacher[0],
        teacher[1],
        jnp.moveaxis(teacher[2], 1, 0),
        student[0],
        student[1],
        jnp.moveaxis(student[2], 1, 0),
        jnp.moveaxis(teacher[3], 1, 0),
        teacher[4].reshape(4, 4, 2, 2, 2, 16, 512),
        jnp.moveaxis(student[3], 1, 0).reshape(3, 2, 16, 512),
        student[4].reshape(2, 16, 512),
    )


def adam_kernel(grads, totals, mq, vq, mo, vo, new_mq, new_vq, up_q, new_mo, new_vo, up_o, loss):
    rms = jnp.sqrt(totals[0:1, 0:1] / (4 * D * INNER))
    factor = 1.0 / jnp.maximum(rms, 1.0)

    def adam(grad, moment, second, new_moment, new_second, update):
        normed = grad * factor
        m = BETA_ONE * moment + (1.0 - BETA_ONE) * normed
        v = BETA_TWO * second + (1.0 - BETA_TWO) * normed * normed
        new_moment[...] = m
        new_second[...] = v
        update[...] = m / (jnp.sqrt(v) + ADAM_EPS)

    for j in range(3):
        adam(grads[j], mq[j], vq[j], new_mq.at[j], new_vq.at[j], up_q.at[j])
    adam(grads[3], mo[...], vo[...], new_mo, new_vo, up_o)
    loss[...] = totals[1:2, 0:1] / (SAMPLES * LATENT)


def adam_update(grads, totals, moment_qkv, second_qkv, moment_out, second_out):
    vmem = pl.BlockSpec(memory_space=pltpu.VMEM)
    mq, vq = (jnp.moveaxis(v, 1, 0) for v in (moment_qkv, second_qkv))
    qkv, out = (jax.ShapeDtypeStruct(v.shape, v.dtype) for v in (mq, moment_out))
    *news, loss = pl.pallas_call(
        adam_kernel,
        out_shape=(qkv, qkv, qkv, out, out, out, jax.ShapeDtypeStruct((1, 1), jnp.float32)),
        in_specs=[vmem] * 6,
        out_specs=(vmem,) * 7,
    )(grads, totals, mq, vq, moment_out, second_out)
    return (*(jnp.moveaxis(v, 0, 1) for v in news[:3]), *news[3:], loss.reshape(()))


def per_device(
    clean_latent,
    noise_draw,
    timestep,
    bucket,
    bucket_weights,
    teacher_embed,
    teacher_final,
    teacher_mod,
    teacher_qkv,
    teacher_out,
    student_embed,
    student_final,
    student_mod,
    student_qkv,
    student_out,
    moment_qkv,
    second_qkv,
    moment_out,
    second_out,
):
    grads, totals = whole_step(
        timestep,
        bucket,
        bucket_weights,
        clean_latent,
        noise_draw,
        (teacher_embed, teacher_final, teacher_mod, teacher_qkv, teacher_out),
        (student_embed, student_final, student_mod, student_qkv, student_out),
    )
    return adam_update(grads, totals, moment_qkv, second_qkv, moment_out, second_out)


def solution(mesh):
    torus = Mesh(
        mesh.devices.reshape(4, 4, 2, 2, mesh.shape["mp"]), ("dp_0", "dp_1", "dp_2", "dp_3", "mp")
    )
    in_specs = (
        P(DP, None),
        P(DP, None),
        P(DP),
        P(DP),
        P(),
        P(),
        P(),
        P(),
        P(None, None, "mp"),
        P(None, "mp"),
        P(),
        P(),
        P(),
        P(DP, None, "mp"),
        P(DP, "mp"),
        P(DP, None, "mp"),
        P(DP, None, "mp"),
        P(DP, "mp"),
        P(DP, "mp"),
    )
    out_specs = (
        P(DP, None, "mp"),
        P(DP, None, "mp"),
        P(DP, None, "mp"),
        P(DP, "mp"),
        P(DP, "mp"),
        P(DP, "mp"),
        P(),
    )
    return jax.shard_map(
        per_device, mesh=torus, in_specs=in_specs, out_specs=out_specs, check_vma=False
    )
```

```python
import math

import jax
import jax.numpy as jnp
import numpy as np
from jax import lax
from jax.experimental import pallas as pl
from jax.experimental.pallas import tpu as pltpu
from jax.sharding import Mesh
from jax.sharding import PartitionSpec as P

D = 2048
HS = 64
INNER = 1024
PATCH_CH = 16
SEQ = 256
LATENT = 4096
SAMPLES = 64
K = 8
TGRID = 16
NBUCKET = 8
DP = ("dp_0", "dp_1", "dp_2", "dp_3")
DP_MP = ("dp_0", "dp_1", "dp_2", "dp_3", "mp")


LN_EPS = 0.01
BETA_ONE = 0.9
BETA_TWO = 0.99
ADAM_EPS = 1e-08


ROWS = 1024
HALF = 1024
CODES = 32767.0
AXES = ("dp_0", "dp_1", "dp_2", "dp_3", "mp")


def remote(src, dst, send, recv, axis, target):
    return pltpu.make_async_remote_copy(
        src_ref=src,
        dst_ref=dst,
        send_sem=send,
        recv_sem=recv,
        device_id={axis: target} if isinstance(axis, str) else dict(zip(axis, target)),
        device_id_type=pl.DeviceIdType.MESH,
    )


def greet(friends):
    barrier = pltpu.get_barrier_semaphore()
    for axis, target in friends:
        pl.semaphore_signal(
            barrier,
            inc=1,
            device_id={axis: target} if isinstance(axis, str) else dict(zip(axis, target)),
            device_id_type=pl.DeviceIdType.MESH,
        )
    pl.semaphore_wait(barrier, len(friends))


def all_places():
    y, x, z, core, mp = (lax.axis_index(a) for a in AXES)
    axes, here = ("mp", "dp_2", "dp_3"), (mp, z, core)
    cube = []
    for k in range(1, 8):
        cube.append((axes, tuple(1 - h if k >> n & 1 else h for n, h in enumerate(here))))
    plane = []
    for k in range(1, 16):
        plane.append((("dp_0", "dp_1"), (lax.rem(y + k // 4, 4), lax.rem(x + k % 4, 4))))
    return [(4 * mp + 2 * z + core, cube), (4 * y + x, plane)]


def sum_over_all(value, inbox, send, recv):
    for stage, (slot, partners) in enumerate(all_places()):
        inbox[stage, slot] = value
        copies = [
            remote(
                inbox.at[stage, slot],
                inbox.at[stage, slot],
                send.at[stage, k],
                recv.at[stage, k],
                axis,
                target,
            )
            for k, (axis, target) in enumerate(partners)
        ]
        for c in copies:
            c.start()
        for c in copies:
            c.wait_recv()
        value = inbox[stage, 0]
        for k in range(1, len(partners) + 1):
            value = value + inbox[stage, k]
        for c in copies:
            c.wait_send()
    return value


def by_columns(body, width):
    def step(n, carry):
        body(pl.ds(pl.multiple_of(n * 256, 256), 256))
        return carry

    lax.fori_loop(0, width // 256, step, 0)


def coder(codes, scales, boxes, box_scales):
    def encode(k, value):
        def body(cols):
            v = value(cols)
            peak = jnp.maximum(jnp.max(jnp.abs(v), axis=0, keepdims=True), 1e-30)
            code = lax.round(v * (CODES / peak), lax.RoundingMethod.TO_NEAREST_EVEN)
            codes[k, :, cols] = code.astype(jnp.int32).astype(jnp.int16)
            scales[k, :, cols] = peak * (1.0 / CODES)

        by_columns(body, codes.shape[2])

    def decoded(k, cols):
        return boxes[k, :, cols].astype(jnp.int32).astype(jnp.float32) * box_scales[k, :, cols]

    return encode, decoded


def ring_reduce(axis, part, codes, scales, boxes, box_scales, send, recv):
    me = lax.axis_index(axis)
    right, left, far = (lax.rem(me + k, 4) for k in (1, 3, 2))
    half, width = part.shape[1] // 2, part.shape[2]
    top, low = pl.ds(0, half), pl.ds(half, half)

    encode, decoded = coder(codes, scales, boxes, box_scales)

    def message(k):
        target = left if k % 2 else right
        return [
            remote(codes.at[k], boxes.at[k], send.at[k, 0], recv.at[k, 0], axis, target),
            remote(scales.at[k], box_scales.at[k], send.at[k, 1], recv.at[k, 1], axis, target),
        ]

    def post(k, value):
        encode(k, value)
        for c in message(k):
            c.start()

    def arrived(*which):
        for k in which:
            for c in message(k):
                c.wait_recv()

    def start():
        post(0, lambda cols: part[far, top, cols])
        post(1, lambda cols: part[far, low, cols])
        post(2, lambda cols: part[right, low, cols])
        post(3, lambda cols: part[left, top, cols])

    def relay():
        arrived(0)
        post(4, lambda cols: part[right, top, cols] + decoded(0, cols))
        arrived(1)
        post(5, lambda cols: part[left, low, cols] + decoded(1, cols))

    def finish(store):
        arrived(3, 4)
        by_columns(
            lambda cols: store(0, cols, part[me, top, cols] + decoded(3, cols) + decoded(4, cols)),
            width,
        )
        arrived(2, 5)
        by_columns(
            lambda cols: store(1, cols, part[me, low, cols] + decoded(2, cols) + decoded(5, cols)),
            width,
        )
        for k in range(6):
            for c in message(k):
                c.wait_send()

    return start, relay, finish


TOKENS = 256
UNROLL = 4
WIDE = 256
NT = (((1,), (1,)), ((), ()))
TN = (((0,), (0,)), ((), ()))


def dot(a, b, dims=(((1,), (0,)), ((), ()))):
    return lax.dot_general(a, b, dims, preferred_element_type=jnp.float32)


def gather_stream(held, slabs, send, recv, short=False):
    y, x, z, core = (lax.axis_index(a) for a in AXES[:4])
    near = {"dp_0": [lax.rem(y + k, 4) for k in (1, 3)], "dp_1": [lax.rem(x + k, 4) for k in (1, 3)]}
    every = slice(None)
    live = []

    def go(spot, k, axis, target):
        ref = held.at[(slabs, *spot)]
        c = remote(ref, ref, send.at[k], recv.at[k], axis, target)
        c.start()
        live.append(c)
        return c

    def ring_direct(first):
        for half, axis in enumerate(("dp_1", "dp_0") if first else ("dp_0", "dp_1")):
            if first:
                spot = (y, x, every, core, half)
            elif half == 0:
                spot = (y, every, every, core, half)
            else:
                spot = (every, x, every, core, half)
            for side in range(2):
                k = (1 if first else 9) + 4 * half + side
                go(spot, k, axis, near[axis][side])

    def ring_relay(first):
        base = 1 if first else 9
        direct = live[-4:]
        for half, axis in enumerate(("dp_1", "dp_0") if first else ("dp_0", "dp_1")):
            for side in range(2):
                direct[2 * half + side].wait_recv()
                back = near[axis][1 - side]
                if first:
                    spot = (y, back) if axis == "dp_1" else (back, x)
                else:
                    spot = (every, back) if axis == "dp_1" else (back, every)
                go((*spot, side, core, half), base + 4 * half + 2 + side, axis, near[axis][side])

    def across(k, spot):
        go((*spot[:3], core, spot[3]), k, "dp_3", 1 - core)

    def ring_straight():
        for half, (axis, me) in enumerate([("dp_1", x), ("dp_0", y)]):
            for k in (1, 2, 3):
                go((y, x, every, core, half), 3 * half + k - 1, axis, lax.rem(me + k, 4))

    def step(k):
        if short:
            k = k + 2
        if k == 0:
            go((y, x, z, core), 0, "dp_2", 1 - z)
        elif k == 1:
            live[-1].wait_recv()
            ring_direct(True)
        elif k == 2:
            ring_straight() if short else ring_relay(True)
        elif k == 3:
            for c in live[-6:] if short else live[-4:]:
                c.wait_recv()
            ring_direct(False)
        elif k == 4:
            ring_relay(False)
            relays.extend(live[-4:])
            across(17, (y, every, every, 0))
            across(18, (every, x, every, 1))
            for n in range(2):
                across(19 + 2 * n, (near["dp_0"][n], every, every, 0))
                across(20 + 2 * n, (every, near["dp_1"][n], every, 1))
        elif k == 5:
            for c in relays:
                c.wait_recv()
            across(23, (lax.rem(y + 2, 4), every, every, 0))
            across(24, (every, lax.rem(x + 2, 4), every, 1))
        else:
            for c in live[-8:]:
                c.wait_recv()
            for c in live:
                c.wait_send()

    relays = []
    return step


def three_terms(v8):
    high = v8.astype(jnp.bfloat16).astype(jnp.float32)
    rest = v8 - high
    middle = rest.astype(jnp.bfloat16).astype(jnp.float32)
    low = rest - middle
    group = lax.broadcasted_iota(jnp.int32, v8.shape, 1) // 16
    picked = jnp.where(
        (group == 0) | (group == 1) | (group == 3),
        high,
        jnp.where((group == 2) | (group == 5), middle, jnp.where(group == 4, low, 0.0)),
    )
    return picked.astype(jnp.bfloat16)


def eightfold(rows):
    v = jnp.broadcast_to(rows[:, None], (32, 8, 128)).reshape(TOKENS, 128)
    token = lax.broadcasted_iota(jnp.int32, v.shape, 0) % 8
    lane = lax.broadcasted_iota(jnp.int32, v.shape, 1)
    v = jnp.where(lane // 16 == token, v, 0.0)
    across = lax.broadcasted_iota(jnp.int32, (128, 128), 1) % 16
    down = lax.broadcasted_iota(jnp.int32, (128, 128), 0) % 16
    spread = jnp.where(across == down, 1.0, 0.0).astype(jnp.bfloat16)
    high = v.astype(jnp.bfloat16)
    rest = v - high.astype(jnp.float32)
    middle = rest.astype(jnp.bfloat16)
    low = (rest - middle.astype(jnp.float32)).astype(jnp.bfloat16)
    return dot(high, spread) + dot(middle, spread) + dot(low, spread)


def picked_level(step, offset, values):
    out = jnp.float32(0.0)
    for k in range(1, K + 1):
        out = jnp.where(step == k, jnp.float32(values[2 * k + offset]), out)
    return out


def step_kernel(
    timestep,
    bucket,
    bucket_weights,
    clean,
    noise,
    tables,
    teacher_embed,
    teacher_final,
    teacher_mod,
    student_embed,
    student_final,
    student_mod,
    teacher_qkv,
    teacher_out_far,
    student_qkv,
    student_out,
    out_far,
    totals,
    out,
    held,
    near_qkv,
    teacher_out,
    wide,
    shaped,
    shaped_s,
    qkv,
    heads,
    heads_in,
    weights,
    terms,
    inverses,
    d_attn,
    embed_t,
    embed_s,
    final_b,
    lat_rows,
    shaped_t,
    proj_t,
    shaped_in,
    proj_in,
    packed_in,
    part_c,
    part_d,
    qkv_sem,
    out_sem,
    grads_sem,
    swap_send,
    swap_recv,
    t_send,
    t_recv,
    s_send,
    s_recv,
    o_send,
    o_recv,
    *rest,
):
    boxes = [rest[4 * k : 4 * k + 4] for k in range(10)]
    last, pair_send, pair_recv, send, recv, z_send, z_recv = rest[40:47]
    inbox, sum_send, sum_recv = rest[47:]
    hidden, hidden_s, mixed, placed = (wide.at[k] for k in range(4))
    packed = near_qkv.at[0, pl.ds(0, 3 * TOKENS)]
    y, x, z, core, mp = (lax.axis_index(a) for a in AXES)
    load_out = pltpu.make_async_copy(teacher_out_far, teacher_out, out_sem)
    load_out.start()
    load = pltpu.make_async_copy(teacher_qkv, near_qkv, qkv_sem)
    load.start()
    held[0:3, y, x, z, core] = student_qkv[...]
    held[3, y, x, z, core] = student_out[...]
    both = ("dp_2", "mp")
    greet([friend for _, partners in all_places() for friend in partners])

    def swap(src, dst, k, axis="mp", target=None):
        target = 1 - mp if target is None else target
        return remote(src, dst, swap_send.at[k], swap_recv.at[k], axis, target)

    load_out.wait()
    spot = (y, x, z, core)
    here = teacher_out.at[spot]
    swaps = [
        swap(here, held.at[(5, *spot)], 0),
        swap(here, held.at[(5, *spot)], 1, both, (1 - z, 1 - mp)),
        swap(student_out, held.at[(4, *spot)], 15),
        swap(student_out, held.at[(4, *spot)], 16, both, (1 - z, 1 - mp)),
    ]
    for c in swaps:
        c.start()
    t_step = gather_stream(held, pl.ds(5, 1), t_send, t_recv, short=True)
    s_step = gather_stream(held, pl.ds(0, 4), s_send, s_recv)
    o_step = gather_stream(held, pl.ds(4, 1), o_send, o_recv, short=True)
    s_step(0)

    step = timestep[0]
    a_f, a_m, a_l = (picked_level(step, -k, ALPHAS) for k in range(3))
    s_f, s_m, s_l = (picked_level(step, -k, SIGMAS) for k in range(3))
    row_weight = bucket_weights[jnp.clip(bucket[0], 0, NBUCKET - 1)]
    places = [
        (teacher_mod, jnp.clip(2 * step - 1, 0, TGRID - 1)),
        (teacher_mod, jnp.clip(2 * step - 2, 0, TGRID - 1)),
        (student_mod, jnp.clip(step - 1, 0, K - 1)),
    ]
    modrows = [[mod[j, pl.ds(at, 1), :] for j in range(3)] for mod, at in places]

    def split_rows(ref):
        v = ref[...]
        h = v.astype(jnp.bfloat16)
        rest = v - h.astype(jnp.float32)
        m = rest.astype(jnp.bfloat16)
        return h, m, (rest - m.astype(jnp.float32)).astype(jnp.bfloat16)

    def stack(parts, out):
        h, m, l = parts
        for k, v in enumerate([h, m, h, l, h, m, jnp.zeros_like(h), jnp.zeros_like(h)]):
            out[16 * k : 16 * k + 16] = v

    def repeat(parts, out):
        for k in range(24):
            out[16 * k : 16 * k + 16] = parts[k // 8]

    def columns(k, width):
        return pl.ds(pl.multiple_of(k * width, width), width)

    def spread(v8, b_ref, out, base=None):
        terms8 = three_terms(v8)

        for n in range(D // WIDE):
            cols = pl.ds(n * WIDE, WIDE)
            h = dot(terms8, b_ref[:, cols])
            out[:, cols] = h if base is None else h + base[:, cols]

    def centred(v):
        mean = jnp.mean(v, axis=-1, keepdims=True)
        c = v - mean
        return c, lax.rsqrt(jnp.mean(c * c, axis=-1, keepdims=True) + LN_EPS), mean

    def by_rows(body):
        def group(n, carry):
            for u in range(UNROLL):
                body(pl.ds(pl.multiple_of(n * (16 * UNROLL) + 16 * u, 16), 16))
            return carry

        lax.fori_loop(0, TOKENS // (16 * UNROLL), group, 0)

    def shape(hid, which, out):
        shift, scale = modrows[which][0], 1.0 + modrows[which][1]

        def body(rows):
            c, inv, _ = centred(hid[rows])
            out[rows] = (c * inv * scale + shift).astype(jnp.bfloat16)

        by_rows(body)

    def project(src, weight):
        def body(j, carry):
            qkv[j] = dot(src[...], weight(j)).astype(jnp.bfloat16)
            return carry

        lax.fori_loop(0, 3, body, 0)

    lane = lax.broadcasted_iota(jnp.int32, (1, 128), 1)
    low_f = jnp.where(lane < 64, 1.0, 0.0)
    sides = [low_f.astype(jnp.bfloat16), (1.0 - low_f).astype(jnp.bfloat16)]
    is_low = lax.broadcasted_iota(jnp.int32, (TOKENS, 128), 1) < 64

    def swap_pair(which, hp):
        cols = pl.ds(128 * hp, 128)
        return swap(heads.at[which, :, cols], heads_in.at[which, :, cols], 3 + 4 * which + hp)

    def attend(which, keep):
        for hp in range(4):
            cols = pl.ds(128 * hp, 128)
            q, k, v = qkv[0, :, cols], qkv[1, :, cols], qkv[2, :, cols]
            outs = []
            for h in range(2):
                s = dot(q * sides[h], k, NT) * 0.125
                e = jnp.exp(s - jnp.max(s, axis=-1, keepdims=True))
                w = e / jnp.sum(e, axis=-1, keepdims=True)
                if keep:
                    weights[2 * hp + h] = w
                outs.append(dot(w.astype(jnp.bfloat16), v))
            heads[which, :, cols] = jnp.where(is_low, outs[0], outs[1]).astype(jnp.bfloat16)
            if hp > 0:
                swap_pair(which, hp - 1).start()
        swap_pair(which, 3).start()

    def swapped(which):
        for hp in range(4):
            swap_pair(which, hp).wait_recv()

    def mix(att, weight, which, base):
        mod_ref, at = places[which]

        for n in range(4):
            cols = pl.ds(n * 512, 512)
            p = dot(att[...], weight(n), NT)
            mixed[:, cols] = base[:, cols] + mod_ref[2, pl.ds(at, 1), cols] * p

    def predict(final, keep):
        def body(rows):
            c, inv, mean = centred(mixed[rows])
            u = c * inv
            if keep:
                inverses[0, rows] = jnp.broadcast_to(inv, (16, 128))
                inverses[1, rows] = jnp.broadcast_to(mean, (16, 128))
            high = u.astype(jnp.bfloat16)
            rest = u - high.astype(jnp.float32)
            middle = rest.astype(jnp.bfloat16)
            terms[0, rows] = high
            terms[1, rows] = middle
            terms[2, rows] = (rest - middle.astype(jnp.float32)).astype(jnp.bfloat16)

        by_rows(body)
        r = dot(terms[0], final[...], NT)
        m = dot(terms[1], final[0:256], NT)
        small = dot(terms[2], final[0:128], NT)
        return (
            r[:, 0:128]
            + (r[:, 128:256] + m[:, 0:128])
            + (r[:, 256:384] + m[:, 128:256] + small)
        )

    def other_rows(slab):
        return lambda n: held[slab, n].reshape(512, 512)

    def near_rows(n):
        return teacher_out[n].reshape(512, 512)

    def turn(src, out):
        def body(n, carry):
            t = src[:, columns(n, 128)].astype(jnp.float32).T.astype(jnp.bfloat16)
            out[pl.ds(2 * n, 2)] = t.reshape(2, 2, 32, TOKENS)
            return carry

        lax.fori_loop(0, D // 128, body, 0)

    def pair(k):
        if k < 2:
            src, dst = ((shaped_t, shaped_in), (proj_t, proj_in))[k]
            src = src.at[:, 1 - core]
        elif k == 2:
            src, dst = heads.at[2], packed_in.at[pl.ds(3 * TOKENS, TOKENS)]
        elif k == 3:
            rows = pl.ds(2 * TOKENS, TOKENS)
            src, dst = packed.at[rows], packed_in.at[rows]
        else:
            rows, cols = pl.ds(0, 2 * TOKENS), pl.ds(128 * (k - 4), 128)
            src, dst = packed.at[rows, cols], packed_in.at[rows, cols]
        return remote(src, dst, pair_send.at[k], pair_recv.at[k], "dp_3", 1 - core)

    half = D // 2
    for k in range(16):
        sin_a, cos_a = tables[0, k : k + 1], tables[1, k : k + 1]
        rows = pl.ds(16 * k, 16)
        placed[rows, :half] = sin_a * tables[3] + cos_a * tables[2]
        placed[rows, half:] = cos_a * tables[3] - sin_a * tables[2]
    stack(split_rows(teacher_embed), embed_t)
    latents = a_f * clean[...] + s_f * noise[...]
    for k in range(32):
        lat_rows[k : k + 1] = latents[:, 128 * k : 128 * k + 128]
    lat0 = eightfold(lat_rows[...])
    spread(lat0, embed_t, hidden, placed)
    shape(hidden, 0, shaped)
    swaps[0].wait_recv()
    swaps[1].wait_recv()
    t_step(0)
    s_step(1)
    load.wait()
    project(shaped, lambda j: near_qkv[j])
    t_step(1)
    attend(0, False)
    s_step(2)
    t_step(2)
    mix(heads.at[0], near_rows, 0, hidden)
    s_step(3)
    repeat(split_rows(teacher_final), final_b)
    t_step(3)
    t_step(4)
    swapped(0)
    mix(heads_in.at[0], other_rows(5), 0, mixed)
    eps0 = predict(final_b, False)
    lat1 = a_m * (lat0 - s_f * eps0) / a_f + s_m * eps0

    spread(lat1, embed_t, hidden, placed)
    shape(hidden, 1, shaped)
    project(shaped, lambda j: near_qkv[j])
    s_step(4)
    swaps[2].wait_recv()
    swaps[3].wait_recv()
    o_step(0)
    attend(1, False)
    mix(heads.at[1], near_rows, 1, hidden)
    stack(split_rows(student_embed), embed_s)
    spread(lat0, embed_s, hidden_s, placed)
    shape(hidden_s, 2, shaped_s)
    swapped(1)
    mix(heads_in.at[1], other_rows(5), 1, mixed)
    s_step(5)
    o_step(1)
    eps1 = predict(final_b, False)
    lat2 = a_l * (lat1 - s_m * eps1) / a_m + s_l * eps1
    target = (lat0 - a_f / a_l * lat2) / (s_f - a_f * s_l / a_l)

    student_terms = split_rows(student_final)
    repeat(student_terms, final_b)
    stack(student_terms, embed_t)
    s_step(6)
    project(shaped_s, lambda j: held[j].reshape(D, 512))
    o_step(2)
    attend(2, True)
    mix(heads.at[2], other_rows(3), 2, hidden_s)
    o_step(3)
    turn(shaped_s, shaped_t)
    swapped(2)
    o_step(4)
    mix(heads_in.at[2], other_rows(4), 2, mixed)
    pair(0).start()
    error = predict(final_b, True) - target
    lanes = lax.broadcasted_iota(jnp.int32, error.shape, 1)
    loss_part = (
        0.5 * row_weight * jnp.sum(jnp.where(lanes < 16, error * error, 0.0))
    )

    spread(2.0 * row_weight * error, embed_t, hidden)

    gate = modrows[2][2]

    def back(rows):
        inv, mean = inverses[0, rows, 0:1], inverses[1, rows, 0:1]
        up, u = hidden[rows], (mixed[rows] - mean) * inv
        first_mean = jnp.mean(up, axis=-1, keepdims=True)
        second_mean = jnp.mean(up * u, axis=-1, keepdims=True)
        d = (up - first_mean - u * second_mean) * inv
        shaped[rows] = (gate * d).astype(jnp.bfloat16)

    by_rows(back)
    turn(shaped, proj_t)
    pair(2).start()
    d_attn[...] = dot(shaped[...], held[3].reshape(D, 512)).astype(jnp.bfloat16)
    pair(1).start()

    extents = [(0, 2 * WIDE), (2 * WIDE, 2 * WIDE)]

    def products(s_ref, b_ref, first, count, add):
        def body(k, carry):
            lhs = s_ref[pl.ds(pl.multiple_of(k * 8, 8), 8)].reshape(256, TOKENS)
            spot = pl.ds(pl.multiple_of(k * 64, 64), 64)
            for j in range(count):
                g = dot(lhs, b_ref[TOKENS * j : TOKENS * (j + 1)])
                cols = pl.ds(WIDE * (first + j), WIDE)
                for i in range(4):
                    block = g[64 * i : 64 * i + 64, :WIDE]
                    wide[i, spot, cols] = wide[i, spot, cols] + block if add else block
                cols = pl.ds(HALF + WIDE * (first + j), WIDE)
                right = g[:, WIDE:]
                wide[k, :, cols] = wide[k, :, cols] + right if add else right
            return carry

        lax.fori_loop(0, 4, body, 0)

    rings = []
    for which, (offset, width) in enumerate(extents):
        for way in range(2):
            for stage in range(2):
                n = len(rings)
                if stage == 0:
                    part = wide.at[:, :, pl.ds(HALF * way + offset, width)]
                else:
                    part = (part_c, part_d)[way].at[:, :, pl.ds(offset, width)]
                axis = ("dp_1", "dp_0")[(way + stage) % 2]
                rings.append(ring_reduce(axis, part, *boxes[n], send.at[n], recv.at[n]))

    def ring_step(which, stage, step):
        offset, width = extents[which]
        for way in range(2):

            def into(half, cols, value, way=way):
                if stage == 0:
                    part = (part_c, part_d)[way].at[:, :, pl.ds(offset, width)]
                    part[2 * half, :, cols] = value[:64]
                    part[2 * half + 1, :, cols] = value[64:]
                else:
                    last.at[way, half, :, pl.ds(offset, width)][:, cols] = value

            do = rings[4 * which + 2 * way + stage][step]
            do(into) if step == 2 else do()

    def z_copies(which):
        codes, scales, codes_in, scales_in = boxes[8 + which]
        return [
            remote(a, b, z_send.at[2 * which + k], z_recv.at[2 * which + k], "dp_2", 1 - z)
            for k, (a, b) in enumerate([(codes, codes_in), (scales, scales_in)])
        ]

    def z_start(which):
        encode, _ = coder(*boxes[8 + which])
        offset, width = extents[which]
        for way in range(2):
            encode(way, lambda cols, way=way: last.at[way, 1 - z, :, pl.ds(offset, width)][:, cols])
        for c in z_copies(which):
            c.start()

    for hp in range(4):
        cols = pl.ds(128 * hp, 128)
        da = d_attn[:, cols]
        outs = [dot(weights[2 * hp + h].astype(jnp.bfloat16), da, TN) for h in range(2)]
        packed[2 * TOKENS :, cols] = jnp.where(is_low, outs[0], outs[1]).astype(jnp.bfloat16)
    products(proj_t.at[:, core], heads.at[2], 3, 1, False)
    pair(3).start()
    pair(1).wait_recv()
    pair(2).wait_recv()
    products(proj_in, packed_in.at[pl.ds(3 * TOKENS, TOKENS)], 3, 1, True)
    products(shaped_t.at[:, core], packed.at[pl.ds(2 * TOKENS, TOKENS)], 2, 1, False)
    pair(0).wait_recv()
    pair(3).wait_recv()
    products(shaped_in, packed_in.at[pl.ds(2 * TOKENS, TOKENS)], 2, 1, True)
    ring_step(1, 0, 0)
    for hp in range(4):
        cols = pl.ds(128 * hp, 128)
        q, k, v, da = qkv[0, :, cols], qkv[1, :, cols], qkv[2, :, cols], d_attn[:, cols]
        outs = []
        for h in range(2):
            w = weights[2 * hp + h]
            dp = dot(da * sides[h], v, NT)
            ds = w * (dp - jnp.sum(w * dp, axis=-1, keepdims=True)) * 0.125
            ds = ds.astype(jnp.bfloat16)
            outs.append((dot(ds, k), dot(ds, q, TN)))
        for j in range(2):
            joined = jnp.where(is_low, outs[0][j], outs[1][j]).astype(jnp.bfloat16)
            packed[TOKENS * j : TOKENS * (j + 1), cols] = joined
        if hp > 0:
            pair(3 + hp).start()
    pair(7).start()
    products(shaped_t.at[:, core], packed, 0, 2, False)
    ring_step(1, 0, 1)
    for k in (4, 5, 6, 7):
        pair(k).wait_recv()
    products(shaped_in, packed_in, 0, 2, True)
    ring_step(0, 0, 0)
    ring_step(1, 0, 2)
    ring_step(1, 1, 0)
    ring_step(0, 0, 1)
    ring_step(1, 1, 1)
    ring_step(0, 0, 2)
    ring_step(0, 1, 0)
    ring_step(1, 1, 2)
    z_start(1)
    ring_step(0, 1, 1)
    ring_step(0, 1, 2)
    z_start(0)
    for which, (offset, width) in enumerate(extents):
        _, decoded = coder(*boxes[8 + which])
        for c in z_copies(which):
            c.wait_recv()
        for way in range(2):
            for j in range(offset // WIDE, (offset + width) // WIDE):
                cols, near = pl.ds(WIDE * j, WIDE), pl.ds(WIDE * j - offset, WIDE)
                out[j, :, pl.ds(WIDE * way, WIDE)] = last[way, z, :, cols] + decoded(way, near)
    leave = pltpu.make_async_copy(out, out_far, grads_sem)
    leave.start()
    squares = jnp.sum(out[...] * out[...])
    row = lax.broadcasted_iota(jnp.int32, (8, 128), 0)
    value = jnp.where(row == 0, squares, loss_part)
    totals[...] = sum_over_all(value, inbox, sum_send, sum_recv)
    leave.wait()
    for c in [*z_copies(0), *z_copies(1)]:
        c.wait_send()
    for c in swaps:
        c.wait_send()
    for k in range(8):
        pair(k).wait_send()
    for which in range(3):
        for hp in range(4):
            swap_pair(which, hp).wait_send()


def levels():
    lamb = 6.0 - 12.0 * np.arange(TGRID + 1) / TGRID
    return [np.sqrt(1.0 / (1.0 + np.exp(sign * lamb))).astype(np.float32) for sign in (-1.0, 1.0)]


ALPHAS, SIGMAS = levels()


def position_tables():
    half = D // 2
    freqs = np.exp(-math.log(10000.0) * np.arange(half) / half)
    fine = np.arange(16)[:, None] * freqs[None]
    angles = (np.sin(16.0 * fine), np.cos(16.0 * fine), np.sin(fine), np.cos(fine))
    return np.stack(angles).astype(np.float32)


def whole_step(timestep, bucket, bucket_weights, clean, noise, teacher, student):
    vmem, smem = (pl.BlockSpec(memory_space=m) for m in (pltpu.VMEM, pltpu.SMEM))
    bf16, f32 = jnp.bfloat16, jnp.float32

    def boxes(width):
        return [
            scratch
            for half in (128, 32, 128, 32)
            for scratch in [pltpu.VMEM((6, half, width), jnp.int16), pltpu.VMEM((6, 1, width), f32)] * 2
        ]

    def last_boxes(width):
        return [pltpu.VMEM((2, 32, width), jnp.int16), pltpu.VMEM((2, 1, width), f32)] * 2

    def semaphores(*shape):
        return [pltpu.SemaphoreType.DMA(shape)] * 2

    return pl.pallas_call(
        step_kernel,
        out_shape=(
            jax.ShapeDtypeStruct((4, 32, 512), f32),
            jax.ShapeDtypeStruct((8, 128), f32),
        ),
        in_specs=[smem] * 3 + [vmem] * 9 + [pl.BlockSpec(memory_space=pl.ANY)] * 2 + [vmem] * 2,
        out_specs=(pl.BlockSpec(memory_space=pl.ANY), vmem),
        scratch_shapes=[
            pltpu.VMEM((4, 32, 512), f32),
            pltpu.VMEM((6, 4, 4, 2, 2, 2, 16, 512), bf16),
            pltpu.VMEM((3, D, 512), bf16),
            pltpu.VMEM((4, 4, 2, 2, 2, 16, 512), bf16),
            pltpu.VMEM((4, TOKENS, D), f32),
            pltpu.VMEM((TOKENS, D), bf16),
            pltpu.VMEM((TOKENS, D), bf16),
            pltpu.VMEM((3, TOKENS, 512), bf16),
            pltpu.VMEM((3, TOKENS, 512), bf16),
            pltpu.VMEM((3, TOKENS, 512), bf16),
            pltpu.VMEM((8, TOKENS, TOKENS), f32),
            pltpu.VMEM((3, TOKENS, D), bf16),
            pltpu.VMEM((2, TOKENS, 128), f32),
            pltpu.VMEM((TOKENS, 512), bf16),
            pltpu.VMEM((128, D), bf16),
            pltpu.VMEM((128, D), bf16),
            pltpu.VMEM((384, D), bf16),
            pltpu.VMEM((32, 128), f32),
            pltpu.VMEM((32, 2, 32, TOKENS), bf16),
            pltpu.VMEM((32, 2, 32, TOKENS), bf16),
            pltpu.VMEM((32, 32, TOKENS), bf16),
            pltpu.VMEM((32, 32, TOKENS), bf16),
            pltpu.VMEM((4 * TOKENS, 512), bf16),
            pltpu.VMEM((4, 64, HALF), f32),
            pltpu.VMEM((4, 64, HALF), f32),
            pltpu.SemaphoreType.DMA,
            pltpu.SemaphoreType.DMA,
            pltpu.SemaphoreType.DMA,
            *semaphores(17),
            *semaphores(25),
            *semaphores(25),
            *semaphores(25),
            *boxes(2 * WIDE),
            *boxes(2 * WIDE),
            *last_boxes(2 * WIDE),
            *last_boxes(2 * WIDE),
            pltpu.VMEM((2, 2, 32, HALF), f32),
            *semaphores(8),
            *semaphores(8, 6, 2),
            *semaphores(4),
            pltpu.VMEM((2, 16, 8, 128), f32),
            *semaphores(2, 15),
        ],
        compiler_params=pltpu.CompilerParams(
            collective_id=2, has_side_effects=True, vmem_limit_bytes=63 * 2**20
        ),
    )(
        timestep,
        bucket,
        bucket_weights,
        clean,
        noise,
        jnp.asarray(position_tables()),
        teacher[0],
        teacher[1],
        jnp.moveaxis(teacher[2], 1, 0),
        student[0],
        student[1],
        jnp.moveaxis(student[2], 1, 0),
        jnp.moveaxis(teacher[3], 1, 0),
        teacher[4].reshape(4, 4, 2, 2, 2, 16, 512),
        jnp.moveaxis(student[3], 1, 0).reshape(3, 2, 16, 512),
        student[4].reshape(2, 16, 512),
    )


def adam_kernel(grads, totals, mq, vq, mo, vo, new_mq, new_vq, up_q, new_mo, new_vo, up_o, loss):
    rms = jnp.sqrt(totals[0:1, 0:1] / (4 * D * INNER))
    factor = 1.0 / jnp.maximum(rms, 1.0)

    def adam(grad, moment, second, new_moment, new_second, update):
        normed = grad * factor
        m = BETA_ONE * moment + (1.0 - BETA_ONE) * normed
        v = BETA_TWO * second + (1.0 - BETA_TWO) * normed * normed
        new_moment[...] = m
        new_second[...] = v
        update[...] = m / (jnp.sqrt(v) + ADAM_EPS)

    for j in range(3):
        adam(grads[j], mq[j], vq[j], new_mq.at[j], new_vq.at[j], up_q.at[j])
    adam(grads[3], mo[...], vo[...], new_mo, new_vo, up_o)
    loss[...] = totals[1:2, 0:1] / (SAMPLES * LATENT)


def adam_update(grads, totals, moment_qkv, second_qkv, moment_out, second_out):
    vmem = pl.BlockSpec(memory_space=pltpu.VMEM)
    mq, vq = (jnp.moveaxis(v, 1, 0) for v in (moment_qkv, second_qkv))
    qkv, out = (jax.ShapeDtypeStruct(v.shape, v.dtype) for v in (mq, moment_out))
    *news, loss = pl.pallas_call(
        adam_kernel,
        out_shape=(qkv, qkv, qkv, out, out, out, jax.ShapeDtypeStruct((1, 1), jnp.float32)),
        in_specs=[vmem] * 6,
        out_specs=(vmem,) * 7,
    )(grads, totals, mq, vq, moment_out, second_out)
    return (*(jnp.moveaxis(v, 0, 1) for v in news[:3]), *news[3:], loss.reshape(()))


def per_device(
    clean_latent,
    noise_draw,
    timestep,
    bucket,
    bucket_weights,
    teacher_embed,
    teacher_final,
    teacher_mod,
    teacher_qkv,
    teacher_out,
    student_embed,
    student_final,
    student_mod,
    student_qkv,
    student_out,
    moment_qkv,
    second_qkv,
    moment_out,
    second_out,
):
    grads, totals = whole_step(
        timestep,
        bucket,
        bucket_weights,
        clean_latent,
        noise_draw,
        (teacher_embed, teacher_final, teacher_mod, teacher_qkv, teacher_out),
        (student_embed, student_final, student_mod, student_qkv, student_out),
    )
    return adam_update(grads, totals, moment_qkv, second_qkv, moment_out, second_out)


def solution(mesh):
    torus = Mesh(
        mesh.devices.reshape(4, 4, 2, 2, mesh.shape["mp"]), ("dp_0", "dp_1", "dp_2", "dp_3", "mp")
    )
    in_specs = (
        P(DP, None),
        P(DP, None),
        P(DP),
        P(DP),
        P(),
        P(),
        P(),
        P(),
        P(None, None, "mp"),
        P(None, "mp"),
        P(),
        P(),
        P(),
        P(DP, None, "mp"),
        P(DP, "mp"),
        P(DP, None, "mp"),
        P(DP, None, "mp"),
        P(DP, "mp"),
        P(DP, "mp"),
    )
    out_specs = (
        P(DP, None, "mp"),
        P(DP, None, "mp"),
        P(DP, None, "mp"),
        P(DP, "mp"),
        P(DP, "mp"),
        P(DP, "mp"),
        P(),
    )
    return jax.shard_map(
        per_device, mesh=torus, in_specs=in_specs, out_specs=out_specs, check_vma=False
    )
```

```python
import math

import jax
import jax.numpy as jnp
import numpy as np
from jax import lax
from jax.experimental import pallas as pl
from jax.experimental.pallas import tpu as pltpu
from jax.sharding import Mesh
from jax.sharding import PartitionSpec as P

D = 2048
HS = 64
INNER = 1024
PATCH_CH = 16
SEQ = 256
LATENT = 4096
SAMPLES = 64
K = 8
TGRID = 16
NBUCKET = 8
DP = ("dp_0", "dp_1", "dp_2", "dp_3")
DP_MP = ("dp_0", "dp_1", "dp_2", "dp_3", "mp")


LN_EPS = 0.01
BETA_ONE = 0.9
BETA_TWO = 0.99
ADAM_EPS = 1e-08


ROWS = 1024
HALF = 1024
CODES = 32767.0
AXES = ("dp_0", "dp_1", "dp_2", "dp_3", "mp")


def remote(src, dst, send, recv, axis, target):
    return pltpu.make_async_remote_copy(
        src_ref=src,
        dst_ref=dst,
        send_sem=send,
        recv_sem=recv,
        device_id={axis: target} if isinstance(axis, str) else dict(zip(axis, target)),
        device_id_type=pl.DeviceIdType.MESH,
    )


def greet(friends):
    barrier = pltpu.get_barrier_semaphore()
    for axis, target in friends:
        pl.semaphore_signal(
            barrier,
            inc=1,
            device_id={axis: target} if isinstance(axis, str) else dict(zip(axis, target)),
            device_id_type=pl.DeviceIdType.MESH,
        )
    pl.semaphore_wait(barrier, len(friends))


def all_places():
    y, x, z, core, mp = (lax.axis_index(a) for a in AXES)
    axes, here = ("mp", "dp_2", "dp_3"), (mp, z, core)
    cube = []
    for k in range(1, 8):
        cube.append((axes, tuple(1 - h if k >> n & 1 else h for n, h in enumerate(here))))
    plane = []
    for k in range(1, 16):
        plane.append((("dp_0", "dp_1"), (lax.rem(y + k // 4, 4), lax.rem(x + k % 4, 4))))
    return [(4 * mp + 2 * z + core, cube), (4 * y + x, plane)]


def sum_over_all(value, inbox, send, recv):
    for stage, (slot, partners) in enumerate(all_places()):
        inbox[stage, slot] = value
        copies = [
            remote(
                inbox.at[stage, slot],
                inbox.at[stage, slot],
                send.at[stage, k],
                recv.at[stage, k],
                axis,
                target,
            )
            for k, (axis, target) in enumerate(partners)
        ]
        for c in copies:
            c.start()
        for c in copies:
            c.wait_recv()
        value = inbox[stage, 0]
        for k in range(1, len(partners) + 1):
            value = value + inbox[stage, k]
        for c in copies:
            c.wait_send()
    return value


def by_columns(body, width):
    def step(n, carry):
        body(pl.ds(pl.multiple_of(n * 256, 256), 256))
        return carry

    lax.fori_loop(0, width // 256, step, 0)


def coder(codes, scales, boxes, box_scales):
    def encode(k, value):
        def body(cols):
            v = value(cols)
            peak = jnp.maximum(jnp.max(jnp.abs(v), axis=0, keepdims=True), 1e-30)
            code = lax.round(v * (CODES / peak), lax.RoundingMethod.TO_NEAREST_EVEN)
            codes[k, :, cols] = code.astype(jnp.int32).astype(jnp.int16)
            scales[k, :, cols] = peak * (1.0 / CODES)

        by_columns(body, codes.shape[2])

    def decoded(k, cols):
        return boxes[k, :, cols].astype(jnp.int32).astype(jnp.float32) * box_scales[k, :, cols]

    return encode, decoded


def ring_reduce(axis, part, codes, scales, boxes, box_scales, send, recv):
    me = lax.axis_index(axis)
    right, left, far = (lax.rem(me + k, 4) for k in (1, 3, 2))
    half, width = part.shape[1] // 2, part.shape[2]
    top, low = pl.ds(0, half), pl.ds(half, half)

    encode, decoded = coder(codes, scales, boxes, box_scales)

    def message(k):
        target = left if k % 2 else right
        return [
            remote(codes.at[k], boxes.at[k], send.at[k, 0], recv.at[k, 0], axis, target),
            remote(scales.at[k], box_scales.at[k], send.at[k, 1], recv.at[k, 1], axis, target),
        ]

    def post(k, value):
        encode(k, value)
        for c in message(k):
            c.start()

    def arrived(*which):
        for k in which:
            for c in message(k):
                c.wait_recv()

    def start():
        post(0, lambda cols: part[far, top, cols])
        post(1, lambda cols: part[far, low, cols])
        post(2, lambda cols: part[right, low, cols])
        post(3, lambda cols: part[left, top, cols])

    def relay():
        arrived(0)
        post(4, lambda cols: part[right, top, cols] + decoded(0, cols))
        arrived(1)
        post(5, lambda cols: part[left, low, cols] + decoded(1, cols))

    def finish(store):
        arrived(3, 4)
        by_columns(
            lambda cols: store(0, cols, part[me, top, cols] + decoded(3, cols) + decoded(4, cols)),
            width,
        )
        arrived(2, 5)
        by_columns(
            lambda cols: store(1, cols, part[me, low, cols] + decoded(2, cols) + decoded(5, cols)),
            width,
        )
        for k in range(6):
            for c in message(k):
                c.wait_send()

    return start, relay, finish


TOKENS = 256
UNROLL = 4
WIDE = 256
NT = (((1,), (1,)), ((), ()))
TN = (((0,), (0,)), ((), ()))


def dot(a, b, dims=(((1,), (0,)), ((), ()))):
    return lax.dot_general(a, b, dims, preferred_element_type=jnp.float32)


def gather_stream(held, slabs, send, recv, short=False):
    y, x, z, core = (lax.axis_index(a) for a in AXES[:4])
    near = {"dp_0": [lax.rem(y + k, 4) for k in (1, 3)], "dp_1": [lax.rem(x + k, 4) for k in (1, 3)]}
    every = slice(None)
    live = []

    def go(spot, k, axis, target):
        ref = held.at[(slabs, *spot)]
        c = remote(ref, ref, send.at[k], recv.at[k], axis, target)
        c.start()
        live.append(c)
        return c

    def ring_direct(first):
        for half, axis in enumerate(("dp_1", "dp_0") if first else ("dp_0", "dp_1")):
            if first:
                spot = (y, x, every, core, half)
            elif half == 0:
                spot = (y, every, every, core, half)
            else:
                spot = (every, x, every, core, half)
            for side in range(2):
                k = (1 if first else 9) + 4 * half + side
                go(spot, k, axis, near[axis][side])

    def ring_relay(first):
        base = 1 if first else 9
        direct = live[-4:]
        for half, axis in enumerate(("dp_1", "dp_0") if first else ("dp_0", "dp_1")):
            for side in range(2):
                direct[2 * half + side].wait_recv()
                back = near[axis][1 - side]
                if first:
                    spot = (y, back) if axis == "dp_1" else (back, x)
                else:
                    spot = (every, back) if axis == "dp_1" else (back, every)
                go((*spot, side, core, half), base + 4 * half + 2 + side, axis, near[axis][side])

    def across(k, spot):
        go((*spot[:3], core, spot[3]), k, "dp_3", 1 - core)

    def ring_straight():
        for half, (axis, me) in enumerate([("dp_1", x), ("dp_0", y)]):
            for k in (1, 2, 3):
                go((y, x, every, core, half), 3 * half + k - 1, axis, lax.rem(me + k, 4))

    def step(k):
        if short:
            k = k + 2
        if k == 0:
            go((y, x, z, core), 0, "dp_2", 1 - z)
        elif k == 1:
            live[-1].wait_recv()
            ring_direct(True)
        elif k == 2:
            ring_straight() if short else ring_relay(True)
        elif k == 3:
            for c in live[-6:] if short else live[-4:]:
                c.wait_recv()
            ring_direct(False)
        elif k == 4:
            ring_relay(False)
            relays.extend(live[-4:])
            across(17, (y, every, every, 0))
            across(18, (every, x, every, 1))
            for n in range(2):
                across(19 + 2 * n, (near["dp_0"][n], every, every, 0))
                across(20 + 2 * n, (every, near["dp_1"][n], every, 1))
        elif k == 5:
            for c in relays:
                c.wait_recv()
            across(23, (lax.rem(y + 2, 4), every, every, 0))
            across(24, (every, lax.rem(x + 2, 4), every, 1))
        else:
            for c in live[-8:]:
                c.wait_recv()
            for c in live:
                c.wait_send()

    relays = []
    return step


def three_terms(v8):
    high = v8.astype(jnp.bfloat16).astype(jnp.float32)
    rest = v8 - high
    middle = rest.astype(jnp.bfloat16).astype(jnp.float32)
    low = rest - middle
    group = lax.broadcasted_iota(jnp.int32, v8.shape, 1) // 16
    picked = jnp.where(
        (group == 0) | (group == 1) | (group == 3),
        high,
        jnp.where((group == 2) | (group == 5), middle, jnp.where(group == 4, low, 0.0)),
    )
    return picked.astype(jnp.bfloat16)


def eightfold(rows):
    v = jnp.broadcast_to(rows[:, None], (32, 8, 128)).reshape(TOKENS, 128)
    token = lax.broadcasted_iota(jnp.int32, v.shape, 0) % 8
    lane = lax.broadcasted_iota(jnp.int32, v.shape, 1)
    v = jnp.where(lane // 16 == token, v, 0.0)
    across = lax.broadcasted_iota(jnp.int32, (128, 128), 1) % 16
    down = lax.broadcasted_iota(jnp.int32, (128, 128), 0) % 16
    spread = jnp.where(across == down, 1.0, 0.0).astype(jnp.bfloat16)
    high = v.astype(jnp.bfloat16)
    rest = v - high.astype(jnp.float32)
    middle = rest.astype(jnp.bfloat16)
    low = (rest - middle.astype(jnp.float32)).astype(jnp.bfloat16)
    return dot(high, spread) + dot(middle, spread) + dot(low, spread)


def picked_level(step, offset, values):
    out = jnp.float32(0.0)
    for k in range(1, K + 1):
        out = jnp.where(step == k, jnp.float32(values[2 * k + offset]), out)
    return out


def step_kernel(
    timestep,
    bucket,
    bucket_weights,
    clean,
    noise,
    tables,
    teacher_embed,
    teacher_final,
    teacher_mod,
    student_embed,
    student_final,
    student_mod,
    teacher_qkv,
    teacher_out_far,
    student_qkv,
    student_out,
    out_far,
    totals,
    out,
    held,
    near_qkv,
    teacher_out,
    wide,
    shaped,
    shaped_s,
    qkv,
    heads,
    heads_in,
    weights,
    terms,
    inverses,
    d_attn,
    embed_t,
    embed_s,
    final_b,
    lat_rows,
    shaped_t,
    proj_t,
    shaped_in,
    proj_in,
    packed_in,
    part_c,
    part_d,
    qkv_sem,
    out_sem,
    grads_sem,
    swap_send,
    swap_recv,
    t_send,
    t_recv,
    s_send,
    s_recv,
    o_send,
    o_recv,
    *rest,
):
    boxes = [rest[4 * k : 4 * k + 4] for k in range(10)]
    last, pair_send, pair_recv, send, recv, z_send, z_recv = rest[40:47]
    inbox, sum_send, sum_recv = rest[47:]
    hidden, hidden_s, mixed, placed = (wide.at[k] for k in range(4))
    packed = near_qkv.at[0, pl.ds(0, 3 * TOKENS)]
    y, x, z, core, mp = (lax.axis_index(a) for a in AXES)
    load_out = pltpu.make_async_copy(teacher_out_far, teacher_out, out_sem)
    load_out.start()
    load = pltpu.make_async_copy(teacher_qkv, near_qkv, qkv_sem)
    load.start()
    held[0:3, y, x, z, core] = student_qkv[...]
    held[3, y, x, z, core] = student_out[...]
    both = ("dp_2", "mp")
    greet([friend for _, partners in all_places() for friend in partners])

    def swap(src, dst, k, axis="mp", target=None):
        target = 1 - mp if target is None else target
        return remote(src, dst, swap_send.at[k], swap_recv.at[k], axis, target)

    load_out.wait()
    spot = (y, x, z, core)
    here = teacher_out.at[spot]
    swaps = [
        swap(here, held.at[(5, *spot)], 0),
        swap(here, held.at[(5, *spot)], 1, both, (1 - z, 1 - mp)),
        swap(student_out, held.at[(4, *spot)], 15),
        swap(student_out, held.at[(4, *spot)], 16, both, (1 - z, 1 - mp)),
    ]
    for c in swaps:
        c.start()
    t_step = gather_stream(held, pl.ds(5, 1), t_send, t_recv, short=True)
    s_step = gather_stream(held, pl.ds(0, 4), s_send, s_recv)
    o_step = gather_stream(held, pl.ds(4, 1), o_send, o_recv, short=True)
    s_step(0)

    step = timestep[0]
    a_f, a_m, a_l = (picked_level(step, -k, ALPHAS) for k in range(3))
    s_f, s_m, s_l = (picked_level(step, -k, SIGMAS) for k in range(3))
    row_weight = bucket_weights[jnp.clip(bucket[0], 0, NBUCKET - 1)]
    places = [
        (teacher_mod, jnp.clip(2 * step - 1, 0, TGRID - 1)),
        (teacher_mod, jnp.clip(2 * step - 2, 0, TGRID - 1)),
        (student_mod, jnp.clip(step - 1, 0, K - 1)),
    ]
    modrows = [[mod[j, pl.ds(at, 1), :] for j in range(3)] for mod, at in places]

    def split_rows(ref):
        v = ref[...]
        h = v.astype(jnp.bfloat16)
        rest = v - h.astype(jnp.float32)
        m = rest.astype(jnp.bfloat16)
        return h, m, (rest - m.astype(jnp.float32)).astype(jnp.bfloat16)

    def stack(parts, out):
        h, m, l = parts
        for k, v in enumerate([h, m, h, l, h, m, jnp.zeros_like(h), jnp.zeros_like(h)]):
            out[16 * k : 16 * k + 16] = v

    def repeat(parts, out):
        for k in range(24):
            out[16 * k : 16 * k + 16] = parts[k // 8]

    def columns(k, width):
        return pl.ds(pl.multiple_of(k * width, width), width)

    def spread(v8, b_ref, out, base=None):
        terms8 = three_terms(v8)

        for n in range(D // WIDE):
            cols = pl.ds(n * WIDE, WIDE)
            h = dot(terms8, b_ref[:, cols])
            out[:, cols] = h if base is None else h + base[:, cols]

    def centred(v):
        mean = jnp.mean(v, axis=-1, keepdims=True)
        c = v - mean
        return c, lax.rsqrt(jnp.mean(c * c, axis=-1, keepdims=True) + LN_EPS), mean

    def by_rows(body):
        def group(n, carry):
            for u in range(UNROLL):
                body(pl.ds(pl.multiple_of(n * (16 * UNROLL) + 16 * u, 16), 16))
            return carry

        lax.fori_loop(0, TOKENS // (16 * UNROLL), group, 0)

    def shape(hid, which, out):
        shift, scale = modrows[which][0], 1.0 + modrows[which][1]

        def body(rows):
            c, inv, _ = centred(hid[rows])
            out[rows] = (c * inv * scale + shift).astype(jnp.bfloat16)

        by_rows(body)

    def project(src, weight):
        def body(j, carry):
            qkv[j] = dot(src[...], weight(j)).astype(jnp.bfloat16)
            return carry

        lax.fori_loop(0, 3, body, 0)

    lane = lax.broadcasted_iota(jnp.int32, (1, 128), 1)
    low_f = jnp.where(lane < 64, 1.0, 0.0)
    sides = [low_f.astype(jnp.bfloat16), (1.0 - low_f).astype(jnp.bfloat16)]
    is_low = lax.broadcasted_iota(jnp.int32, (TOKENS, 128), 1) < 64

    def swap_pair(which, hp):
        cols = pl.ds(128 * hp, 128)
        return swap(heads.at[which, :, cols], heads_in.at[which, :, cols], 3 + 4 * which + hp)

    def attend(which, keep):
        for hp in range(4):
            cols = pl.ds(128 * hp, 128)
            q, k, v = qkv[0, :, cols], qkv[1, :, cols], qkv[2, :, cols]
            outs = []
            for h in range(2):
                s = dot(q * sides[h], k, NT) * 0.125
                e = jnp.exp(s - jnp.max(s, axis=-1, keepdims=True))
                w = e / jnp.sum(e, axis=-1, keepdims=True)
                if keep:
                    weights[2 * hp + h] = w
                outs.append(dot(w.astype(jnp.bfloat16), v))
            heads[which, :, cols] = jnp.where(is_low, outs[0], outs[1]).astype(jnp.bfloat16)
            if hp > 0:
                swap_pair(which, hp - 1).start()
        swap_pair(which, 3).start()

    def swapped(which):
        for hp in range(4):
            swap_pair(which, hp).wait_recv()

    def mix(att, weight, which, base):
        mod_ref, at = places[which]

        for n in range(4):
            cols = pl.ds(n * 512, 512)
            p = dot(att[...], weight(n), NT)
            mixed[:, cols] = base[:, cols] + mod_ref[2, pl.ds(at, 1), cols] * p

    def predict(final, keep):
        def body(rows):
            c, inv, mean = centred(mixed[rows])
            u = c * inv
            if keep:
                inverses[0, rows] = jnp.broadcast_to(inv, (16, 128))
                inverses[1, rows] = jnp.broadcast_to(mean, (16, 128))
            high = u.astype(jnp.bfloat16)
            rest = u - high.astype(jnp.float32)
            middle = rest.astype(jnp.bfloat16)
            terms[0, rows] = high
            terms[1, rows] = middle
            terms[2, rows] = (rest - middle.astype(jnp.float32)).astype(jnp.bfloat16)

        by_rows(body)
        r = dot(terms[0], final[...], NT)
        m = dot(terms[1], final[0:256], NT)
        small = dot(terms[2], final[0:128], NT)
        return (
            r[:, 0:128]
            + (r[:, 128:256] + m[:, 0:128])
            + (r[:, 256:384] + m[:, 128:256] + small)
        )

    def other_rows(slab):
        return lambda n: held[slab, n].reshape(512, 512)

    def near_rows(n):
        return teacher_out[n].reshape(512, 512)

    def turn(src, out):
        def body(n, carry):
            for u in range(4):
                m = 4 * n + u
                t = src[:, columns(m, 128)].astype(jnp.float32).T.astype(jnp.bfloat16)
                out[pl.ds(2 * m, 2)] = t.reshape(2, 2, 32, TOKENS)
            return carry

        lax.fori_loop(0, D // 512, body, 0)

    def pair(k):
        if k < 2:
            src, dst = ((shaped_t, shaped_in), (proj_t, proj_in))[k]
            src = src.at[:, 1 - core]
        elif k == 2:
            src, dst = heads.at[2], packed_in.at[pl.ds(3 * TOKENS, TOKENS)]
        elif k == 3:
            rows = pl.ds(2 * TOKENS, TOKENS)
            src, dst = packed.at[rows], packed_in.at[rows]
        else:
            rows, cols = pl.ds(0, 2 * TOKENS), pl.ds(128 * (k - 4), 128)
            src, dst = packed.at[rows, cols], packed_in.at[rows, cols]
        return remote(src, dst, pair_send.at[k], pair_recv.at[k], "dp_3", 1 - core)

    half = D // 2
    for k in range(16):
        sin_a, cos_a = tables[0, k : k + 1], tables[1, k : k + 1]
        rows = pl.ds(16 * k, 16)
        placed[rows, :half] = sin_a * tables[3] + cos_a * tables[2]
        placed[rows, half:] = cos_a * tables[3] - sin_a * tables[2]
    stack(split_rows(teacher_embed), embed_t)
    latents = a_f * clean[...] + s_f * noise[...]
    for k in range(32):
        lat_rows[k : k + 1] = latents[:, 128 * k : 128 * k + 128]
    lat0 = eightfold(lat_rows[...])
    spread(lat0, embed_t, hidden, placed)
    shape(hidden, 0, shaped)
    swaps[0].wait_recv()
    swaps[1].wait_recv()
    t_step(0)
    s_step(1)
    load.wait()
    project(shaped, lambda j: near_qkv[j])
    t_step(1)
    attend(0, False)
    s_step(2)
    t_step(2)
    mix(heads.at[0], near_rows, 0, hidden)
    s_step(3)
    repeat(split_rows(teacher_final), final_b)
    t_step(3)
    t_step(4)
    swapped(0)
    mix(heads_in.at[0], other_rows(5), 0, mixed)
    eps0 = predict(final_b, False)
    lat1 = a_m * (lat0 - s_f * eps0) / a_f + s_m * eps0

    spread(lat1, embed_t, hidden, placed)
    shape(hidden, 1, shaped)
    project(shaped, lambda j: near_qkv[j])
    s_step(4)
    swaps[2].wait_recv()
    swaps[3].wait_recv()
    o_step(0)
    attend(1, False)
    mix(heads.at[1], near_rows, 1, hidden)
    stack(split_rows(student_embed), embed_s)
    spread(lat0, embed_s, hidden_s, placed)
    shape(hidden_s, 2, shaped_s)
    swapped(1)
    mix(heads_in.at[1], other_rows(5), 1, mixed)
    s_step(5)
    o_step(1)
    eps1 = predict(final_b, False)
    lat2 = a_l * (lat1 - s_m * eps1) / a_m + s_l * eps1
    target = (lat0 - a_f / a_l * lat2) / (s_f - a_f * s_l / a_l)

    student_terms = split_rows(student_final)
    repeat(student_terms, final_b)
    stack(student_terms, embed_t)
    s_step(6)
    project(shaped_s, lambda j: held[j].reshape(D, 512))
    o_step(2)
    attend(2, True)
    mix(heads.at[2], other_rows(3), 2, hidden_s)
    o_step(3)
    turn(shaped_s, shaped_t)
    swapped(2)
    o_step(4)
    mix(heads_in.at[2], other_rows(4), 2, mixed)
    pair(0).start()
    error = predict(final_b, True) - target
    lanes = lax.broadcasted_iota(jnp.int32, error.shape, 1)
    loss_part = (
        0.5 * row_weight * jnp.sum(jnp.where(lanes < 16, error * error, 0.0))
    )

    spread(2.0 * row_weight * error, embed_t, hidden)

    gate = modrows[2][2]

    def back(rows):
        inv, mean = inverses[0, rows, 0:1], inverses[1, rows, 0:1]
        up, u = hidden[rows], (mixed[rows] - mean) * inv
        first_mean = jnp.mean(up, axis=-1, keepdims=True)
        second_mean = jnp.mean(up * u, axis=-1, keepdims=True)
        d = (up - first_mean - u * second_mean) * inv
        shaped[rows] = (gate * d).astype(jnp.bfloat16)

    by_rows(back)
    turn(shaped, proj_t)
    pair(2).start()
    d_attn[...] = dot(shaped[...], held[3].reshape(D, 512)).astype(jnp.bfloat16)
    pair(1).start()

    extents = [(0, 2 * WIDE), (2 * WIDE, 2 * WIDE)]

    def products(s_ref, b_ref, first, count, add):
        for k in range(4):
            lhs = s_ref[pl.ds(8 * k, 8)].reshape(256, TOKENS)
            spot = pl.ds(64 * k, 64)
            for j in range(count):
                g = dot(lhs, b_ref[TOKENS * j : TOKENS * (j + 1)])
                cols = pl.ds(WIDE * (first + j), WIDE)
                for i in range(4):
                    block = g[64 * i : 64 * i + 64, :WIDE]
                    wide[i, spot, cols] = wide[i, spot, cols] + block if add else block
                cols = pl.ds(HALF + WIDE * (first + j), WIDE)
                right = g[:, WIDE:]
                wide[k, :, cols] = wide[k, :, cols] + right if add else right

    rings = []
    for which, (offset, width) in enumerate(extents):
        for way in range(2):
            for stage in range(2):
                n = len(rings)
                if stage == 0:
                    part = wide.at[:, :, pl.ds(HALF * way + offset, width)]
                else:
                    part = (part_c, part_d)[way].at[:, :, pl.ds(offset, width)]
                axis = ("dp_1", "dp_0")[(way + stage) % 2]
                rings.append(ring_reduce(axis, part, *boxes[n], send.at[n], recv.at[n]))

    def ring_step(which, stage, step):
        offset, width = extents[which]
        for way in range(2):

            def into(half, cols, value, way=way):
                if stage == 0:
                    part = (part_c, part_d)[way].at[:, :, pl.ds(offset, width)]
                    part[2 * half, :, cols] = value[:64]
                    part[2 * half + 1, :, cols] = value[64:]
                else:
                    last.at[way, half, :, pl.ds(offset, width)][:, cols] = value

            do = rings[4 * which + 2 * way + stage][step]
            do(into) if step == 2 else do()

    def z_copies(which):
        codes, scales, codes_in, scales_in = boxes[8 + which]
        return [
            remote(a, b, z_send.at[2 * which + k], z_recv.at[2 * which + k], "dp_2", 1 - z)
            for k, (a, b) in enumerate([(codes, codes_in), (scales, scales_in)])
        ]

    def z_start(which):
        encode, _ = coder(*boxes[8 + which])
        offset, width = extents[which]
        for way in range(2):
            encode(way, lambda cols, way=way: last.at[way, 1 - z, :, pl.ds(offset, width)][:, cols])
        for c in z_copies(which):
            c.start()

    for hp in range(4):
        cols = pl.ds(128 * hp, 128)
        da = d_attn[:, cols]
        outs = [dot(weights[2 * hp + h].astype(jnp.bfloat16), da, TN) for h in range(2)]
        packed[2 * TOKENS :, cols] = jnp.where(is_low, outs[0], outs[1]).astype(jnp.bfloat16)
    products(proj_t.at[:, core], heads.at[2], 3, 1, False)
    pair(3).start()
    pair(1).wait_recv()
    pair(2).wait_recv()
    products(proj_in, packed_in.at[pl.ds(3 * TOKENS, TOKENS)], 3, 1, True)
    products(shaped_t.at[:, core], packed.at[pl.ds(2 * TOKENS, TOKENS)], 2, 1, False)
    pair(0).wait_recv()
    pair(3).wait_recv()
    products(shaped_in, packed_in.at[pl.ds(2 * TOKENS, TOKENS)], 2, 1, True)
    ring_step(1, 0, 0)
    for hp in range(4):
        cols = pl.ds(128 * hp, 128)
        q, k, v, da = qkv[0, :, cols], qkv[1, :, cols], qkv[2, :, cols], d_attn[:, cols]
        outs = []
        for h in range(2):
            w = weights[2 * hp + h]
            dp = dot(da * sides[h], v, NT)
            ds = w * (dp - jnp.sum(w * dp, axis=-1, keepdims=True)) * 0.125
            ds = ds.astype(jnp.bfloat16)
            outs.append((dot(ds, k), dot(ds, q, TN)))
        for j in range(2):
            joined = jnp.where(is_low, outs[0][j], outs[1][j]).astype(jnp.bfloat16)
            packed[TOKENS * j : TOKENS * (j + 1), cols] = joined
        if hp > 0:
            pair(3 + hp).start()
    pair(7).start()
    products(shaped_t.at[:, core], packed, 0, 2, False)
    ring_step(1, 0, 1)
    for k in (4, 5, 6, 7):
        pair(k).wait_recv()
    products(shaped_in, packed_in, 0, 2, True)
    ring_step(0, 0, 0)
    ring_step(1, 0, 2)
    ring_step(0, 0, 1)
    ring_step(0, 0, 2)
    ring_step(0, 1, 0)
    ring_step(1, 1, 0)
    ring_step(0, 1, 1)
    ring_step(1, 1, 1)
    ring_step(0, 1, 2)
    z_start(0)
    ring_step(1, 1, 2)
    z_start(1)
    for which, (offset, width) in enumerate(extents):
        _, decoded = coder(*boxes[8 + which])
        for c in z_copies(which):
            c.wait_recv()
        for way in range(2):
            for j in range(offset // WIDE, (offset + width) // WIDE):
                cols, near = pl.ds(WIDE * j, WIDE), pl.ds(WIDE * j - offset, WIDE)
                out[j, :, pl.ds(WIDE * way, WIDE)] = last[way, z, :, cols] + decoded(way, near)
    leave = pltpu.make_async_copy(out, out_far, grads_sem)
    leave.start()
    squares = jnp.sum(out[...] * out[...])
    row = lax.broadcasted_iota(jnp.int32, (8, 128), 0)
    value = jnp.where(row == 0, squares, loss_part)
    totals[...] = sum_over_all(value, inbox, sum_send, sum_recv)
    leave.wait()
    for c in [*z_copies(0), *z_copies(1)]:
        c.wait_send()
    for c in swaps:
        c.wait_send()
    for k in range(8):
        pair(k).wait_send()
    for which in range(3):
        for hp in range(4):
            swap_pair(which, hp).wait_send()


def levels():
    lamb = 6.0 - 12.0 * np.arange(TGRID + 1) / TGRID
    return [np.sqrt(1.0 / (1.0 + np.exp(sign * lamb))).astype(np.float32) for sign in (-1.0, 1.0)]


ALPHAS, SIGMAS = levels()


def position_tables():
    half = D // 2
    freqs = np.exp(-math.log(10000.0) * np.arange(half) / half)
    fine = np.arange(16)[:, None] * freqs[None]
    angles = (np.sin(16.0 * fine), np.cos(16.0 * fine), np.sin(fine), np.cos(fine))
    return np.stack(angles).astype(np.float32)


def whole_step(timestep, bucket, bucket_weights, clean, noise, teacher, student):
    vmem, smem = (pl.BlockSpec(memory_space=m) for m in (pltpu.VMEM, pltpu.SMEM))
    bf16, f32 = jnp.bfloat16, jnp.float32

    def boxes(width):
        return [
            scratch
            for half in (128, 32, 128, 32)
            for scratch in [pltpu.VMEM((6, half, width), jnp.int16), pltpu.VMEM((6, 1, width), f32)] * 2
        ]

    def last_boxes(width):
        return [pltpu.VMEM((2, 32, width), jnp.int16), pltpu.VMEM((2, 1, width), f32)] * 2

    def semaphores(*shape):
        return [pltpu.SemaphoreType.DMA(shape)] * 2

    return pl.pallas_call(
        step_kernel,
        out_shape=(
            jax.ShapeDtypeStruct((4, 32, 512), f32),
            jax.ShapeDtypeStruct((8, 128), f32),
        ),
        in_specs=[smem] * 3 + [vmem] * 9 + [pl.BlockSpec(memory_space=pl.ANY)] * 2 + [vmem] * 2,
        out_specs=(pl.BlockSpec(memory_space=pl.ANY), vmem),
        scratch_shapes=[
            pltpu.VMEM((4, 32, 512), f32),
            pltpu.VMEM((6, 4, 4, 2, 2, 2, 16, 512), bf16),
            pltpu.VMEM((3, D, 512), bf16),
            pltpu.VMEM((4, 4, 2, 2, 2, 16, 512), bf16),
            pltpu.VMEM((4, TOKENS, D), f32),
            pltpu.VMEM((TOKENS, D), bf16),
            pltpu.VMEM((TOKENS, D), bf16),
            pltpu.VMEM((3, TOKENS, 512), bf16),
            pltpu.VMEM((3, TOKENS, 512), bf16),
            pltpu.VMEM((3, TOKENS, 512), bf16),
            pltpu.VMEM((8, TOKENS, TOKENS), f32),
            pltpu.VMEM((3, TOKENS, D), bf16),
            pltpu.VMEM((2, TOKENS, 128), f32),
            pltpu.VMEM((TOKENS, 512), bf16),
            pltpu.VMEM((128, D), bf16),
            pltpu.VMEM((128, D), bf16),
            pltpu.VMEM((384, D), bf16),
            pltpu.VMEM((32, 128), f32),
            pltpu.VMEM((32, 2, 32, TOKENS), bf16),
            pltpu.VMEM((32, 2, 32, TOKENS), bf16),
            pltpu.VMEM((32, 32, TOKENS), bf16),
            pltpu.VMEM((32, 32, TOKENS), bf16),
            pltpu.VMEM((4 * TOKENS, 512), bf16),
            pltpu.VMEM((4, 64, HALF), f32),
            pltpu.VMEM((4, 64, HALF), f32),
            pltpu.SemaphoreType.DMA,
            pltpu.SemaphoreType.DMA,
            pltpu.SemaphoreType.DMA,
            *semaphores(17),
            *semaphores(25),
            *semaphores(25),
            *semaphores(25),
            *boxes(2 * WIDE),
            *boxes(2 * WIDE),
            *last_boxes(2 * WIDE),
            *last_boxes(2 * WIDE),
            pltpu.VMEM((2, 2, 32, HALF), f32),
            *semaphores(8),
            *semaphores(8, 6, 2),
            *semaphores(4),
            pltpu.VMEM((2, 16, 8, 128), f32),
            *semaphores(2, 15),
        ],
        compiler_params=pltpu.CompilerParams(
            collective_id=2, has_side_effects=True, vmem_limit_bytes=63 * 2**20
        ),
    )(
        timestep,
        bucket,
        bucket_weights,
        clean,
        noise,
        jnp.asarray(position_tables()),
        teacher[0],
        teacher[1],
        jnp.moveaxis(teacher[2], 1, 0),
        student[0],
        student[1],
        jnp.moveaxis(student[2], 1, 0),
        jnp.moveaxis(teacher[3], 1, 0),
        teacher[4].reshape(4, 4, 2, 2, 2, 16, 512),
        jnp.moveaxis(student[3], 1, 0).reshape(3, 2, 16, 512),
        student[4].reshape(2, 16, 512),
    )


def adam_kernel(grads, totals, mq, vq, mo, vo, new_mq, new_vq, up_q, new_mo, new_vo, up_o, loss):
    rms = jnp.sqrt(totals[0:1, 0:1] / (4 * D * INNER))
    factor = 1.0 / jnp.maximum(rms, 1.0)

    def adam(grad, moment, second, new_moment, new_second, update):
        normed = grad * factor
        m = BETA_ONE * moment + (1.0 - BETA_ONE) * normed
        v = BETA_TWO * second + (1.0 - BETA_TWO) * normed * normed
        new_moment[...] = m
        new_second[...] = v
        update[...] = m / (jnp.sqrt(v) + ADAM_EPS)

    for j in range(3):
        adam(grads[j], mq[j], vq[j], new_mq.at[j], new_vq.at[j], up_q.at[j])
    adam(grads[3], mo[...], vo[...], new_mo, new_vo, up_o)
    loss[...] = totals[1:2, 0:1] / (SAMPLES * LATENT)


def adam_update(grads, totals, moment_qkv, second_qkv, moment_out, second_out):
    vmem = pl.BlockSpec(memory_space=pltpu.VMEM)
    mq, vq = (jnp.moveaxis(v, 1, 0) for v in (moment_qkv, second_qkv))
    qkv, out = (jax.ShapeDtypeStruct(v.shape, v.dtype) for v in (mq, moment_out))
    *news, loss = pl.pallas_call(
        adam_kernel,
        out_shape=(qkv, qkv, qkv, out, out, out, jax.ShapeDtypeStruct((1, 1), jnp.float32)),
        in_specs=[vmem] * 6,
        out_specs=(vmem,) * 7,
    )(grads, totals, mq, vq, moment_out, second_out)
    return (*(jnp.moveaxis(v, 0, 1) for v in news[:3]), *news[3:], loss.reshape(()))


def per_device(
    clean_latent,
    noise_draw,
    timestep,
    bucket,
    bucket_weights,
    teacher_embed,
    teacher_final,
    teacher_mod,
    teacher_qkv,
    teacher_out,
    student_embed,
    student_final,
    student_mod,
    student_qkv,
    student_out,
    moment_qkv,
    second_qkv,
    moment_out,
    second_out,
):
    grads, totals = whole_step(
        timestep,
        bucket,
        bucket_weights,
        clean_latent,
        noise_draw,
        (teacher_embed, teacher_final, teacher_mod, teacher_qkv, teacher_out),
        (student_embed, student_final, student_mod, student_qkv, student_out),
    )
    return adam_update(grads, totals, moment_qkv, second_qkv, moment_out, second_out)


def solution(mesh):
    torus = Mesh(
        mesh.devices.reshape(4, 4, 2, 2, mesh.shape["mp"]), ("dp_0", "dp_1", "dp_2", "dp_3", "mp")
    )
    in_specs = (
        P(DP, None),
        P(DP, None),
        P(DP),
        P(DP),
        P(),
        P(),
        P(),
        P(),
        P(None, None, "mp"),
        P(None, "mp"),
        P(),
        P(),
        P(),
        P(DP, None, "mp"),
        P(DP, "mp"),
        P(DP, None, "mp"),
        P(DP, None, "mp"),
        P(DP, "mp"),
        P(DP, "mp"),
    )
    out_specs = (
        P(DP, None, "mp"),
        P(DP, None, "mp"),
        P(DP, None, "mp"),
        P(DP, "mp"),
        P(DP, "mp"),
        P(DP, "mp"),
        P(),
    )
    return jax.shard_map(
        per_device, mesh=torus, in_specs=in_specs, out_specs=out_specs, check_vma=False
    )
```
